256 devices in a mesh: gx: 8 (over y, core), gy: 32 (over x, z).
Axes of the slice: x: 4, y: 4, z: 8, core: 2. Of those that a mesh axis runs over, the one named last changes fastest.
Arguments:
- source: float32 [64, 32, 4096], P(None, 'gx', 'gy'), may hold values from -6 to 6
- initial: float32 [64, 32, 4096], P(None, 'gx', 'gy'), may hold values from -6 to 6
- reaction: float32 [64, 32, 4096], P(None, 'gx', 'gy'), may hold values from 1 to 3
- stiffness: float32 [32, 4096], P('gx', 'gy'), may hold values from 0.5 to 2
- line_op: float32 [8, 8], replicated, may hold values from -1.6 to 5.6
- face_deriv: float32 [8], replicated, may hold values from -2 to 2
- wall_flags: int32 [4, 32, 4096], P(None, 'gx', 'gy'), may hold values 0 or 1
Outputs:
- hessenberg: float32 [6, 5], replicated
- krylov_basis: float32 [6, 64, 32, 4096], P(None, None, 'gx', 'gy')
The draws below stay inside these ranges and needn't reach their ends.
All inputs are finite; a program needn't handle non-finite values. No bound on the sum of `wall_flags` on one device may be relied on, other than what follows from the above.
Results may differ from the reference program's by a relative error of at most 0.0003.
Values sent between devices are 32-bit elements; how exact they have to be, the bound alone decides.
A program may use at most 64 MiB of HBM per device.

```python
import math
import jax
import jax.numpy as jnp
from jax import lax

P_SIZE = 8
ITERS = 5
NEX = 32
NEY = 4096


def draw_line_op(key, part):
    first_key, second_key = jax.random.split(jax.random.fold_in(key, 11))
    offdiag = jnp.clip(jax.random.normal(first_key, (P_SIZE, P_SIZE), jnp.float32) * 0.4, -1.6, 1.6)
    diagonal = jax.random.uniform(second_key, (P_SIZE,), jnp.float32, 2.0, 4.0)
    return offdiag * (1.0 - jnp.eye(P_SIZE, dtype=jnp.float32)) + jnp.diag(diagonal)


def place_ends(values, rng, least, largest):
    longest = values.shape.index(max(values.shape))
    spots = []
    for shift in (0, 1):
        where = [jax.random.randint(jax.random.fold_in(rng, axis), (), 0, length) for axis, length in enumerate(values.shape)]
        where[longest] = (where[longest] + shift) % values.shape[longest]
        spots.append(tuple(where))
    return values.at[spots[0]].set(least).at[spots[1]].set(largest)


def block_scale(rng, extent, cuts, low, largest):
    def one(position, shards_of):
        draws = jax.random.uniform(jax.random.fold_in(jax.random.fold_in(rng, 6), position), (shards_of,), jnp.float32, low / len(cuts), largest / len(cuts))
        return jnp.repeat(jnp.exp(draws), extent[position] // shards_of).reshape((-1,) + (1,) * (len(extent) - position - 1))

    factor_of = one(*cuts[0])
    for cut in cuts[1:]:
        factor_of = factor_of * one(*cut)
    return factor_of


def gaussian(rng, extent, deviation, most, cuts=(), held_as=jnp.bfloat16):
    values = deviation * jax.random.normal(rng, extent, jnp.float32)
    if cuts:
        values = values * block_scale(rng, extent, cuts, -0.22, 0.18)
    return jnp.clip(values, -most, most).astype(held_as)


def setup_inputs(seed: int = 0) -> dict:
    streams_of = jax.random.split(jax.random.key(seed), 8)
    source = gaussian(streams_of[0], (P_SIZE * P_SIZE, NEX, NEY), 1.0, 6.0, ((1, 8), (2, 32)), jnp.float32)
    initial = gaussian(streams_of[1], (P_SIZE * P_SIZE, NEX, NEY), 1.0, 6.0, ((1, 8), (2, 32)), jnp.float32)
    reaction = jnp.clip(1.0 + 2.0 * jax.random.uniform(streams_of[2], (P_SIZE * P_SIZE, NEX, NEY), jnp.float32) ** block_scale(streams_of[2], (P_SIZE * P_SIZE, NEX, NEY), ((1, 8), (2, 32)), -0.2, 0.2), 1.0, 3.0)
    stiffness = jnp.clip(jnp.exp(math.log(2.0) - 1.3862944 * jax.random.uniform(streams_of[3], (NEX, NEY), jnp.float32) ** block_scale(streams_of[3], (NEX, NEY), ((0, 8), (1, 32)), -0.2, 0.2)), 0.5, 2.0)
    line_op = draw_line_op(jax.random.fold_in(streams_of[7], 71), 0)
    face_deriv = gaussian(streams_of[5], (P_SIZE,), 0.5, 2.0, (), jnp.float32)
    wall_flags = place_ends((jax.random.randint(streams_of[6], (4, NEX, NEY), 0, 4) < 1).astype(jnp.int32), jax.random.fold_in(streams_of[6], 1), 0, 1)
    return {"source": source, "initial": initial, "reaction": reaction, "stiffness": stiffness, "line_op": line_op, "face_deriv": face_deriv, "wall_flags": wall_flags}


TAU = 2.0
FLOOR = 0.1

def block_sum(values):
    flat = values.reshape(-1)
    width = 1024
    extra = -flat.shape[0] % width
    flat = jnp.concatenate([flat, jnp.zeros((extra,), flat.dtype)])
    return jnp.sum(lax.optimization_barrier(jnp.sum(flat.reshape(-1, width), axis=1)))

def apply_op(field, reaction, stiffness, line_op, face_deriv, wall_flags):
    highest = lax.Precision.HIGHEST
    nodes = field.reshape(P_SIZE, P_SIZE, field.shape[1], field.shape[2])
    interior = stiffness * (jnp.einsum('ac,cbxy->abxy', line_op, nodes, precision=highest) + jnp.einsum('bc,acxy->abxy', line_op, nodes, precision=highest))
    reversed_w = face_deriv[::-1]
    west_val = nodes[0]
    east_val = nodes[P_SIZE - 1]
    south_val = nodes[:, 0]
    north_val = nodes[:, P_SIZE - 1]
    west_der = jnp.einsum('c,cbxy->bxy', face_deriv, nodes, precision=highest)
    east_der = jnp.einsum('c,cbxy->bxy', reversed_w, nodes, precision=highest)
    south_der = jnp.einsum('c,acxy->axy', face_deriv, nodes, precision=highest)
    north_der = jnp.einsum('c,acxy->axy', reversed_w, nodes, precision=highest)
    opened = 1.0 - wall_flags.astype(field.dtype)
    add_east = TAU * (east_val - opened[1] * jnp.roll(west_val, -1, 1)) + 0.5 * (east_der - opened[1] * jnp.roll(west_der, -1, 1))
    add_west = TAU * (west_val - opened[0] * jnp.roll(east_val, 1, 1)) + 0.5 * (west_der - opened[0] * jnp.roll(east_der, 1, 1))
    add_north = TAU * (north_val - opened[3] * jnp.roll(south_val, -1, 2)) + 0.5 * (north_der - opened[3] * jnp.roll(south_der, -1, 2))
    add_south = TAU * (south_val - opened[2] * jnp.roll(north_val, 1, 2)) + 0.5 * (south_der - opened[2] * jnp.roll(north_der, 1, 2))
    result = reaction.reshape(nodes.shape) * nodes + interior
    result = result.at[0].add(add_west).at[P_SIZE - 1].add(add_east)
    result = result.at[:, 0].add(add_south).at[:, P_SIZE - 1].add(add_north)
    return result.reshape(field.shape)

def reference(source, initial, reaction, stiffness, line_op, face_deriv, wall_flags):
    total = float(P_SIZE * P_SIZE * NEX * NEY)

    def operate(field):
        return apply_op(field, reaction, stiffness, line_op, face_deriv, wall_flags)
    first = source - operate(initial)
    beta_first = jnp.sqrt(block_sum(first * first) / total + FLOOR)
    vectors = [first / beta_first]
    hessen = jnp.zeros((ITERS + 1, ITERS), source.dtype)
    for step in range(ITERS):
        image = operate(vectors[step])
        coeffs = [block_sum(vector * image) / total for vector in vectors]
        for index in range(len(vectors)):
            image = image - coeffs[index] * vectors[index]
            hessen = hessen.at[index, step].set(coeffs[index])
        beta = jnp.sqrt(block_sum(image * image) / total + FLOOR)
        hessen = hessen.at[step + 1, step].set(beta)
        vectors.append(image / beta)
    return (hessen, jnp.stack(vectors))
```

```python
import functools

import jax
import jax.numpy as jnp
from jax import lax
from jax.experimental import pallas as pl
from jax.experimental.pallas import tpu as pltpu
from jax.sharding import Mesh
from jax.sharding import PartitionSpec as P

P_SIZE = 8
ITERS = 5
NV = ITERS + 1
TAU = 2.0
FLOOR = 0.1
MESH = pl.DeviceIdType.MESH
AXES = ("y", "c", "x", "z")
PAIRS = [(i, j) for j in range(NV) for i in range(j + 1)]


def two_sum(a, b):
    s = a + b
    t = s - a
    return s, (a - (s - t)) + (b - t)


def quick(a, b):
    s = a + b
    return s, b - (s - a)


def split(a):
    c = a * 4097.0
    hi = c - (c - a)
    return hi, a - hi


def two_prod(a, b):
    p = a * b
    ah, al = split(a)
    bh, bl = split(b)
    return p, ((ah * bh - p) + ah * bl + al * bh) + al * bl


def add2(a, b):
    s, e = two_sum(a[0], b[0])
    return quick(s, e + (a[1] + b[1]))


def mul2(a, b):
    p, e = two_prod(a[0], b[0])
    return quick(p, e + (a[0] * b[1] + a[1] * b[0]))


def mul1(a, b):
    p, e = two_prod(a[0], b)
    return quick(p, e + a[1] * b)


def tree(items, op):
    items = list(items)
    while len(items) > 1:
        nxt = [op(items[i], items[i + 1]) for i in range(0, len(items) - 1, 2)]
        if len(items) % 2:
            nxt.append(items[-1])
        items = nxt
    return items[0]


def sublane_total(a):
    for s in (4, 2, 1):
        a = add2(a, tuple(pltpu.roll(v, s, 0) for v in a))
    return a


def kernel(sizes, line, fd, src_h, x0_h, rx_h, st_h, wf_h, hess, out_h,
           srcv, xin, rxin, stin, wfin, w, rx, st, op, qf, sxy, rxy, row1, buf1, row2, buf2, vout,
           lsem, osem, hs, hr, s1, r1, s2, r2):
    ny, nc, nx, nz = sizes
    y, c, x, z = (lax.axis_index(a) for a in AXES)

    def gx(s):
        g = lax.rem(y * nc + c + ny * nc + s, ny * nc)
        return (g // nc, lax.rem(g, nc), x, z)

    def gy(s):
        g = lax.rem(x * nz + z + nx * nz + s, nx * nz)
        return (y, c, g // nz, lax.rem(g, nz))

    east, west, north, south = gx(1), gx(-1), gy(1), gy(-1)
    group1 = [
        (lax.rem(y + i, ny), lax.rem(c + j, nc), lax.rem(x + k, nx), z)
        for i in range(ny) for j in range(nc) for k in range(nx) if i + j + k > 0
    ]
    group2 = [(y, c, x, lax.rem(z + k, nz)) for k in range(1, nz)]
    barrier = pltpu.get_barrier_semaphore()
    greeted = [east, west, north, south] + group1 + group2
    for peer in greeted:
        pl.semaphore_signal(barrier, inc=1, device_id=peer, device_id_type=MESH)
    loads = [
        pltpu.make_async_copy(a, b, lsem.at[i])
        for i, (a, b) in enumerate([(x0_h, xin), (rx_h, rxin), (src_h, srcv), (st_h, stin), (wf_h, wfin)])
    ]
    for cp in loads:
        cp.start()

    n = P_SIZE
    total = float(ny * nc * nx * nz * src_h.shape[0] * src_h.shape[1] * src_h.shape[2])
    lop = [[line[i, j] for j in range(n)] for i in range(n)]
    g = [0.5 * fd[i] + (TAU if i == 0 else 0.0) for i in range(n)]
    diag = lop[0][0]
    for i in range(1, n):
        diag = diag + lop[i][i]
    shift = 3.0 + 0.3125 * diag + 0.25 * fd[0]

    lane = lax.broadcasted_iota(jnp.int32, (8, 128), 1)
    sub = lax.broadcasted_iota(jnp.int32, (8, 128), 0)
    group = lane // 16
    zero4 = jnp.zeros((4, 128), jnp.float32)
    for cp in loads:
        cp.wait()
    for q in range(n * n):
        w[0, q, 0:4, :] = xin[q]
        w[0, q, 4:8, :] = zero4
        rx[q, 0:4, :] = rxin[q] - shift
        rx[q, 4:8, :] = zero4
    st[0:4, :] = stin[...]
    st[4:8, :] = zero4
    for f in range(4):
        op[f, 0:4, :] = 1.0 - wfin[f].astype(jnp.float32)
        op[f, 4:8, :] = zero4
    pl.semaphore_wait(barrier, len(greeted))

    def apply(k):
        def v(a, b):
            return w[k, a * n + b]

        pn = ps = jnp.zeros((8, 128), jnp.float32)
        for a in range(n):
            qs = tree([g[i] * v(a, i) for i in range(n)], jnp.add)
            qn = tree([g[i] * v(a, n - 1 - i) for i in range(n)], jnp.add)
            qf[2, a] = qs
            qf[3, a] = qn
            pn = jnp.where(group == a, pltpu.roll(qn, (16 * a + 1) % 128, 1), pn)
            ps = jnp.where(group == a, pltpu.roll(qs, 16 * a, 1), ps)
        sxy[k, 2] = ps
        sxy[k, 3] = pn
        for b in range(n):
            qw = tree([g[i] * v(i, b) for i in range(n)], jnp.add)
            qe = tree([g[i] * v(n - 1 - i, b) for i in range(n)], jnp.add)
            qf[0, b] = qw
            qf[1, b] = qe
            sxy[k, 0, pl.ds(b, 1), :] = qw[0:1, :]
            sxy[k, 1, pl.ds(b, 1), :] = qe[3:4, :]
        copies = []
        for f, peer in ((3, north), (2, south), (1, east), (0, west)):
            cp = pltpu.make_async_remote_copy(
                src_ref=sxy.at[k, f], dst_ref=rxy.at[k, f], send_sem=hs.at[k, f], recv_sem=hr.at[k, f],
                device_id=peer, device_id_type=MESH)
            cp.start()
            copies.append(cp)
        stiff = st[...]
        for b in range(n):
            col = [v(i, b) for i in range(n)]
            for a in range(n):
                acc = tree([lop[a][i] * col[i] for i in range(n)] + [lop[b][i] * v(a, i) for i in range(n)], jnp.add)
                w[k + 1, a * n + b] = rx[a * n + b] * col[a] + stiff * acc
        for cp in copies:
            cp.wait()
        for b in range(n):
            before = jnp.where(sub == 0, jnp.broadcast_to(rxy[k, 1, pl.ds(b, 1), :], (8, 128)), pltpu.roll(qf[1, b], 1, 0))
            after = jnp.where(sub == 3, jnp.broadcast_to(rxy[k, 0, pl.ds(b, 1), :], (8, 128)), pltpu.roll(qf[0, b], 7, 0))
            w[k + 1, b] = w[k + 1, b] + (qf[0, b] - op[0] * before)
            w[k + 1, 7 * n + b] = w[k + 1, 7 * n + b] + (qf[1, b] - op[1] * after)
        rn = rxy[k, 3]
        rs = rxy[k, 2]
        for a in range(n):
            before = jnp.where(lane == 0, pltpu.roll(rn, (128 - 16 * a) % 128, 1), pltpu.roll(qf[3, a], 1, 1))
            after = jnp.where(lane == 127, pltpu.roll(rs, (127 - 16 * a) % 128, 1), pltpu.roll(qf[2, a], 127, 1))
            w[k + 1, a * n] = w[k + 1, a * n] + (qf[2, a] - op[2] * before)
            w[k + 1, a * n + 7] = w[k + 1, a * n + 7] + (qf[3, a] - op[3] * after)

    apply(0)
    for q in range(n * n):
        w[1, q, 0:4, :] = w[1, q, 0:4, :] - (srcv[q] - shift * xin[q])

    def step(k, carry):
        apply(k)
        return carry

    lax.fori_loop(1, NV, step, 0)

    def gram(q, acc):
        vals = [w[i + 1, q] for i in range(NV)]
        return tuple(t + vals[i] * vals[j] for t, (i, j) in zip(acc, PAIRS))

    acc = lax.fori_loop(0, n * n, gram, tuple(jnp.zeros((8, 128), jnp.float32) for _ in PAIRS))
    line_row = jnp.zeros((8, 128), jnp.float32)
    for base in range(0, len(PAIRS), 8):
        packed = jnp.zeros((8, 128), jnp.float32)
        for i, t in enumerate(acc[base:base + 8]):
            t = jnp.where(sub < 4, t, 0.0)
            t = t + pltpu.roll(t, 4, 0)
            t = t + pltpu.roll(t, 2, 0)
            t = t + pltpu.roll(t, 1, 0)
            packed = jnp.where(sub == i, t, packed)
        packed = jnp.sum(packed, axis=1, keepdims=True) * (1.0 / total)
        line_row = line_row + jnp.where(lane == sub + base, packed, 0.0)
    for s in (4, 2, 1):
        line_row = line_row + pltpu.roll(line_row, s, 0)
    row1[...] = line_row[0:1, :]
    copies = []
    for j, peer in enumerate(group1):
        cp = pltpu.make_async_remote_copy(
            src_ref=row1, dst_ref=buf1.at[j], send_sem=s1.at[j], recv_sem=r1.at[j], device_id=peer, device_id_type=MESH)
        cp.start()
        copies.append(cp)
    for cp in copies:
        cp.wait()
    zero1 = jnp.zeros((1, 128), jnp.float32)
    part = tree([(row1[...], zero1)] + [(buf1[j], zero1) for j in range(len(group1))], add2)
    row2[0:1, :] = part[0]
    row2[1:2, :] = part[1]
    copies = []
    for j, peer in enumerate(group2):
        cp = pltpu.make_async_remote_copy(
            src_ref=row2, dst_ref=buf2.at[j], send_sem=s2.at[j], recv_sem=r2.at[j], device_id=peer, device_id_type=MESH)
        cp.start()
        copies.append(cp)
    for cp in copies:
        cp.wait()
    part = tree([part] + [(buf2[j, 0:1, :], buf2[j, 1:2, :]) for j in range(len(group2))], add2)

    slot = {}
    for p, (i, j) in enumerate(PAIRS):
        slot[i, j] = slot[j, i] = p
    columns = []
    for k in range(NV):
        at = jnp.full((8, 128), -1, jnp.int32)
        for i in range(NV):
            at = jnp.where(sub == i, slot[i, k], at)
        columns.append(tuple(
            jnp.broadcast_to(
                jnp.sum(jnp.where(lane == at, jnp.broadcast_to(t, (8, 128)), 0.0), axis=1, keepdims=True), (8, 128))
            for t in part))

    def spread(t, k):
        return jnp.broadcast_to(t[k:k + 1, :], (8, 128))

    def times_gram(u):
        return tree([mul2(columns[k], tuple(spread(t, k) for t in u)) for k in range(NV)], add2)

    def dot(a, b):
        return sublane_total(mul2(a, b))

    hmat = jnp.zeros((8, 128), jnp.float32)
    zeros = jnp.zeros((8, 128), jnp.float32)
    u = (jnp.where(sub == 0, -1.0, 0.0), zeros)
    e = times_gram(u)
    coefs, images = [], []
    for j in range(NV):
        square = dot(u, e)[0] + FLOOR
        inv = lax.rsqrt(square)
        if j > 0:
            hmat = jnp.where((sub == j) & (lane == j - 1), square * inv, hmat)
        coefs.append(mul1(u, inv))
        images.append(mul1(e, inv))
        if j == ITERS:
            break
        moved = tuple(pltpu.roll(t, 1, 0) for t in coefs[j])
        u = add2(moved, mul1(coefs[j], jnp.broadcast_to(shift, (8, 128))))
        e = times_gram(u)
        hs_j = [dot(images[i], u)[0] for i in range(j + 1)]
        for i in range(j + 1):
            hmat = jnp.where((sub == i) & (lane == j), hs_j[i], hmat)
        u = tree([u] + [mul1(coefs[i], -hs_j[i]) for i in range(j + 1)], add2)
        e = tree([e] + [mul1(images[i], -hs_j[i]) for i in range(j + 1)], add2)
    hess[...] = hmat[0:NV, 0:ITERS]

    weights = [[jnp.broadcast_to(coefs[j][0][i:i + 1, :], (8, 128)) for i in range(j + 1)] for j in range(NV)]

    outs = []
    for j in range(NV):
        def combine(q, carry, j=j):
            t = tree([weights[j][i] * w[i + 1, q] for i in range(j + 1)], jnp.add)
            vout[j, q] = t[0:4, :]
            return carry

        lax.fori_loop(0, n * n, combine, 0, unroll=8)
        cp = pltpu.make_async_copy(vout.at[j], out_h.at[j], osem.at[j])
        cp.start()
        outs.append(cp)
    for cp in outs:
        cp.wait()


def solution(mesh):
    ny, nc, nx, nz = 4, 2, 4, 8
    finer = Mesh(mesh.devices.reshape(ny, nc, nx, nz), AXES)
    gxs, gys = ("y", "c"), ("x", "z")
    sizes = (ny, nc, nx, nz)
    f32 = jnp.float32

    def body(source, initial, reaction, stiffness, line_op, face_deriv, wall_flags):
        nodes, ex, ey = source.shape
        n1, n2 = ny * nc * nx - 1, nz - 1
        anywhere = pl.BlockSpec(memory_space=pl.ANY)
        scalars = pl.BlockSpec(memory_space=pltpu.SMEM)
        vm = pltpu.VMEM
        dma = pltpu.SemaphoreType.DMA
        return pl.pallas_call(
            functools.partial(kernel, sizes),
            out_shape=(
                jax.ShapeDtypeStruct((NV, ITERS), f32),
                jax.ShapeDtypeStruct((NV, nodes, ex, ey), f32),
            ),
            in_specs=[scalars, scalars] + [anywhere] * 5,
            out_specs=(pl.BlockSpec(memory_space=pltpu.VMEM), anywhere),
            scratch_shapes=[
                vm((nodes, ex, ey), f32), vm((nodes, ex, ey), f32), vm((nodes, ex, ey), f32),
                vm((ex, ey), f32), vm((4, ex, ey), jnp.int32),
                vm((NV + 1, nodes, 8, ey), f32), vm((nodes, 8, ey), f32), vm((8, ey), f32), vm((4, 8, ey), f32),
                vm((4, 8, 8, ey), f32),
                vm((NV, 4, 8, ey), f32), vm((NV, 4, 8, ey), f32),
                vm((1, 128), f32), vm((n1, 1, 128), f32), vm((2, 128), f32), vm((n2, 2, 128), f32),
                vm((NV, nodes, ex, ey), f32),
                dma((5,)), dma((NV,)), dma((NV, 4)), dma((NV, 4)), dma((n1,)), dma((n1,)), dma((n2,)), dma((n2,)),
            ],
            compiler_params=pltpu.CompilerParams(
                collective_id=0, has_side_effects=True, vmem_limit_bytes=48 * 1024 * 1024),
            name="arnoldi",
        )(line_op, face_deriv, source, initial, reaction, stiffness, wall_flags)

    placed = (P(None, gxs, gys), P(None, gxs, gys), P(None, gxs, gys), P(gxs, gys), P(), P(), P(None, gxs, gys))
    return jax.shard_map(
        body, mesh=finer, in_specs=placed, out_specs=(P(), P(None, None, gxs, gys)), check_vma=False)
```

```python
import functools

import jax
import jax.numpy as jnp
from jax import lax
from jax.experimental import pallas as pl
from jax.experimental.pallas import tpu as pltpu
from jax.sharding import Mesh
from jax.sharding import PartitionSpec as P

P_SIZE = 8
ITERS = 5
NV = ITERS + 1
TAU = 2.0
FLOOR = 0.1
MESH = pl.DeviceIdType.MESH
AXES = ("y", "c", "x", "z")
PAIRS = [(i, j) for j in range(NV) for i in range(j + 1)]


def two_sum(a, b):
    s = a + b
    t = s - a
    return s, (a - (s - t)) + (b - t)


def quick(a, b):
    s = a + b
    return s, b - (s - a)


def split(a):
    c = a * 4097.0
    hi = c - (c - a)
    return hi, a - hi


def two_prod(a, b):
    p = a * b
    ah, al = split(a)
    bh, bl = split(b)
    return p, ((ah * bh - p) + ah * bl + al * bh) + al * bl


def add2(a, b):
    s, e = two_sum(a[0], b[0])
    return quick(s, e + (a[1] + b[1]))


def mul2(a, b):
    p, e = two_prod(a[0], b[0])
    return quick(p, e + (a[0] * b[1] + a[1] * b[0]))


def mul1(a, b):
    p, e = two_prod(a[0], b)
    return quick(p, e + a[1] * b)


def tree(items, op):
    items = list(items)
    while len(items) > 1:
        nxt = [op(items[i], items[i + 1]) for i in range(0, len(items) - 1, 2)]
        if len(items) % 2:
            nxt.append(items[-1])
        items = nxt
    return items[0]


def sublane_total(a):
    for s in (4, 2, 1):
        a = add2(a, tuple(pltpu.roll(v, s, 0) for v in a))
    return a


def kernel(sizes, line, fd, src_h, x0_h, rx_h, st_h, wf_h, hess, vout,
           xl, sl, rl, stl, wfl, opl, w, sv, rx, st, op, gw, pk, lb, rb, qs, qr, gqs, gql, gqr, qf,
           row1, buf1, row2, buf2,
           lsem, hs, hr, s1, r1, s2, r2):
    ny, nc, nx, nz = sizes
    y, c, x, z = (lax.axis_index(a) for a in AXES)

    def at(dx, dy):
        i = lax.rem(y * nc + c + ny * nc + dx, ny * nc)
        j = lax.rem(x * nz + z + nx * nz + dy, nx * nz)
        return (i // nc, lax.rem(i, nc), j // nz, lax.rem(j, nz))

    group1 = [
        (lax.rem(y + i, ny), lax.rem(c + j, nc), lax.rem(x + k, nx), z)
        for i in range(ny) for j in range(nc) for k in range(nx) if i + j + k > 0
    ]
    group2 = [(y, c, x, lax.rem(z + k, nz)) for k in range(1, nz)]
    around = {(i, j): at(i, j) for i in (-1, 0, 1) for j in (-1, 0, 1) if (i, j) != (0, 0)}
    barrier = pltpu.get_barrier_semaphore()
    greeted = list(around.values()) + group1 + group2
    for peer in greeted:
        pl.semaphore_signal(barrier, inc=1, device_id=peer, device_id_type=MESH)
    own = pl.ds(0, 4)
    pairs = [(x0_h, xl.at[:, own, :]), (rx_h, rl.at[:, own, :]), (src_h, sl.at[:, own, :]), (st_h, stl.at[own, :]),
             (wf_h, wfl.at[:, own, :]), (x0_h, w.at[0, :, own, :]), (rx_h, rx.at[:, own, :]), (src_h, sv.at[:, own, :])]
    loads = [pltpu.make_async_copy(a, b, lsem.at[i]) for i, (a, b) in enumerate(pairs)]
    for cp in loads:
        cp.start()

    n = P_SIZE
    total = float(ny * nc * nx * nz * src_h.shape[0] * src_h.shape[1] * src_h.shape[2])
    lop = [[line[i, j] for j in range(n)] for i in range(n)]
    g = [0.5 * fd[i] + (TAU if i == 0 else 0.0) for i in range(n)]
    diag = lop[0][0]
    for i in range(1, n):
        diag = diag + lop[i][i]
    shift = 3.0 + 0.3125 * diag + 0.25 * fd[0]

    lane = lax.broadcasted_iota(jnp.int32, (8, 128), 1)
    sub = lax.broadcasted_iota(jnp.int32, (8, 128), 0)
    group = lane // 16
    slot16 = lax.rem(lane, 16)

    def lroll(t, s):
        s = s % 128
        return t if s == 0 else pltpu.roll(t, s, 1)

    def gather_groups(items, s):
        out = lroll(items[0], s)
        for a in range(1, len(items)):
            out = jnp.where(group == a, lroll(items[a], 16 * a + s), out)
        return out

    cline, cface = [], []
    for k in range(n):
        t = jnp.zeros((8, 128), jnp.float32)
        for a in range(n):
            t = jnp.where(group == a, lop[a][(a - k) % n], t)
        cline.append(t)
        cface.append(jnp.where(group == 0, g[(n - k) % n], jnp.where(group == n - 1, g[k], 0.0)))

    def x_faces(v):
        qw = [tree([g[i] * v(i, b) for i in range(n)], jnp.add) for b in range(n)]
        qe = [tree([g[i] * v(n - 1 - i, b) for i in range(n)], jnp.add) for b in range(n)]
        return qw, qe

    def strip_faces(t):
        rolled = [t] + [lroll(t, 16 * k) for k in range(1, n)]
        return rolled, tree([cface[k] * rolled[k] for k in range(n)], jnp.add)

    for cp in loads[:5]:
        cp.wait()
    opl[...] = 1.0 - wfl[...].astype(jnp.float32)
    qw, qe = x_faces(lambda a, b: xl[a * n + b])
    for b in range(n):
        qs[0, 0, pl.ds(b, 1), :] = qw[b][2:3, :]
        qs[0, 1, pl.ds(b, 1), :] = qe[b][1:2, :]
    for b in range(n):
        px = gather_groups([xl[a * n + b] for a in range(n)], 6)
        ps = gather_groups([sl[a * n + b] for a in range(n)], 6)
        pr = gather_groups([rl[a * n + b] for a in range(n)], 6)
        pk[0, b] = jnp.where(slot16 < 6, px, jnp.where(slot16 < 11, lroll(ps, 5), lroll(pr, 10)))
        pk[1, b] = jnp.where(slot16 < 6, lroll(px, -6), jnp.where(slot16 < 11, ps, lroll(pr, 5)))
        face = strip_faces(px)[1]
        gqs[0, 0, pl.ds(b, 1), :] = face[2:3, :]
        gqs[0, 1, pl.ds(b, 1), :] = face[1:2, :]
    pst = gather_groups([stl[...]] + [opl[f] for f in range(4)], 6)
    pk[0, n] = pst
    pk[1, n] = pst
    pl.semaphore_wait(barrier, len(greeted))

    def send(copies, peer, pieces, first):
        for i, (a, b) in enumerate(pieces):
            cp = pltpu.make_async_remote_copy(
                src_ref=a, dst_ref=b, send_sem=hs.at[first + i], recv_sem=hr.at[first + i],
                device_id=peer, device_id_type=MESH)
            cp.start()
            copies.append(cp)
        return first + len(pieces)

    def rows(lo):
        return pl.ds(lo, 2)

    copies, used = [], 0
    for dy, k, dst in ((1, 0, lb), (-1, 1, rb)):
        used = send(copies, around[0, dy], [(pk.at[k, :, own, :], dst.at[:, own, :])], used)
    for dy, k, dst, gq in ((1, 0, lb, gql), (-1, 1, rb, gqr)):
        for dx, lo, to in ((1, 2, 6), (-1, 0, 4)):
            side = 1 if dx > 0 else 0
            used = send(copies, around[dx, dy], [
                (pk.at[k, :, rows(lo), :], dst.at[:, rows(to), :]), (gqs.at[0, side], gq.at[0, side])], used)
    for dx, lo, to in ((1, 2, 6), (-1, 0, 4)):
        side = 1 if dx > 0 else 0
        used = send(copies, around[dx, 0], [
            (xl.at[:, rows(lo), :], w.at[0, :, rows(to), :]),
            (rl.at[:, rows(lo), :], rx.at[:, rows(to), :]),
            (sl.at[:, rows(lo), :], sv.at[:, rows(to), :]),
            (stl.at[rows(lo), :], st.at[rows(to), :]),
            (opl.at[:, rows(lo), :], op.at[:, rows(to), :]),
            (qs.at[0, side], qr.at[0, side])], used)
    st[0:4, :] = stl[0:4, :]
    op[:, 0:4, :] = opl[:, 0:4, :]
    for cp in loads[5:]:
        cp.wait()
    for cp in copies:
        cp.wait()

    before_half = slot16 < 6
    gsv, grx = [], []
    for b in range(n):
        lo, hi = lb[b], rb[b]
        gw[0, b] = jnp.where(before_half, lo, lroll(hi, 6))
        gsv.append(jnp.where(before_half, lroll(lo, -5), hi))
        grx.append(jnp.where(before_half, lroll(lo, -10), lroll(hi, -5)))
    both = jnp.where(before_half, lb[n], rb[n])
    spreads = []
    for f in range(5):
        t = jnp.where(group == f, both, 0.0)
        for s in (16, 32, 64):
            t = t + lroll(t, s)
        spreads.append(t)
    gst = spreads[0]
    gopw = jnp.where(group == 0, spreads[1], 0.0)
    gope = jnp.where(group == n - 1, spreads[2], 0.0)
    gops, gopn = spreads[3], spreads[4]
    for side in (0, 1):
        gqr[0, side] = jnp.where(before_half, gql[0, side], gqr[0, side])

    def apply(k, last=False, fresh=None):
        wide = k != 2

        def v(a, b):
            return w[k, a * n + b]

        def keep(a, b, t):
            if wide:
                w[k + 1, a * n + b] = t
            else:
                w[k + 1, a * n + b, 0:4, :] = t[0:4, :]

        gv = [gw[k, b] for b in range(n)]
        gqsouth = tree([g[i] * gv[i] for i in range(n)], jnp.add)
        gqnorth = tree([g[i] * gv[n - 1 - i] for i in range(n)], jnp.add)
        qsouth = [tree([g[i] * v(a, i) for i in range(n)], jnp.add) for a in range(n)]
        qnorth = [tree([g[i] * v(a, n - 1 - i) for i in range(n)], jnp.add) for a in range(n)]
        for a in range(n):
            below = jnp.where(lane == 0, lroll(gqnorth, -(16 * a + 5)), lroll(qnorth[a], 1))
            above = jnp.where(lane == 127, lroll(gqsouth, 121 - 16 * a), lroll(qsouth[a], -1))
            qf[2, a] = qsouth[a] - op[2] * below
            qf[3, a] = qnorth[a] - op[3] * above
        if not last:
            mn = gather_groups(qnorth, 7)
            ms = gather_groups(qsouth, 5)
            sterm = gqsouth - gops * jnp.where(slot16 == 6, mn, lroll(gqnorth, 1))
            nterm = gqnorth - gopn * jnp.where(slot16 == 5, ms, lroll(gqsouth, -1))
            for b in range(n):
                rolled, face = strip_faces(gv[b])
                prev = pltpu.roll(lroll(face, 16), 1, 0)
                nxt = pltpu.roll(lroll(face, -16), 7, 0)
                if fresh is not None:
                    prev = jnp.where(sub == 6, jnp.broadcast_to(lroll(gqr[fresh, 1, pl.ds(b, 1), :], 16), (8, 128)), prev)
                    nxt = jnp.where(sub == 5, jnp.broadcast_to(lroll(gqr[fresh, 0, pl.ds(b, 1), :], -16), (8, 128)), nxt)
                acc = tree([cline[i] * rolled[i] for i in range(n)] + [lop[b][i] * gv[i] for i in range(n)], jnp.add)
                t = grx[b] * gv[b] + gst * acc + (face - (gopw * prev + gope * nxt))
                if b == 0:
                    t = t + sterm
                if b == n - 1:
                    t = t + nterm
                t = t - (gsv[b] if k == 0 else shift * gv[b])
                if wide:
                    gw[k + 1, b] = t
                else:
                    gw[k + 1, b, 0:4, :] = t[0:4, :]
        stiff = st[...]
        for b in range(n):
            col = [v(i, b) for i in range(n)]
            qwest = tree([g[i] * col[i] for i in range(n)], jnp.add)
            qeast = tree([g[i] * col[n - 1 - i] for i in range(n)], jnp.add)
            prev = pltpu.roll(qeast, 1, 0)
            nxt = pltpu.roll(qwest, 7, 0)
            if fresh is not None:
                prev = jnp.where(sub == 6, jnp.broadcast_to(qr[fresh, 1, pl.ds(b, 1), :], (8, 128)), prev)
                nxt = jnp.where(sub == 5, jnp.broadcast_to(qr[fresh, 0, pl.ds(b, 1), :], (8, 128)), nxt)
            for a in range(n):
                acc = tree([lop[a][i] * col[i] for i in range(n)] + [lop[b][i] * v(a, i) for i in range(n)], jnp.add)
                if k == 0:
                    t = rx[a * n + b] * col[a] - sv[a * n + b] + stiff * acc
                else:
                    t = (rx[a * n + b] - shift) * col[a] + stiff * acc
                if a == 0:
                    t = t + (qwest - op[0] * prev)
                if a == n - 1:
                    t = t + (qeast - op[1] * nxt)
                if b == 0:
                    t = t + qf[2, a]
                if b == n - 1:
                    t = t + qf[3, a]
                keep(a, b, t)

    apply(0, fresh=0)
    apply(1)
    apply(2)
    qw, qe = x_faces(lambda a, b: w[3, a * n + b, 0:4, :])
    for b in range(n):
        qs[1, 0, pl.ds(b, 1), :] = qw[b][2:3, :]
        qs[1, 1, pl.ds(b, 1), :] = qe[b][1:2, :]
        t = jnp.concatenate([gw[3, b, 0:4, :]] * 2, axis=0)
        face = strip_faces(t)[1]
        gqs[1, 0, pl.ds(b, 1), :] = face[2:3, :]
        gqs[1, 1, pl.ds(b, 1), :] = face[1:2, :]
    copies = []
    for dx, lo, to in ((1, 2, 6), (-1, 0, 4)):
        side = 1 if dx > 0 else 0
        used = send(copies, around[dx, 0], [
            (w.at[3, :, rows(lo), :], w.at[3, :, rows(to), :]),
            (gw.at[3, :, rows(lo), :], gw.at[3, :, rows(to), :]),
            (qs.at[1, side], qr.at[1, side]),
            (gqs.at[1, side], gqr.at[1, side])], used)
    for cp in copies:
        cp.wait()
    apply(3, fresh=1)
    apply(4)
    apply(5, last=True)

    def gram(q, acc):
        vals = [w[i + 1, q] for i in range(NV)]
        return tuple(t + vals[i] * vals[j] for t, (i, j) in zip(acc, PAIRS))

    acc = lax.fori_loop(0, n * n, gram, tuple(jnp.zeros((8, 128), jnp.float32) for _ in PAIRS))
    line_row = jnp.zeros((8, 128), jnp.float32)
    for base in range(0, len(PAIRS), 8):
        packed = jnp.zeros((8, 128), jnp.float32)
        for i, t in enumerate(acc[base:base + 8]):
            t = jnp.where(sub < 4, t, 0.0)
            t = t + pltpu.roll(t, 4, 0)
            t = t + pltpu.roll(t, 2, 0)
            t = t + pltpu.roll(t, 1, 0)
            packed = jnp.where(sub == i, t, packed)
        packed = jnp.sum(packed, axis=1, keepdims=True) * (1.0 / total)
        line_row = line_row + jnp.where(lane == sub + base, packed, 0.0)
    for s in (4, 2, 1):
        line_row = line_row + pltpu.roll(line_row, s, 0)
    row1[...] = line_row[0:1, :]
    copies = []
    for j, peer in enumerate(group1):
        cp = pltpu.make_async_remote_copy(
            src_ref=row1, dst_ref=buf1.at[j], send_sem=s1.at[j], recv_sem=r1.at[j], device_id=peer, device_id_type=MESH)
        cp.start()
        copies.append(cp)
    for cp in copies:
        cp.wait()
    zero1 = jnp.zeros((1, 128), jnp.float32)
    part = tree([(row1[...], zero1)] + [(buf1[j], zero1) for j in range(len(group1))], add2)
    row2[0:1, :] = part[0]
    row2[1:2, :] = part[1]
    copies = []
    for j, peer in enumerate(group2):
        cp = pltpu.make_async_remote_copy(
            src_ref=row2, dst_ref=buf2.at[j], send_sem=s2.at[j], recv_sem=r2.at[j], device_id=peer, device_id_type=MESH)
        cp.start()
        copies.append(cp)
    for cp in copies:
        cp.wait()
    part = tree([part] + [(buf2[j, 0:1, :], buf2[j, 1:2, :]) for j in range(len(group2))], add2)

    slot = {}
    for p, (i, j) in enumerate(PAIRS):
        slot[i, j] = slot[j, i] = p
    columns = []
    for k in range(NV):
        at = jnp.full((8, 128), -1, jnp.int32)
        for i in range(NV):
            at = jnp.where(sub == i, slot[i, k], at)
        columns.append(tuple(
            jnp.broadcast_to(
                jnp.sum(jnp.where(lane == at, jnp.broadcast_to(t, (8, 128)), 0.0), axis=1, keepdims=True), (8, 128))
            for t in part))

    def spread(t, k):
        return jnp.broadcast_to(t[k:k + 1, :], (8, 128))

    def times_gram(u):
        return tree([mul2(columns[k], tuple(spread(t, k) for t in u)) for k in range(NV)], add2)

    def dot(a, b):
        return sublane_total(mul2(a, b))

    hmat = jnp.zeros((8, 128), jnp.float32)
    zeros = jnp.zeros((8, 128), jnp.float32)
    u = (jnp.where(sub == 0, -1.0, 0.0), zeros)
    e = times_gram(u)
    coefs, images = [], []
    for j in range(NV):
        square = dot(u, e)[0] + FLOOR
        inv = lax.rsqrt(square)
        if j > 0:
            hmat = jnp.where((sub == j) & (lane == j - 1), square * inv, hmat)
        coefs.append(mul1(u, inv))
        images.append(mul1(e, inv))
        if j == ITERS:
            break
        moved = tuple(pltpu.roll(t, 1, 0) for t in coefs[j])
        u = add2(moved, mul1(coefs[j], jnp.broadcast_to(shift, (8, 128))))
        e = times_gram(u)
        hs_j = [dot(images[i], u)[0] for i in range(j + 1)]
        for i in range(j + 1):
            hmat = jnp.where((sub == i) & (lane == j), hs_j[i], hmat)
        u = tree([u] + [mul1(coefs[i], -hs_j[i]) for i in range(j + 1)], add2)
        e = tree([e] + [mul1(images[i], -hs_j[i]) for i in range(j + 1)], add2)
    hess[...] = hmat[0:NV, 0:ITERS]

    weights = [[jnp.broadcast_to(coefs[j][0][i:i + 1, :], (8, 128)) for i in range(j + 1)] for j in range(NV)]

    for j in range(NV):
        def combine(q, carry, j=j):
            t = tree([weights[j][i] * w[i + 1, q] for i in range(j + 1)], jnp.add)
            vout[j, q] = t[0:4, :]
            return carry

        lax.fori_loop(0, n * n, combine, 0, unroll=8)


def solution(mesh):
    ny, nc, nx, nz = 4, 2, 4, 8
    finer = Mesh(mesh.devices.reshape(ny, nc, nx, nz), AXES)
    gxs, gys = ("y", "c"), ("x", "z")
    sizes = (ny, nc, nx, nz)
    f32 = jnp.float32

    def body(source, initial, reaction, stiffness, line_op, face_deriv, wall_flags):
        nodes, ex, ey = source.shape
        n1, n2 = ny * nc * nx - 1, nz - 1
        hbm = pl.BlockSpec(memory_space=pltpu.HBM)
        scalars = pl.BlockSpec(memory_space=pltpu.SMEM)
        local = pl.BlockSpec(memory_space=pltpu.VMEM)
        vm = pltpu.VMEM
        dma = pltpu.SemaphoreType.DMA
        tile = (8, ey)
        sends = 2 + 8 + 12 + 8
        return pl.pallas_call(
            functools.partial(kernel, sizes),
            out_shape=(
                jax.ShapeDtypeStruct((NV, ITERS), f32),
                jax.ShapeDtypeStruct((NV, nodes, ex, ey), f32),
            ),
            in_specs=[scalars, scalars] + [hbm] * 5,
            out_specs=(local, local),
            scratch_shapes=[
                vm((nodes,) + tile, f32), vm((nodes,) + tile, f32), vm((nodes,) + tile, f32), vm(tile, f32),
                vm((4,) + tile, jnp.int32), vm((4,) + tile, f32),
                vm((NV + 1, nodes) + tile, f32), vm((nodes,) + tile, f32), vm((nodes,) + tile, f32), vm(tile, f32),
                vm((4,) + tile, f32), vm((NV, 8) + tile, f32),
                vm((2, 9) + tile, f32), vm((9,) + tile, f32), vm((9,) + tile, f32),
                vm((2, 2) + tile, f32), vm((2, 2) + tile, f32), vm((2, 2) + tile, f32), vm((1, 2) + tile, f32),
                vm((2, 2) + tile, f32), vm((4, 8) + tile, f32),
                vm((1, 128), f32), vm((n1, 1, 128), f32), vm((2, 128), f32), vm((n2, 2, 128), f32),
                dma((8,)), dma((sends,)), dma((sends,)), dma((n1,)), dma((n1,)), dma((n2,)), dma((n2,)),
            ],
            compiler_params=pltpu.CompilerParams(
                collective_id=0, has_side_effects=True, vmem_limit_bytes=48 * 1024 * 1024),
            name="arnoldi",
        )(line_op, face_deriv, source, initial, reaction, stiffness, wall_flags)

    placed = (P(None, gxs, gys), P(None, gxs, gys), P(None, gxs, gys), P(gxs, gys), P(), P(), P(None, gxs, gys))
    return jax.shard_map(
        body, mesh=finer, in_specs=placed, out_specs=(P(), P(None, None, gxs, gys)), check_vma=False)
```

```python
import functools

import jax
import jax.numpy as jnp
from jax import lax
from jax.experimental import pallas as pl
from jax.experimental.pallas import tpu as pltpu
from jax.sharding import Mesh
from jax.sharding import PartitionSpec as P

P_SIZE = 8
ITERS = 5
NV = ITERS + 1
TAU = 2.0
FLOOR = 0.1
MESH = pl.DeviceIdType.MESH
AXES = ("y", "c", "x", "z")
PAIRS = [(i, j) for j in range(NV) for i in range(j + 1)]


def two_sum(a, b):
    s = a + b
    t = s - a
    return s, (a - (s - t)) + (b - t)


def quick(a, b):
    s = a + b
    return s, b - (s - a)


def split(a):
    c = a * 4097.0
    hi = c - (c - a)
    return hi, a - hi


def two_prod(a, b):
    p = a * b
    ah, al = split(a)
    bh, bl = split(b)
    return p, ((ah * bh - p) + ah * bl + al * bh) + al * bl


def add2(a, b):
    s, e = two_sum(a[0], b[0])
    return quick(s, e + (a[1] + b[1]))


def mul2(a, b):
    p, e = two_prod(a[0], b[0])
    return quick(p, e + (a[0] * b[1] + a[1] * b[0]))


def mul1(a, b):
    p, e = two_prod(a[0], b)
    return quick(p, e + a[1] * b)


def tree(items, op):
    items = list(items)
    while len(items) > 1:
        nxt = [op(items[i], items[i + 1]) for i in range(0, len(items) - 1, 2)]
        if len(items) % 2:
            nxt.append(items[-1])
        items = nxt
    return items[0]


def sublane_total(a):
    for s in (4, 2, 1):
        a = add2(a, tuple(pltpu.roll(v, s, 0) for v in a))
    return a


def kernel(sizes, line_h, fd_h, src_h, x0_h, rx_h, st_h, wf_h, w, cw, hm,
           xl, sl, rl, stl, wfl, opl, x0, sv, rx, st, op, gw, pk, lb, rb, qs, qr, gqs, gql, gqr, qf,
           row1, buf1, row2, buf2, line, fd,
           lsem, hs, hr, s1, r1, s2, r2):
    ny, nc, nx, nz = sizes
    y, c, x, z = (lax.axis_index(a) for a in AXES)

    def at(dx, dy):
        i = lax.rem(y * nc + c + ny * nc + dx, ny * nc)
        j = lax.rem(x * nz + z + nx * nz + dy, nx * nz)
        return (i // nc, lax.rem(i, nc), j // nz, lax.rem(j, nz))

    group1 = [
        (lax.rem(y + i, ny), lax.rem(c + j, nc), lax.rem(x + k, nx), z)
        for i in range(ny) for j in range(nc) for k in range(nx) if i + j + k > 0
    ]
    group2 = [(y, c, x, lax.rem(z + k, nz)) for k in range(1, nz)]
    around = {(i, j): at(i, j) for i in (-1, 0, 1) for j in (-1, 0, 1) if (i, j) != (0, 0)}
    own = pl.ds(0, 4)
    pairs = [(line_h, line), (fd_h, fd), (x0_h, xl.at[:, own, :]), (rx_h, rl.at[:, own, :]), (src_h, sl.at[:, own, :]), (st_h, stl.at[own, :]),
             (wf_h, wfl.at[:, own, :]), (x0_h, x0.at[:, own, :]), (rx_h, rx.at[:, own, :]), (src_h, sv.at[:, own, :])]
    loads = [pltpu.make_async_copy(a, b, lsem.at[i]) for i, (a, b) in enumerate(pairs)]
    for cp in loads:
        cp.start()

    barrier = pltpu.get_barrier_semaphore()
    greeted = list(around.values()) + group1 + group2
    for peer in greeted:
        pl.semaphore_signal(barrier, inc=1, device_id=peer, device_id_type=MESH)
    for cp in loads[:2]:
        cp.wait()
    n = P_SIZE
    total = float(ny * nc * nx * nz * src_h.shape[0] * src_h.shape[1] * src_h.shape[2])
    lop = [[line[i, j] for j in range(n)] for i in range(n)]
    g = [0.5 * fd[i] + (TAU if i == 0 else 0.0) for i in range(n)]
    diag = lop[0][0]
    for i in range(1, n):
        diag = diag + lop[i][i]
    shift = 3.0 + 0.3125 * diag + 0.25 * fd[0]

    lane = lax.broadcasted_iota(jnp.int32, (8, 128), 1)
    sub = lax.broadcasted_iota(jnp.int32, (8, 128), 0)
    group = lane // 16
    slot16 = lax.rem(lane, 16)

    def lroll(t, s):
        s = s % 128
        return t if s == 0 else pltpu.roll(t, s, 1)

    def gather_groups(items, s):
        out = lroll(items[0], s)
        for a in range(1, len(items)):
            out = jnp.where(group == a, lroll(items[a], 16 * a + s), out)
        return out

    cline, cface = [], []
    for k in range(n):
        t = jnp.zeros((8, 128), jnp.float32)
        for a in range(n):
            t = jnp.where(group == a, lop[a][(a - k) % n], t)
        cline.append(t)
        cface.append(jnp.where(group == 0, g[(n - k) % n], jnp.where(group == n - 1, g[k], 0.0)))

    def x_faces(v):
        qw = [tree([g[i] * v(i, b) for i in range(n)], jnp.add) for b in range(n)]
        qe = [tree([g[i] * v(n - 1 - i, b) for i in range(n)], jnp.add) for b in range(n)]
        return qw, qe

    def strip_faces(t):
        rolled = [t] + [lroll(t, 16 * k) for k in range(1, n)]
        return rolled, tree([cface[k] * rolled[k] for k in range(n)], jnp.add)

    for cp in loads[2:7]:
        cp.wait()
    opl[...] = 1.0 - wfl[...].astype(jnp.float32)
    qw, qe = x_faces(lambda a, b: xl[a * n + b])
    for b in range(n):
        qs[0, 0, pl.ds(b, 1), :] = qw[b][2:3, :]
        qs[0, 1, pl.ds(b, 1), :] = qe[b][1:2, :]
    for b in range(n):
        px = gather_groups([xl[a * n + b] for a in range(n)], 6)
        ps = gather_groups([sl[a * n + b] for a in range(n)], 6)
        pr = gather_groups([rl[a * n + b] for a in range(n)], 6)
        pk[0, b] = jnp.where(slot16 < 6, px, jnp.where(slot16 < 11, lroll(ps, 5), lroll(pr, 10)))
        pk[1, b] = jnp.where(slot16 < 6, lroll(px, -6), jnp.where(slot16 < 11, ps, lroll(pr, 5)))
    gqs[0, 0] = lroll(qs[0, 0], 6)
    gqs[0, 1] = lroll(qs[0, 1], 118)
    pst = gather_groups([stl[...]] + [opl[f] for f in range(4)], 6)
    pk[0, n] = pst
    pk[1, n] = pst
    pl.semaphore_wait(barrier, len(greeted))

    def send(copies, peer, pieces, first):
        for i, (a, b) in enumerate(pieces):
            cp = pltpu.make_async_remote_copy(
                src_ref=a, dst_ref=b, send_sem=hs.at[first + i], recv_sem=hr.at[first + i],
                device_id=peer, device_id_type=MESH)
            cp.start()
            copies.append(cp)
        return first + len(pieces)

    def rows(lo):
        return pl.ds(lo, 2)

    copies, used = [], 0
    for dy, k, dst in ((1, 0, lb), (-1, 1, rb)):
        used = send(copies, around[0, dy], [(pk.at[k, :, own, :], dst.at[:, own, :])], used)
    for dy, k, dst, gq in ((1, 0, lb, gql), (-1, 1, rb, gqr)):
        for dx, lo, to in ((1, 2, 6), (-1, 0, 4)):
            side = 1 if dx > 0 else 0
            used = send(copies, around[dx, dy], [
                (pk.at[k, :, rows(lo), :], dst.at[:, rows(to), :]), (gqs.at[0, side], gq.at[0, side])], used)
    for dx, lo, to in ((1, 2, 6), (-1, 0, 4)):
        side = 1 if dx > 0 else 0
        used = send(copies, around[dx, 0], [
            (xl.at[:, rows(lo), :], x0.at[:, rows(to), :]),
            (rl.at[:, rows(lo), :], rx.at[:, rows(to), :]),
            (sl.at[:, rows(lo), :], sv.at[:, rows(to), :]),
            (stl.at[rows(lo), :], st.at[rows(to), :]),
            (opl.at[:, rows(lo), :], op.at[:, rows(to), :]),
            (qs.at[0, side], qr.at[0, side])], used)
    st[0:4, :] = stl[0:4, :]
    op[:, 0:4, :] = opl[:, 0:4, :]
    for cp in loads[7:]:
        cp.wait()
    for cp in copies:
        cp.wait()

    before_half = slot16 < 6
    gsv, grx = [], []
    for b in range(n):
        lo, hi = lb[b], rb[b]
        gw[0, b] = jnp.where(before_half, lo, lroll(hi, 6))
        gsv.append(jnp.where(before_half, lroll(lo, -5), hi))
        grx.append(jnp.where(before_half, lroll(lo, -10), lroll(hi, -5)))
    both = jnp.where(before_half, lb[n], rb[n])
    spreads = []
    for f in range(5):
        t = jnp.where(group == f, both, 0.0)
        for s in (16, 32, 64):
            t = t + lroll(t, s)
        spreads.append(t)
    gst = spreads[0]
    gopw = jnp.where(group == 0, spreads[1], 0.0)
    gope = jnp.where(group == n - 1, spreads[2], 0.0)
    gops, gopn = spreads[3], spreads[4]
    for side in (0, 1):
        gqr[0, side] = jnp.where(before_half, gql[0, side], gqr[0, side])

    def apply(k, last=False, fresh=None):
        wide = k != 2

        def v(a, b):
            return w[k - 1, a * n + b] if k else x0[a * n + b]

        def keep(a, b, t):
            if wide:
                w[k, a * n + b] = t
            else:
                w[k, a * n + b, 0:4, :] = t[0:4, :]

        gv = [gw[k, b] for b in range(n)]
        gqsouth = tree([g[i] * gv[i] for i in range(n)], jnp.add)
        gqnorth = tree([g[i] * gv[n - 1 - i] for i in range(n)], jnp.add)
        qsouth = [tree([g[i] * v(a, i) for i in range(n)], jnp.add) for a in range(n)]
        qnorth = [tree([g[i] * v(a, n - 1 - i) for i in range(n)], jnp.add) for a in range(n)]
        for a in range(n):
            below = jnp.where(lane == 0, lroll(gqnorth, -(16 * a + 5)), lroll(qnorth[a], 1))
            above = jnp.where(lane == 127, lroll(gqsouth, 121 - 16 * a), lroll(qsouth[a], -1))
            qf[2, a] = qsouth[a] - op[2] * below
            qf[3, a] = qnorth[a] - op[3] * above
        if not last:
            mn = gather_groups(qnorth, 7)
            ms = gather_groups(qsouth, 5)
            sterm = gqsouth - gops * jnp.where(slot16 == 6, mn, lroll(gqnorth, 1))
            nterm = gqnorth - gopn * jnp.where(slot16 == 5, ms, lroll(gqsouth, -1))
            for b in range(n):
                rolled, face = strip_faces(gv[b])
                prev = pltpu.roll(lroll(face, 16), 1, 0)
                nxt = pltpu.roll(lroll(face, -16), 7, 0)
                if fresh is not None:
                    prev = jnp.where(sub == 6, jnp.broadcast_to(lroll(gqr[fresh, 1, pl.ds(b, 1), :], 16), (8, 128)), prev)
                    nxt = jnp.where(sub == 5, jnp.broadcast_to(lroll(gqr[fresh, 0, pl.ds(b, 1), :], -16), (8, 128)), nxt)
                acc = tree([cline[i] * rolled[i] for i in range(n)] + [lop[b][i] * gv[i] for i in range(n)], jnp.add)
                t = grx[b] * gv[b] + gst * acc + (face - (gopw * prev + gope * nxt))
                if b == 0:
                    t = t + sterm
                if b == n - 1:
                    t = t + nterm
                t = t - (gsv[b] if k == 0 else shift * gv[b])
                if wide:
                    gw[k + 1, b] = t
                else:
                    gw[k + 1, b, 0:4, :] = t[0:4, :]
        stiff = st[...]
        for b in range(n):
            col = [v(i, b) for i in range(n)]
            qwest = tree([g[i] * col[i] for i in range(n)], jnp.add)
            qeast = tree([g[i] * col[n - 1 - i] for i in range(n)], jnp.add)
            prev = pltpu.roll(qeast, 1, 0)
            nxt = pltpu.roll(qwest, 7, 0)
            if fresh is not None:
                prev = jnp.where(sub == 6, jnp.broadcast_to(qr[fresh, 1, pl.ds(b, 1), :], (8, 128)), prev)
                nxt = jnp.where(sub == 5, jnp.broadcast_to(qr[fresh, 0, pl.ds(b, 1), :], (8, 128)), nxt)
            for a in range(n):
                acc = tree([lop[a][i] * col[i] for i in range(n)] + [lop[b][i] * v(a, i) for i in range(n)], jnp.add)
                if k == 0:
                    t = rx[a * n + b] * col[a] - sv[a * n + b] + stiff * acc
                else:
                    t = (rx[a * n + b] - shift) * col[a] + stiff * acc
                if a == 0:
                    t = t + (qwest - op[0] * prev)
                if a == n - 1:
                    t = t + (qeast - op[1] * nxt)
                if b == 0:
                    t = t + qf[2, a]
                if b == n - 1:
                    t = t + qf[3, a]
                keep(a, b, t)

    apply(0, fresh=0)
    apply(1)
    apply(2)
    qw, qe = x_faces(lambda a, b: w[2, a * n + b, 0:4, :])
    for b in range(n):
        qs[1, 0, pl.ds(b, 1), :] = qw[b][2:3, :]
        qs[1, 1, pl.ds(b, 1), :] = qe[b][1:2, :]
        t = jnp.concatenate([gw[3, b, 0:4, :]] * 2, axis=0)
        face = strip_faces(t)[1]
        gqs[1, 0, pl.ds(b, 1), :] = face[2:3, :]
        gqs[1, 1, pl.ds(b, 1), :] = face[1:2, :]
    copies = []
    for dx, lo, to in ((1, 2, 6), (-1, 0, 4)):
        side = 1 if dx > 0 else 0
        used = send(copies, around[dx, 0], [
            (w.at[2, :, rows(lo), :], w.at[2, :, rows(to), :]),
            (gw.at[3, :, rows(lo), :], gw.at[3, :, rows(to), :]),
            (qs.at[1, side], qr.at[1, side]),
            (gqs.at[1, side], gqr.at[1, side])], used)
    def gram(pairs):
        top = max(j for i, j in pairs) + 1

        def body(q, acc):
            vals = [w[i, q] for i in range(top)]
            return tuple(t + vals[i] * vals[j] for t, (i, j) in zip(acc, pairs))

        return lax.fori_loop(0, n * n, body, tuple(jnp.zeros((8, 128), jnp.float32) for _ in pairs), unroll=2)

    early = [p for p in PAIRS if p[1] < 2]
    first = gram(early)
    for cp in copies:
        cp.wait()
    apply(3, fresh=1)
    apply(4)
    apply(5, last=True)

    acc = first + gram(PAIRS[len(early):])
    line_row = jnp.zeros((8, 128), jnp.float32)
    for base in range(0, len(PAIRS), 8):
        packed = jnp.zeros((8, 128), jnp.float32)
        for i, t in enumerate(acc[base:base + 8]):
            t = jnp.where(sub < 4, t, 0.0)
            t = t + pltpu.roll(t, 4, 0)
            t = t + pltpu.roll(t, 2, 0)
            t = t + pltpu.roll(t, 1, 0)
            packed = jnp.where(sub == i, t, packed)
        packed = jnp.sum(packed, axis=1, keepdims=True) * (1.0 / total)
        line_row = line_row + jnp.where(lane == sub + base, packed, 0.0)
    for s in (4, 2, 1):
        line_row = line_row + pltpu.roll(line_row, s, 0)
    row1[...] = line_row[0:1, :]
    copies = []
    for j, peer in enumerate(group1):
        cp = pltpu.make_async_remote_copy(
            src_ref=row1, dst_ref=buf1.at[j], send_sem=s1.at[j], recv_sem=r1.at[j], device_id=peer, device_id_type=MESH)
        cp.start()
        copies.append(cp)
    for cp in copies:
        cp.wait()
    zero1 = jnp.zeros((1, 128), jnp.float32)
    part = tree([(row1[...], zero1)] + [(buf1[j], zero1) for j in range(len(group1))], add2)
    row2[0:1, :] = part[0]
    row2[1:2, :] = part[1]
    copies = []
    for j, peer in enumerate(group2):
        cp = pltpu.make_async_remote_copy(
            src_ref=row2, dst_ref=buf2.at[j], send_sem=s2.at[j], recv_sem=r2.at[j], device_id=peer, device_id_type=MESH)
        cp.start()
        copies.append(cp)
    for cp in copies:
        cp.wait()
    part = tree([part] + [(buf2[j, 0:1, :], buf2[j, 1:2, :]) for j in range(len(group2))], add2)

    slot = {}
    for p, (i, j) in enumerate(PAIRS):
        slot[i, j] = slot[j, i] = p
    columns = []
    for k in range(NV):
        at = jnp.full((8, 128), -1, jnp.int32)
        for i in range(NV):
            at = jnp.where(sub == i, slot[i, k], at)
        columns.append(tuple(
            jnp.broadcast_to(
                jnp.sum(jnp.where(lane == at, jnp.broadcast_to(t, (8, 128)), 0.0), axis=1, keepdims=True), (8, 128))
            for t in part))

    def spread(t, k):
        return jnp.broadcast_to(t[k:k + 1, :], (8, 128))

    def times_gram(u):
        return tree([mul2(columns[k], tuple(spread(t, k) for t in u)) for k in range(NV)], add2)

    def dot(a, b):
        return sublane_total(mul2(a, b))

    hmat = jnp.zeros((8, 128), jnp.float32)
    zeros = jnp.zeros((8, 128), jnp.float32)
    u = (jnp.where(sub == 0, -1.0, 0.0), zeros)
    e = times_gram(u)
    coefs, images = [], []
    for j in range(NV):
        square = dot(u, e)[0] + FLOOR
        inv = lax.rsqrt(square)
        if j > 0:
            hmat = jnp.where((sub == j) & (lane == j - 1), square * inv, hmat)
        coefs.append(mul1(u, inv))
        images.append(mul1(e, inv))
        if j == ITERS:
            break
        moved = tuple(pltpu.roll(t, 1, 0) for t in coefs[j])
        u = add2(moved, mul1(coefs[j], jnp.broadcast_to(shift, (8, 128))))
        e = times_gram(u)
        hs_j = [dot(images[i], u)[0] for i in range(j + 1)]
        for i in range(j + 1):
            hmat = jnp.where((sub == i) & (lane == j), hs_j[i], hmat)
        u = tree([u] + [mul1(coefs[i], -hs_j[i]) for i in range(j + 1)], add2)
        e = tree([e] + [mul1(images[i], -hs_j[i]) for i in range(j + 1)], add2)
    hm[...] = hmat
    for j in range(NV):
        cw[j] = coefs[j][0]


def output_kernel(w, cw, hm, hess_h, out_h, hess, vout, sem):
    nodes = w.shape[1]
    hess[...] = hm[0:NV, 0:ITERS]
    outs = [pltpu.make_async_copy(hess, hess_h, sem.at[0])]
    outs[0].start()
    for j in range(NV):
        weights = [jnp.broadcast_to(cw[j, pl.ds(i, 1), :], (8, 128)) for i in range(j + 1)]

        def combine(q, carry):
            t = tree([weights[i] * w[i, q] for i in range(j + 1)], jnp.add)
            vout[j, q] = t[0:4, :]
            return carry

        lax.fori_loop(0, nodes, combine, 0, unroll=8)
        cp = pltpu.make_async_copy(vout.at[j], out_h.at[j], sem.at[j + 1])
        cp.start()
        outs.append(cp)
    for cp in outs:
        cp.wait()


def solution(mesh):
    ny, nc, nx, nz = 4, 2, 4, 8
    finer = Mesh(mesh.devices.reshape(ny, nc, nx, nz), AXES)
    gxs, gys = ("y", "c"), ("x", "z")
    sizes = (ny, nc, nx, nz)
    f32 = jnp.float32

    def body(source, initial, reaction, stiffness, line_op, face_deriv, wall_flags):
        nodes, ex, ey = source.shape
        n1, n2 = ny * nc * nx - 1, nz - 1
        hbm = pl.BlockSpec(memory_space=pltpu.HBM)
        scalars = pl.BlockSpec(memory_space=pltpu.SMEM)
        local = pl.BlockSpec(memory_space=pltpu.VMEM)
        vm = pltpu.VMEM
        dma = pltpu.SemaphoreType.DMA
        tile = (8, ey)
        sends = 2 + 8 + 12 + 8
        w, cw, hm = pl.pallas_call(
            functools.partial(kernel, sizes),
            out_shape=(
                pltpu.VMEM((NV, nodes) + tile, f32), pltpu.VMEM((NV,) + tile, f32), pltpu.VMEM(tile, f32),
            ),
            in_specs=[hbm] * 7,
            out_specs=(local, local, local),
            scratch_shapes=[
                vm((nodes,) + tile, f32), vm((nodes,) + tile, f32), vm((nodes,) + tile, f32), vm(tile, f32),
                vm((4,) + tile, jnp.int32), vm((4,) + tile, f32),
                vm((nodes,) + tile, f32), vm((nodes,) + tile, f32), vm((nodes,) + tile, f32), vm(tile, f32),
                vm((4,) + tile, f32), vm((NV, 8) + tile, f32),
                vm((2, 9) + tile, f32), vm((9,) + tile, f32), vm((9,) + tile, f32),
                vm((2, 2) + tile, f32), vm((2, 2) + tile, f32), vm((2, 2) + tile, f32), vm((1, 2) + tile, f32),
                vm((2, 2) + tile, f32), vm((4, 8) + tile, f32),
                vm((1, 128), f32), vm((n1, 1, 128), f32), vm((2, 128), f32), vm((n2, 2, 128), f32),
                pltpu.SMEM((P_SIZE, P_SIZE), f32), pltpu.SMEM((P_SIZE,), f32),
                dma((10,)), dma((sends,)), dma((sends,)), dma((n1,)), dma((n1,)), dma((n2,)), dma((n2,)),
            ],
            compiler_params=pltpu.CompilerParams(
                collective_id=0, has_side_effects=True, vmem_limit_bytes=48 * 1024 * 1024),
            name="arnoldi",
        )(*[pltpu.with_memory_space_constraint(t, pltpu.HBM) for t in (
            line_op, face_deriv, source, initial, reaction, stiffness, wall_flags)])
        return pl.pallas_call(
            output_kernel,
            out_shape=(
                jax.ShapeDtypeStruct((NV, ITERS), f32),
                jax.ShapeDtypeStruct((NV, nodes, ex, ey), f32),
            ),
            in_specs=[local] * 3,
            out_specs=(hbm, hbm),
            scratch_shapes=[vm((NV, ITERS), f32), vm((NV, nodes, ex, ey), f32), dma((NV + 1,))],
            compiler_params=pltpu.CompilerParams(vmem_limit_bytes=16 * 1024 * 1024),
            name="combine",
        )(w, cw, hm)

    placed = (P(None, gxs, gys), P(None, gxs, gys), P(None, gxs, gys), P(gxs, gys), P(), P(), P(None, gxs, gys))
    return jax.shard_map(
        body, mesh=finer, in_specs=placed, out_specs=(P(), P(None, None, gxs, gys)), check_vma=False)
```

```python
import functools

import jax
import jax.numpy as jnp
from jax import lax
from jax.experimental import pallas as pl
from jax.experimental.pallas import tpu as pltpu
from jax.sharding import Mesh
from jax.sharding import PartitionSpec as P

P_SIZE = 8
ITERS = 5
NV = ITERS + 1
TAU = 2.0
FLOOR = 0.1
MESH = pl.DeviceIdType.MESH
AXES = ("y", "c", "x", "z")
PAIRS = [(i, j) for j in range(NV) for i in range(j + 1)]


def two_sum(a, b):
    s = a + b
    t = s - a
    return s, (a - (s - t)) + (b - t)


def split(a):
    c = a * 4097.0
    hi = c - (c - a)
    return hi, a - hi


def two_prod(a, b):
    p = a * b
    ah, al = split(a)
    bh, bl = split(b)
    return p, ((ah * bh - p) + ah * bl + al * bh) + al * bl


def add2(a, b):
    s, e = two_sum(a[0], b[0])
    return s, e + (a[1] + b[1])


def mul2(a, b):
    p, e = two_prod(a[0], b[0])
    return p, e + (a[0] * b[1] + a[1] * b[0])


def mul1(a, b):
    p, e = two_prod(a[0], b)
    return p, e + a[1] * b


def tidy(a):
    return two_sum(*a)


def tree(items, op):
    items = list(items)
    while len(items) > 1:
        nxt = [op(items[i], items[i + 1]) for i in range(0, len(items) - 1, 2)]
        if len(items) % 2:
            nxt.append(items[-1])
        items = nxt
    return items[0]


def sublane_total(a):
    for s in (4, 2, 1):
        a = add2(a, tuple(pltpu.roll(v, s, 0) for v in a))
    return tidy(a)


def kernel(sizes, line_h, fd_h, src_h, x0_h, rx_h, st_h, wf_h, wp, cw, hm,
           xl, sl, rl, stl, wfl, opl, w, x0, sv, rx, st, op, gw, pk, lb, rb, qs, qr, gqs, gql, gqr, qf,
           row1, buf1, row2, buf2, line, fd,
           lsem, hs, hr, s1, r1, s2, r2):
    ny, nc, nx, nz = sizes
    y, c, x, z = (lax.axis_index(a) for a in AXES)

    def at(dx, dy):
        i = lax.rem(y * nc + c + ny * nc + dx, ny * nc)
        j = lax.rem(x * nz + z + nx * nz + dy, nx * nz)
        return (i // nc, lax.rem(i, nc), j // nz, lax.rem(j, nz))

    hub = c == nc - 1
    plane = [(lax.rem(y + i, ny), lax.rem(x + k, nx)) for i in range(ny) for k in range(nx)]
    planes = [lax.rem(z + k, nz) for k in range(1, nz)]
    me = (c * ny + y) * nx + x
    around = {(i, j): at(i, j) for i in (-1, 0, 1) for j in (-1, 0, 1) if (i, j) != (0, 0)}
    own = pl.ds(0, 4)
    pairs = [(line_h, line), (fd_h, fd), (x0_h, xl.at[:, own, :]), (rx_h, rl.at[:, own, :]), (src_h, sl.at[:, own, :]), (st_h, stl.at[own, :]),
             (wf_h, wfl.at[:, own, :]), (x0_h, x0.at[:, own, :]), (rx_h, rx.at[:, own, :]), (src_h, sv.at[:, own, :])]
    loads = [pltpu.make_async_copy(a, b, lsem.at[i]) for i, (a, b) in enumerate(pairs)]
    for cp in loads:
        cp.start()

    barrier = pltpu.get_barrier_semaphore()
    def greet(peer):
        pl.semaphore_signal(barrier, inc=1, device_id=peer, device_id_type=MESH)

    for peer in around.values():
        greet(peer)
    for i, (yy, xx) in enumerate(plane):
        greet((yy, nc - 1, xx, z) if i else (y, nc - 1 - c, x, z))
    for zz in planes:
        greet((y, nc - 1, x, zz))

    @pl.when(hub)
    def _():
        for yy, xx in plane[1:]:
            greet((yy, 0, xx, z))
        for zz in planes:
            greet((y, 0, x, zz))

    for cp in loads[:2]:
        cp.wait()
    n = P_SIZE
    total = float(ny * nc * nx * nz * src_h.shape[0] * src_h.shape[1] * src_h.shape[2])
    lop = [[line[i, j] for j in range(n)] for i in range(n)]
    g = [0.5 * fd[i] + (TAU if i == 0 else 0.0) for i in range(n)]
    diag = lop[0][0]
    for i in range(1, n):
        diag = diag + lop[i][i]
    shift = 3.0 + 0.3125 * diag + 0.25 * fd[0]

    lane = lax.broadcasted_iota(jnp.int32, (8, 128), 1)
    sub = lax.broadcasted_iota(jnp.int32, (8, 128), 0)
    group = lane // 16
    slot16 = lax.rem(lane, 16)

    def lroll(t, s):
        s = s % 128
        return t if s == 0 else pltpu.roll(t, s, 1)

    def gather_groups(items, s):
        out = lroll(items[0], s)
        for a in range(1, len(items)):
            out = jnp.where(group == a, lroll(items[a], 16 * a + s), out)
        return out

    cline, cface = [], []
    for k in range(n):
        t = jnp.zeros((8, 128), jnp.float32)
        for a in range(n):
            t = jnp.where(group == a, lop[a][(a - k) % n], t)
        cline.append(t)
        cface.append(jnp.where(group == 0, g[(n - k) % n], jnp.where(group == n - 1, g[k], 0.0)))

    def x_faces(v):
        qw = [tree([g[i] * v(i, b) for i in range(n)], jnp.add) for b in range(n)]
        qe = [tree([g[i] * v(n - 1 - i, b) for i in range(n)], jnp.add) for b in range(n)]
        return qw, qe

    def strip_faces(t):
        rolled = [t] + [lroll(t, 16 * k) for k in range(1, n)]
        return rolled, tree([cface[k] * rolled[k] for k in range(n)], jnp.add)

    for cp in loads[2:7]:
        cp.wait()
    opl[...] = 1.0 - wfl[...].astype(jnp.float32)
    qw, qe = x_faces(lambda a, b: xl[a * n + b])
    for b in range(n):
        qs[0, 0, pl.ds(b, 1), :] = qw[b][2:3, :]
        qs[0, 1, pl.ds(b, 1), :] = qe[b][1:2, :]
    for b in range(n):
        px = gather_groups([xl[a * n + b] for a in range(n)], 6)
        ps = gather_groups([sl[a * n + b] for a in range(n)], 6)
        pr = gather_groups([rl[a * n + b] for a in range(n)], 6)
        pk[0, b] = jnp.where(slot16 < 6, px, jnp.where(slot16 < 11, lroll(ps, 5), lroll(pr, 10)))
        pk[1, b] = jnp.where(slot16 < 6, lroll(px, -6), jnp.where(slot16 < 11, ps, lroll(pr, 5)))
    gqs[0, 0] = lroll(qs[0, 0], 6)
    gqs[0, 1] = lroll(qs[0, 1], 118)
    pst = gather_groups([stl[...]] + [opl[f] for f in range(4)], 6)
    pk[0, n] = pst
    pk[1, n] = pst
    @pl.when(hub)
    def _():
        pl.semaphore_wait(barrier, 8 + 31 + 14)

    @pl.when(jnp.logical_not(hub))
    def _():
        pl.semaphore_wait(barrier, 8 + 16 + 7)


    def send(copies, peer, pieces, first):
        for i, (a, b) in enumerate(pieces):
            cp = pltpu.make_async_remote_copy(
                src_ref=a, dst_ref=b, send_sem=hs.at[first + i], recv_sem=hr.at[first + i],
                device_id=peer, device_id_type=MESH)
            cp.start()
            copies.append(cp)
        return first + len(pieces)

    def rows(lo):
        return pl.ds(lo, 2)

    copies, used = [], 0
    for dy, k, dst in ((1, 0, lb), (-1, 1, rb)):
        used = send(copies, around[0, dy], [(pk.at[k, :, own, :], dst.at[:, own, :])], used)
    for dy, k, dst, gq in ((1, 0, lb, gql), (-1, 1, rb, gqr)):
        for dx, lo, to in ((1, 2, 6), (-1, 0, 4)):
            side = 1 if dx > 0 else 0
            used = send(copies, around[dx, dy], [
                (pk.at[k, :, rows(lo), :], dst.at[:, rows(to), :]), (gqs.at[0, side], gq.at[0, side])], used)
    for dx, lo, to in ((1, 2, 6), (-1, 0, 4)):
        side = 1 if dx > 0 else 0
        used = send(copies, around[dx, 0], [
            (xl.at[:, rows(lo), :], x0.at[:, rows(to), :]),
            (rl.at[:, rows(lo), :], rx.at[:, rows(to), :]),
            (sl.at[:, rows(lo), :], sv.at[:, rows(to), :]),
            (stl.at[rows(lo), :], st.at[rows(to), :]),
            (opl.at[:, rows(lo), :], op.at[:, rows(to), :]),
            (qs.at[0, side], qr.at[0, side])], used)
    st[0:4, :] = stl[0:4, :]
    op[:, 0:4, :] = opl[:, 0:4, :]
    for cp in loads[7:]:
        cp.wait()
    for cp in copies:
        cp.wait()

    before_half = slot16 < 6
    gsv, grx = [], []
    for b in range(n):
        lo, hi = lb[b], rb[b]
        gw[0, b] = jnp.where(before_half, lo, lroll(hi, 6))
        gsv.append(jnp.where(before_half, lroll(lo, -5), hi))
        grx.append(jnp.where(before_half, lroll(lo, -10), lroll(hi, -5)))
    both = jnp.where(before_half, lb[n], rb[n])
    spreads = []
    for f in range(5):
        t = jnp.where(group == f, both, 0.0)
        for s in (16, 32, 64):
            t = t + lroll(t, s)
        spreads.append(t)
    gst = spreads[0]
    gopw = jnp.where(group == 0, spreads[1], 0.0)
    gope = jnp.where(group == n - 1, spreads[2], 0.0)
    gops, gopn = spreads[3], spreads[4]
    for side in (0, 1):
        gqr[0, side] = jnp.where(before_half, gql[0, side], gqr[0, side])

    def apply(k, last=False, fresh=None, after_strip=None, after_half=None):
        wide = k != 2

        def v(a, b):
            return w[k - 1, a * n + b] if k else x0[a * n + b]

        gv = [gw[k, b] for b in range(n)]
        gqsouth = tree([g[i] * gv[i] for i in range(n)], jnp.add)
        gqnorth = tree([g[i] * gv[n - 1 - i] for i in range(n)], jnp.add)
        qsouth = [tree([g[i] * v(a, i) for i in range(n)], jnp.add) for a in range(n)]
        qnorth = [tree([g[i] * v(a, n - 1 - i) for i in range(n)], jnp.add) for a in range(n)]
        for a in range(n):
            below = jnp.where(lane == 0, lroll(gqnorth, -(16 * a + 5)), lroll(qnorth[a], 1))
            above = jnp.where(lane == 127, lroll(gqsouth, 121 - 16 * a), lroll(qsouth[a], -1))
            qf[2, a] = qsouth[a] - op[2] * below
            qf[3, a] = qnorth[a] - op[3] * above
        if not last:
            mn = gather_groups(qnorth, 7)
            ms = gather_groups(qsouth, 5)
            sterm = gqsouth - gops * jnp.where(slot16 == 6, mn, lroll(gqnorth, 1))
            nterm = gqnorth - gopn * jnp.where(slot16 == 5, ms, lroll(gqsouth, -1))
            for b in range(n):
                rolled, face = strip_faces(gv[b])
                prev = pltpu.roll(lroll(face, 16), 1, 0)
                nxt = pltpu.roll(lroll(face, -16), 7, 0)
                if fresh is not None:
                    prev = jnp.where(sub == 6, jnp.broadcast_to(lroll(gqr[fresh, 1, pl.ds(b, 1), :], 16), (8, 128)), prev)
                    nxt = jnp.where(sub == 5, jnp.broadcast_to(lroll(gqr[fresh, 0, pl.ds(b, 1), :], -16), (8, 128)), nxt)
                acc = tree([cline[i] * rolled[i] for i in range(n)] + [lop[b][i] * gv[i] for i in range(n)], jnp.add)
                t = grx[b] * gv[b] + gst * acc + (face - (gopw * prev + gope * nxt))
                if b == 0:
                    t = t + sterm
                if b == n - 1:
                    t = t + nterm
                t = t - (gsv[b] if k == 0 else shift * gv[b])
                if wide:
                    gw[k + 1, b] = t
                else:
                    gw[k + 1, b, 0:4, :] = t[0:4, :]
            if after_strip is not None:
                after_strip()
        for b in range(n):
            qwest = tree([g[i] * v(i, b) for i in range(n)], jnp.add)
            qeast = tree([g[i] * v(n - 1 - i, b) for i in range(n)], jnp.add)
            prev = pltpu.roll(qeast, 1, 0)
            nxt = pltpu.roll(qwest, 7, 0)
            if fresh is not None:
                prev = jnp.where(sub == 6, jnp.broadcast_to(qr[fresh, 1, pl.ds(b, 1), :], (8, 128)), prev)
                nxt = jnp.where(sub == 5, jnp.broadcast_to(qr[fresh, 0, pl.ds(b, 1), :], (8, 128)), nxt)
            qf[0, b] = qwest - op[0] * prev
            qf[1, b] = qeast - op[1] * nxt
        stiff = st[...]
        for a in range(n):
            row = [v(a, i) for i in range(n)]
            even = None
            for b in range(n):
                acc = tree([lop[b][i] * row[i] for i in range(n)] + [lop[a][i] * v(i, b) for i in range(n)], jnp.add)
                if k == 0:
                    t = rx[a * n + b] * row[b] - sv[a * n + b] + stiff * acc
                else:
                    t = (rx[a * n + b] - shift) * row[b] + stiff * acc
                if a == 0:
                    t = t + qf[0, b]
                if a == n - 1:
                    t = t + qf[1, b]
                if b == 0:
                    t = t + qf[2, a]
                if b == n - 1:
                    t = t + qf[3, a]
                if k == 2:
                    w[k, a * n + b, 0:4, :] = t[0:4, :]
                elif not last:
                    w[k, a * n + b] = t
                if b % 2 == 0:
                    even = t
                else:
                    wp[k, (a * n + b) // 2] = jnp.where(sub < 4, even, pltpu.roll(t, 4, 0))
            if a == 3 and after_half is not None:
                after_half()

    apply(0, fresh=0)
    apply(1)
    copies = []
    sides = ((1, 2, 6), (-1, 0, 4))

    def send_strip():
        nonlocal used
        for b in range(n):
            t = jnp.concatenate([gw[3, b, 0:4, :]] * 2, axis=0)
            face = strip_faces(t)[1]
            gqs[1, 0, pl.ds(b, 1), :] = face[2:3, :]
            gqs[1, 1, pl.ds(b, 1), :] = face[1:2, :]
        for dx, lo, to in sides:
            side = 1 if dx > 0 else 0
            used = send(copies, around[dx, 0], [
                (gw.at[3, :, rows(lo), :], gw.at[3, :, rows(to), :]), (gqs.at[1, side], gqr.at[1, side])], used)

    def send_block(first):
        nonlocal used
        part = pl.ds(first, n * n // 2)
        for dx, lo, to in sides:
            used = send(copies, around[dx, 0], [(w.at[2, part, rows(lo), :], w.at[2, part, rows(to), :])], used)

    apply(2, after_strip=send_strip, after_half=lambda: send_block(0))
    send_block(n * n // 2)
    qw, qe = x_faces(lambda a, b: w[2, a * n + b, 0:4, :])
    for b in range(n):
        qs[1, 0, pl.ds(b, 1), :] = qw[b][2:3, :]
        qs[1, 1, pl.ds(b, 1), :] = qe[b][1:2, :]
    for dx, lo, to in sides:
        side = 1 if dx > 0 else 0
        used = send(copies, around[dx, 0], [(qs.at[1, side], qr.at[1, side])], used)
    def gram(pairs):
        top = max(j for i, j in pairs) + 1

        def body(q, acc):
            vals = [wp[i, q] for i in range(top)]
            return tuple(t + vals[i] * vals[j] for t, (i, j) in zip(acc, pairs))

        return lax.fori_loop(0, n * n // 2, body, tuple(jnp.zeros((8, 128), jnp.float32) for _ in pairs), unroll=8)

    early = [p for p in PAIRS if p[1] < 3]
    first = gram(early)
    for cp in copies:
        cp.wait()
    apply(3, fresh=1)
    apply(4)
    apply(5, last=True)

    acc = first + gram(PAIRS[len(early):])
    line_row = jnp.zeros((8, 128), jnp.float32)
    for base in range(0, len(PAIRS), 8):
        packed = jnp.zeros((8, 128), jnp.float32)
        for i, t in enumerate(acc[base:base + 8]):
            t = t + pltpu.roll(t, 4, 0)
            t = t + pltpu.roll(t, 2, 0)
            t = t + pltpu.roll(t, 1, 0)
            packed = jnp.where(sub == i, t, packed)
        packed = jnp.sum(packed, axis=1, keepdims=True) * (1.0 / total)
        line_row = line_row + jnp.where(lane == sub + base, packed, 0.0)
    for s in (4, 2, 1):
        line_row = line_row + pltpu.roll(line_row, s, 0)
    zero1 = jnp.zeros((1, 128), jnp.float32)
    row1[...] = line_row[0:1, :]

    def to_hub(j, index, peer):
        return pltpu.make_async_remote_copy(
            src_ref=row1, dst_ref=buf1.at[index], send_sem=s1.at[j], recv_sem=r1.at[index],
            device_id=peer, device_id_type=MESH)

    def across(j, index, peer):
        return pltpu.make_async_remote_copy(
            src_ref=row2, dst_ref=buf2.at[index], send_sem=s2.at[j], recv_sem=r2.at[index],
            device_id=peer, device_id_type=MESH)

    partner = (y, nc - 1 - c, x, z)
    for j, (yy, xx) in enumerate(plane):
        if j:
            to_hub(j, me, (yy, nc - 1, xx, z)).start()

    @pl.when(hub)
    def _():
        buf1[me] = row1[...]
        for j, (yy, xx) in enumerate(plane):
            for cc in range(nc):
                if j or cc != nc - 1:
                    to_hub(j, (cc * ny + yy) * nx + xx, partner).wait_recv()
        total1 = tree([(buf1[j], zero1) for j in range(nc * ny * nx)], add2)
        total1 = tidy(total1)
        row2[0:1, :] = total1[0]
        row2[1:2, :] = total1[1]
        k = 0
        for zz in planes:
            for cc in (nc - 1, 0):
                across(k, z, (y, cc, x, zz)).start()
                k += 1
        across(k, z, partner).start()
        buf2[z] = row2[...]

    @pl.when(jnp.logical_not(hub))
    def _():
        to_hub(0, me, partner).start()
        across(0, z, partner).wait_recv()
        to_hub(0, me, partner).wait_send()

    for zz in planes:
        across(0, zz, partner).wait_recv()
    for j in range(1, len(plane)):
        to_hub(j, me, partner).wait_send()

    @pl.when(hub)
    def _():
        for k in range(2 * len(planes) + 1):
            across(k, z, partner).wait_send()

    part = tidy(tree([(buf2[j, 0:1, :], buf2[j, 1:2, :]) for j in range(nz)], add2))

    slot = {}
    for p, (i, j) in enumerate(PAIRS):
        slot[i, j] = slot[j, i] = p
    columns = []
    for k in range(NV):
        at = jnp.full((8, 128), -1, jnp.int32)
        for i in range(NV):
            at = jnp.where(sub == i, slot[i, k], at)
        columns.append(tuple(
            jnp.broadcast_to(
                jnp.sum(jnp.where(lane == at, jnp.broadcast_to(t, (8, 128)), 0.0), axis=1, keepdims=True), (8, 128))
            for t in part))

    def spread(t, k):
        return jnp.broadcast_to(t[k:k + 1, :], (8, 128))

    def dot(a, b):
        return sublane_total(mul2(a, b))

    wide_shift = jnp.broadcast_to(shift, (8, 128))
    moved = [add2(columns[k + 1], mul1(columns[k], wide_shift)) for k in range(ITERS)]
    moved = [tidy(t) for t in moved]
    hmat = jnp.zeros((8, 128), jnp.float32)
    zeros = jnp.zeros((8, 128), jnp.float32)
    u = (jnp.where(sub == 0, -1.0, 0.0), zeros)
    e = tuple(-t for t in columns[0])
    ratio = None
    coefs, images = [], []
    for j in range(NV):
        square = dot(u, e)[0]
        square = (square if ratio is None else square * (ratio * ratio)) + FLOOR
        inv = lax.rsqrt(square)
        if j > 0:
            hmat = jnp.where((sub == j) & (lane == j - 1), square * inv, hmat)
        unit = inv if ratio is None else inv * ratio
        coefs.append(tidy(mul1(u, unit)))
        if j == ITERS:
            break
        images.append(tidy(mul1(e, unit)))
        m = tidy(add2(tuple(pltpu.roll(t, 1, 0) for t in u), mul1(u, wide_shift)))
        f = tree([mul2(moved[k], tuple(spread(t, k) for t in u)) for k in range(j + 1)], add2)
        parts = [dot(images[i], m)[0] for i in range(j)]
        own = dot(e, m)[0] * (unit * unit)
        for i in range(j):
            hmat = jnp.where((sub == i) & (lane == j), parts[i] * unit, hmat)
        hmat = jnp.where((sub == j) & (lane == j), own, hmat)
        u, e = (
            tidy(tree([x] + [mul1(basis[i], -parts[i]) for i in range(j)] + [mul1(latest, -own)], add2))
            for x, basis, latest in ((m, coefs, u), (f, images, e)))
        ratio = unit
    hm[...] = hmat
    for j in range(NV):
        cw[j] = coefs[j][0]


def output_kernel(w, cw, hm, hess_h, out_h, hess, vout, sem):
    half = w.shape[1]
    hess[...] = hm[0:NV, 0:ITERS]
    outs = [pltpu.make_async_copy(hess, hess_h, sem.at[0])]
    outs[0].start()
    for j in range(NV):
        weights = [jnp.broadcast_to(cw[j, pl.ds(i, 1), :], (8, 128)) for i in range(j + 1)]

        def combine(q, carry):
            t = tree([weights[i] * w[i, q] for i in range(j + 1)], jnp.add)
            vout[j, 2 * q] = t[0:4, :]
            vout[j, 2 * q + 1] = t[4:8, :]
            return carry

        lax.fori_loop(0, half, combine, 0, unroll=8)
        cp = pltpu.make_async_copy(vout.at[j], out_h.at[j], sem.at[j + 1])
        cp.start()
        outs.append(cp)
    for cp in outs:
        cp.wait()


def solution(mesh):
    ny, nc, nx, nz = 4, 2, 4, 8
    finer = Mesh(mesh.devices.reshape(ny, nc, nx, nz), AXES)
    gxs, gys = ("y", "c"), ("x", "z")
    sizes = (ny, nc, nx, nz)
    f32 = jnp.float32

    def body(source, initial, reaction, stiffness, line_op, face_deriv, wall_flags):
        nodes, ex, ey = source.shape
        hbm = pl.BlockSpec(memory_space=pltpu.HBM)
        scalars = pl.BlockSpec(memory_space=pltpu.SMEM)
        local = pl.BlockSpec(memory_space=pltpu.VMEM)
        vm = pltpu.VMEM
        dma = pltpu.SemaphoreType.DMA
        tile = (8, ey)
        sends = 2 + 8 + 12 + 10
        w, cw, hm = pl.pallas_call(
            functools.partial(kernel, sizes),
            out_shape=(
                pltpu.VMEM((NV, nodes // 2) + tile, f32), pltpu.VMEM((NV,) + tile, f32), pltpu.VMEM(tile, f32),
            ),
            in_specs=[hbm] * 7,
            out_specs=(local, local, local),
            scratch_shapes=[
                vm((nodes,) + tile, f32), vm((nodes,) + tile, f32), vm((nodes,) + tile, f32), vm(tile, f32),
                vm((4,) + tile, jnp.int32), vm((4,) + tile, f32),
                vm((NV - 1, nodes) + tile, f32), vm((nodes,) + tile, f32), vm((nodes,) + tile, f32), vm((nodes,) + tile, f32),
                vm(tile, f32), vm((4,) + tile, f32), vm((NV, 8) + tile, f32),
                vm((2, 9) + tile, f32), vm((9,) + tile, f32), vm((9,) + tile, f32),
                vm((2, 2) + tile, f32), vm((2, 2) + tile, f32), vm((2, 2) + tile, f32), vm((1, 2) + tile, f32),
                vm((2, 2) + tile, f32), vm((4, 8) + tile, f32),
                vm((1, 128), f32), vm((nc * ny * nx, 1, 128), f32), vm((2, 128), f32), vm((nz, 2, 128), f32),
                pltpu.SMEM((P_SIZE, P_SIZE), f32), pltpu.SMEM((P_SIZE,), f32),
                dma((10,)), dma((sends,)), dma((sends,)), dma((ny * nx,)), dma((nc * ny * nx,)), dma((2 * nz - 1,)), dma((nz,)),
            ],
            compiler_params=pltpu.CompilerParams(
                collective_id=0, has_side_effects=True, vmem_limit_bytes=48 * 1024 * 1024),
            name="arnoldi",
        )(*[pltpu.with_memory_space_constraint(t, pltpu.HBM) for t in (
            line_op, face_deriv, source, initial, reaction, stiffness, wall_flags)])
        return pl.pallas_call(
            output_kernel,
            out_shape=(
                jax.ShapeDtypeStruct((NV, ITERS), f32),
                jax.ShapeDtypeStruct((NV, nodes, ex, ey), f32),
            ),
            in_specs=[local] * 3,
            out_specs=(hbm, hbm),
            scratch_shapes=[vm((NV, ITERS), f32), vm((NV, nodes, ex, ey), f32), dma((NV + 1,))],
            compiler_params=pltpu.CompilerParams(vmem_limit_bytes=16 * 1024 * 1024),
            name="combine",
        )(w, cw, hm)

    placed = (P(None, gxs, gys), P(None, gxs, gys), P(None, gxs, gys), P(gxs, gys), P(), P(), P(None, gxs, gys))
    return jax.shard_map(
        body, mesh=finer, in_specs=placed, out_specs=(P(), P(None, None, gxs, gys)), check_vma=False)
```

```python
import functools

import jax
import jax.numpy as jnp
from jax import lax
from jax.experimental import pallas as pl
from jax.experimental.pallas import tpu as pltpu
from jax.sharding import Mesh
from jax.sharding import PartitionSpec as P

P_SIZE = 8
ITERS = 5
NV = ITERS + 1
TAU = 2.0
FLOOR = 0.1
MESH = pl.DeviceIdType.MESH
AXES = ("y", "c", "x", "z")
PAIRS = [(i, j) for j in range(NV) for i in range(j + 1)]


def two_sum(a, b):
    s = a + b
    t = s - a
    return s, (a - (s - t)) + (b - t)


def split(a):
    c = a * 4097.0
    hi = c - (c - a)
    return hi, a - hi


def two_prod(a, b):
    p = a * b
    ah, al = split(a)
    bh, bl = split(b)
    return p, ((ah * bh - p) + ah * bl + al * bh) + al * bl


def add2(a, b):
    s, e = two_sum(a[0], b[0])
    return s, e + (a[1] + b[1])


def mul2(a, b):
    p, e = two_prod(a[0], b[0])
    return p, e + (a[0] * b[1] + a[1] * b[0])


def mul1(a, b):
    p, e = two_prod(a[0], b)
    return p, e + a[1] * b


def tidy(a):
    return two_sum(*a)


def tree(items, op):
    items = list(items)
    while len(items) > 1:
        nxt = [op(items[i], items[i + 1]) for i in range(0, len(items) - 1, 2)]
        if len(items) % 2:
            nxt.append(items[-1])
        items = nxt
    return items[0]


def sublane_total(a):
    for s in (4, 2, 1):
        a = add2(a, tuple(pltpu.roll(v, s, 0) for v in a))
    return tidy(a)


def kernel(sizes, line_h, fd_h, src_h, x0_h, rx_h, st_h, wf_h, wp, cw, hm,
           xl, sl, rl, stl, wfl, opl, w, x0, sv, rx, st, op, gw, pk, lb, rb, qs, qr, gqs, gql, gqr, qf,
           row1, buf1, row2, buf2, line, fd, rxp, cpair,
           lsem, hs, hr, s1, r1, s2, r2):
    ny, nc, nx, nz = sizes
    y, c, x, z = (lax.axis_index(a) for a in AXES)

    def at(dx, dy):
        i = lax.rem(y * nc + c + ny * nc + dx, ny * nc)
        j = lax.rem(x * nz + z + nx * nz + dy, nx * nz)
        return (i // nc, lax.rem(i, nc), j // nz, lax.rem(j, nz))

    hub = c == nc - 1
    plane = [(lax.rem(y + i, ny), lax.rem(x + k, nx)) for i in range(ny) for k in range(nx)]
    planes = [lax.rem(z + k, nz) for k in range(1, nz)]
    me = (c * ny + y) * nx + x
    around = {(i, j): at(i, j) for i in (-1, 0, 1) for j in (-1, 0, 1) if (i, j) != (0, 0)}
    own = pl.ds(0, 4)
    pairs = [(line_h, line), (fd_h, fd), (x0_h, xl.at[:, own, :]), (rx_h, rl.at[:, own, :]), (src_h, sl.at[:, own, :]), (st_h, stl.at[own, :]),
             (wf_h, wfl.at[:, own, :]), (x0_h, x0.at[:, own, :]), (rx_h, rx.at[:, own, :]), (src_h, sv.at[:, own, :])]
    loads = [pltpu.make_async_copy(a, b, lsem.at[i]) for i, (a, b) in enumerate(pairs)]
    for cp in loads:
        cp.start()

    barrier = pltpu.get_barrier_semaphore()

    def greet(peer):
        pl.semaphore_signal(barrier, inc=1, device_id=peer, device_id_type=MESH)

    far = sorted(range(1, nz), key=lambda k: -min(k, nz - k))
    flat = sorted(range(1, ny * nx), key=lambda i: -min(i // nx, ny - i // nx) - min(i % nx, nx - i % nx))
    for k in far:
        greet((y, nc - 1, x, planes[k - 1]))
    for i in flat:
        greet((plane[i][0], nc - 1, plane[i][1], z))

    @pl.when(hub)
    def _():
        for k in far:
            greet((y, 0, x, planes[k - 1]))
        for i in flat:
            greet((plane[i][0], 0, plane[i][1], z))

    for peer in around.values():
        greet(peer)
    greet((y, nc - 1 - c, x, z))

    for cp in loads[:2]:
        cp.wait()
    n = P_SIZE
    total = float(ny * nc * nx * nz * src_h.shape[0] * src_h.shape[1] * src_h.shape[2])
    lop = [[line[i, j] for j in range(n)] for i in range(n)]
    g = [0.5 * fd[i] + (TAU if i == 0 else 0.0) for i in range(n)]
    diag = lop[0][0]
    for i in range(1, n):
        diag = diag + lop[i][i]
    shift = 3.0 + 0.3125 * diag + 0.25 * fd[0]

    lane = lax.broadcasted_iota(jnp.int32, (8, 128), 1)
    sub = lax.broadcasted_iota(jnp.int32, (8, 128), 0)
    group = lane // 16
    slot16 = lax.rem(lane, 16)

    def lroll(t, s):
        s = s % 128
        return t if s == 0 else pltpu.roll(t, s, 1)

    def gather_groups(items, s):
        out = lroll(items[0], s)
        for a in range(1, len(items)):
            out = jnp.where(group == a, lroll(items[a], 16 * a + s), out)
        return out

    cline, cface = [], []
    for k in range(n):
        t = jnp.zeros((8, 128), jnp.float32)
        for a in range(n):
            t = jnp.where(group == a, lop[a][(a - k) % n], t)
        cline.append(t)
        cface.append(jnp.where(group == 0, g[(n - k) % n], jnp.where(group == n - 1, g[k], 0.0)))

    def x_faces(v):
        qw = [tree([g[i] * v(i, b) for i in range(n)], jnp.add) for b in range(n)]
        qe = [tree([g[i] * v(n - 1 - i, b) for i in range(n)], jnp.add) for b in range(n)]
        return qw, qe

    def strip_faces(t):
        rolled = [t] + [lroll(t, 16 * k) for k in range(1, n)]
        return rolled, tree([cface[k] * rolled[k] for k in range(n)], jnp.add)

    for cp in loads[2:7]:
        cp.wait()
    opl[...] = 1.0 - wfl[...].astype(jnp.float32)
    qw, qe = x_faces(lambda a, b: xl[a * n + b])
    for b in range(n):
        qs[0, 0, pl.ds(b, 1), :] = qw[b][2:3, :]
        qs[0, 1, pl.ds(b, 1), :] = qe[b][1:2, :]
    for b in range(n):
        px = gather_groups([xl[a * n + b] for a in range(n)], 6)
        ps = gather_groups([sl[a * n + b] for a in range(n)], 6)
        pr = gather_groups([rl[a * n + b] for a in range(n)], 6)
        pk[0, b] = jnp.where(slot16 < 6, px, jnp.where(slot16 < 11, lroll(ps, 5), lroll(pr, 10)))
        pk[1, b] = jnp.where(slot16 < 6, lroll(px, -6), jnp.where(slot16 < 11, ps, lroll(pr, 5)))
    gqs[0, 0] = lroll(qs[0, 0], 6)
    gqs[0, 1] = lroll(qs[0, 1], 118)
    pst = gather_groups([stl[...]] + [opl[f] for f in range(4)], 6)
    pk[0, n] = pst
    pk[1, n] = pst
    @pl.when(hub)
    def _():
        pl.semaphore_wait(barrier, 8 + 31 + 14)

    @pl.when(jnp.logical_not(hub))
    def _():
        pl.semaphore_wait(barrier, 8 + 16 + 7)


    def send(copies, peer, pieces, first):
        for i, (a, b) in enumerate(pieces):
            cp = pltpu.make_async_remote_copy(
                src_ref=a, dst_ref=b, send_sem=hs.at[first + i], recv_sem=hr.at[first + i],
                device_id=peer, device_id_type=MESH)
            cp.start()
            copies.append(cp)
        return first + len(pieces)

    def rows(lo):
        return pl.ds(lo, 2)

    copies, used = [], 0
    for dy, k, dst in ((1, 0, lb), (-1, 1, rb)):
        used = send(copies, around[0, dy], [(pk.at[k, :, own, :], dst.at[:, own, :])], used)
    for dy, k, dst, gq in ((1, 0, lb, gql), (-1, 1, rb, gqr)):
        for dx, lo, to in ((1, 2, 6), (-1, 0, 4)):
            side = 1 if dx > 0 else 0
            used = send(copies, around[dx, dy], [
                (pk.at[k, :, rows(lo), :], dst.at[:, rows(to), :]), (gqs.at[0, side], gq.at[0, side])], used)
    for dx, lo, to in ((1, 2, 6), (-1, 0, 4)):
        side = 1 if dx > 0 else 0
        used = send(copies, around[dx, 0], [
            (xl.at[:, rows(lo), :], x0.at[:, rows(to), :]),
            (rl.at[:, rows(lo), :], rx.at[:, rows(to), :]),
            (sl.at[:, rows(lo), :], sv.at[:, rows(to), :]),
            (stl.at[rows(lo), :], st.at[rows(to), :]),
            (opl.at[:, rows(lo), :], op.at[:, rows(to), :]),
            (qs.at[0, side], qr.at[0, side])], used)
    st[0:4, :] = stl[0:4, :]
    op[:, 0:4, :] = opl[:, 0:4, :]
    for q in range(0, n * n, 2):
        rxp[q // 2] = jnp.where(sub < 4, rl[q], pltpu.roll(rl[q + 1], 4, 0)) - shift
    for cp in loads[7:]:
        cp.wait()
    for cp in copies:
        cp.wait()

    before_half = slot16 < 6
    gsv, grx = [], []
    for b in range(n):
        lo, hi = lb[b], rb[b]
        gw[0, b] = jnp.where(before_half, lo, lroll(hi, 6))
        gsv.append(jnp.where(before_half, lroll(lo, -5), hi))
        grx.append(jnp.where(before_half, lroll(lo, -10), lroll(hi, -5)))
    both = jnp.where(before_half, lb[n], rb[n])
    spreads = []
    for f in range(5):
        t = jnp.where(group == f, both, 0.0)
        for s in (16, 32, 64):
            t = t + lroll(t, s)
        spreads.append(t)
    gst = spreads[0]
    gopw = jnp.where(group == 0, spreads[1], 0.0)
    gope = jnp.where(group == n - 1, spreads[2], 0.0)
    gops, gopn = spreads[3], spreads[4]
    for side in (0, 1):
        gqr[0, side] = jnp.where(before_half, gql[0, side], gqr[0, side])

    low = sub < 4
    for j in range(n // 2):
        for i in range(n // 2):
            cpair[0, j * 4 + i] = jnp.where(low, lop[2 * j][2 * i], lop[2 * j + 1][2 * i + 1])
            cpair[1, j * 4 + i] = jnp.where(low, lop[2 * j][2 * i + 1], lop[2 * j + 1][2 * i])

    def pair_up(even, odd):
        return jnp.where(low, even, pltpu.roll(odd, 4, 0))

    def apply(k, last=False, fresh=None, after_strip=None, after_half=None):
        wide = k != 2

        def v(a, b):
            return w[k - 1, a * n + b] if k else x0[a * n + b]

        gv = [gw[k, b] for b in range(n)]
        gqsouth = tree([g[i] * gv[i] for i in range(n)], jnp.add)
        gqnorth = tree([g[i] * gv[n - 1 - i] for i in range(n)], jnp.add)
        qsouth = [tree([g[i] * v(a, i) for i in range(n)], jnp.add) for a in range(n)]
        qnorth = [tree([g[i] * v(a, n - 1 - i) for i in range(n)], jnp.add) for a in range(n)]
        for a in range(n):
            below = jnp.where(lane == 0, lroll(gqnorth, -(16 * a + 5)), lroll(qnorth[a], 1))
            above = jnp.where(lane == 127, lroll(gqsouth, 121 - 16 * a), lroll(qsouth[a], -1))
            qf[2, a] = qsouth[a] - op[2] * below
            qf[3, a] = qnorth[a] - op[3] * above
        if not last:
            mn = gather_groups(qnorth, 7)
            ms = gather_groups(qsouth, 5)
            sterm = gqsouth - gops * jnp.where(slot16 == 6, mn, lroll(gqnorth, 1))
            nterm = gqnorth - gopn * jnp.where(slot16 == 5, ms, lroll(gqsouth, -1))
            for b in range(n):
                rolled, face = strip_faces(gv[b])
                prev = pltpu.roll(lroll(face, 16), 1, 0)
                nxt = pltpu.roll(lroll(face, -16), 7, 0)
                if fresh is not None:
                    prev = jnp.where(sub == 6, jnp.broadcast_to(lroll(gqr[fresh, 1, pl.ds(b, 1), :], 16), (8, 128)), prev)
                    nxt = jnp.where(sub == 5, jnp.broadcast_to(lroll(gqr[fresh, 0, pl.ds(b, 1), :], -16), (8, 128)), nxt)
                acc = tree([cline[i] * rolled[i] for i in range(n)] + [lop[b][i] * gv[i] for i in range(n)], jnp.add)
                t = grx[b] * gv[b] + gst * acc + (face - (gopw * prev + gope * nxt))
                if b == 0:
                    t = t + sterm
                if b == n - 1:
                    t = t + nterm
                t = t - (gsv[b] if k == 0 else shift * gv[b])
                if wide:
                    gw[k + 1, b] = t
                else:
                    gw[k + 1, b, 0:4, :] = t[0:4, :]
            if after_strip is not None:
                after_strip()
        for b in range(n):
            qwest = tree([g[i] * v(i, b) for i in range(n)], jnp.add)
            qeast = tree([g[i] * v(n - 1 - i, b) for i in range(n)], jnp.add)
            prev = pltpu.roll(qeast, 1, 0)
            nxt = pltpu.roll(qwest, 7, 0)
            if fresh is not None:
                prev = jnp.where(sub == 6, jnp.broadcast_to(qr[fresh, 1, pl.ds(b, 1), :], (8, 128)), prev)
                nxt = jnp.where(sub == 5, jnp.broadcast_to(qr[fresh, 0, pl.ds(b, 1), :], (8, 128)), nxt)
            qf[0, b] = qwest - op[0] * prev
            qf[1, b] = qeast - op[1] * nxt
        if not wide or last:
            stiff = pair_up(st[...], st[...])
            for a in range(n):
                tiles = [wp[k - 1, a * 4 + j] for j in range(4)]
                swapped = [pltpu.roll(t, 4, 0) for t in tiles]
                for j in range(4):
                    q = a * n + 2 * j
                    acc = tree([lop[a][i] * wp[k - 1, i * 4 + j] for i in range(n)]
                               + [cpair[0, j * 4 + i] * tiles[i] for i in range(4)]
                               + [cpair[1, j * 4 + i] * swapped[i] for i in range(4)], jnp.add)
                    t = rxp[q // 2] * tiles[j] + stiff * acc
                    if a == 0:
                        t = t + pair_up(qf[0, 2 * j], qf[0, 2 * j + 1])
                    if a == n - 1:
                        t = t + pair_up(qf[1, 2 * j], qf[1, 2 * j + 1])
                    if j == 0:
                        t = t + jnp.where(low, qf[2, a], 0.0)
                    if j == 3:
                        t = t + jnp.where(low, 0.0, pltpu.roll(qf[3, a], 4, 0))
                    wp[k, q // 2] = t
                    if not last:
                        w[k, q, 0:4, :] = t[0:4, :]
                        w[k, q + 1, 0:4, :] = pltpu.roll(t, 4, 0)[0:4, :]
                if a == 3 and after_half is not None:
                    after_half()
            return
        stiff = st[...]
        for a in range(n):
            row = [v(a, i) for i in range(n)]
            even = None
            for b in range(n):
                acc = tree([lop[b][i] * row[i] for i in range(n)] + [lop[a][i] * v(i, b) for i in range(n)], jnp.add)
                if k == 0:
                    t = rx[a * n + b] * row[b] - sv[a * n + b] + stiff * acc
                else:
                    t = (rx[a * n + b] - shift) * row[b] + stiff * acc
                if a == 0:
                    t = t + qf[0, b]
                if a == n - 1:
                    t = t + qf[1, b]
                if b == 0:
                    t = t + qf[2, a]
                if b == n - 1:
                    t = t + qf[3, a]
                w[k, a * n + b] = t
                if b % 2 == 0:
                    even = t
                else:
                    wp[k, (a * n + b) // 2] = pair_up(even, t)

    apply(0, fresh=0)
    apply(1)
    copies = []
    sides = ((1, 2, 6), (-1, 0, 4))

    def send_strip():
        nonlocal used
        for b in range(n):
            t = jnp.concatenate([gw[3, b, 0:4, :]] * 2, axis=0)
            face = strip_faces(t)[1]
            gqs[1, 0, pl.ds(b, 1), :] = face[2:3, :]
            gqs[1, 1, pl.ds(b, 1), :] = face[1:2, :]
        for dx, lo, to in sides:
            side = 1 if dx > 0 else 0
            used = send(copies, around[dx, 0], [
                (gw.at[3, :, rows(lo), :], gw.at[3, :, rows(to), :]), (gqs.at[1, side], gqr.at[1, side])], used)

    def send_block(first):
        nonlocal used
        part = pl.ds(first, n * n // 2)
        for dx, lo, to in sides:
            used = send(copies, around[dx, 0], [(w.at[2, part, rows(lo), :], w.at[2, part, rows(to), :])], used)

    apply(2, after_strip=send_strip, after_half=lambda: send_block(0))
    send_block(n * n // 2)
    qw, qe = x_faces(lambda a, b: w[2, a * n + b, 0:4, :])
    for b in range(n):
        qs[1, 0, pl.ds(b, 1), :] = qw[b][2:3, :]
        qs[1, 1, pl.ds(b, 1), :] = qe[b][1:2, :]
    for dx, lo, to in sides:
        side = 1 if dx > 0 else 0
        used = send(copies, around[dx, 0], [(qs.at[1, side], qr.at[1, side])], used)
    def gram(pairs):
        top = max(j for i, j in pairs) + 1

        def body(q, acc):
            vals = [wp[i, q] for i in range(top)]
            return tuple(t + vals[i] * vals[j] for t, (i, j) in zip(acc, pairs))

        return lax.fori_loop(0, n * n // 2, body, tuple(jnp.zeros((8, 128), jnp.float32) for _ in pairs), unroll=8)

    early = [p for p in PAIRS if p[1] < 3]
    first = gram(early)
    for cp in copies:
        cp.wait()
    apply(3, fresh=1)
    apply(4)
    apply(5, last=True)

    acc = first + gram(PAIRS[len(early):])
    line_row = jnp.zeros((8, 128), jnp.float32)
    for base in range(0, len(PAIRS), 8):
        packed = jnp.zeros((8, 128), jnp.float32)
        for i, t in enumerate(acc[base:base + 8]):
            t = t + pltpu.roll(t, 4, 0)
            t = t + pltpu.roll(t, 2, 0)
            t = t + pltpu.roll(t, 1, 0)
            packed = jnp.where(sub == i, t, packed)
        packed = jnp.sum(packed, axis=1, keepdims=True) * (1.0 / total)
        line_row = line_row + jnp.where(lane == sub + base, packed, 0.0)
    for s in (4, 2, 1):
        line_row = line_row + pltpu.roll(line_row, s, 0)
    zero1 = jnp.zeros((1, 128), jnp.float32)
    row1[...] = line_row[0:1, :]

    def to_hub(j, index, peer):
        return pltpu.make_async_remote_copy(
            src_ref=row1, dst_ref=buf1.at[index], send_sem=s1.at[j], recv_sem=r1.at[index],
            device_id=peer, device_id_type=MESH)

    def across(j, index, peer):
        return pltpu.make_async_remote_copy(
            src_ref=row2, dst_ref=buf2.at[index], send_sem=s2.at[j], recv_sem=r2.at[index],
            device_id=peer, device_id_type=MESH)

    partner = (y, nc - 1 - c, x, z)
    for j, (yy, xx) in enumerate(plane):
        if j:
            to_hub(j, me, (yy, nc - 1, xx, z)).start()

    @pl.when(hub)
    def _():
        buf1[me] = row1[...]
        for j, (yy, xx) in enumerate(plane):
            for cc in range(nc):
                if j or cc != nc - 1:
                    to_hub(j, (cc * ny + yy) * nx + xx, partner).wait_recv()
        total1 = tree([(buf1[j], zero1) for j in range(nc * ny * nx)], add2)
        total1 = tidy(total1)
        row2[0:1, :] = total1[0]
        row2[1:2, :] = total1[1]
        k = 0
        for zz in planes:
            for cc in (nc - 1, 0):
                across(k, z, (y, cc, x, zz)).start()
                k += 1
        across(k, z, partner).start()
        buf2[z] = row2[...]

    @pl.when(jnp.logical_not(hub))
    def _():
        to_hub(0, me, partner).start()
        across(0, z, partner).wait_recv()
        to_hub(0, me, partner).wait_send()

    for zz in planes:
        across(0, zz, partner).wait_recv()
    for j in range(1, len(plane)):
        to_hub(j, me, partner).wait_send()

    @pl.when(hub)
    def _():
        for k in range(2 * len(planes) + 1):
            across(k, z, partner).wait_send()

    part = tidy(tree([(buf2[j, 0:1, :], buf2[j, 1:2, :]) for j in range(nz)], add2))

    slot = {}
    for p, (i, j) in enumerate(PAIRS):
        slot[i, j] = slot[j, i] = p
    columns = []
    for k in range(NV):
        at = jnp.full((8, 128), -1, jnp.int32)
        for i in range(NV):
            at = jnp.where(sub == i, slot[i, k], at)
        columns.append(tuple(
            jnp.broadcast_to(
                jnp.sum(jnp.where(lane == at, jnp.broadcast_to(t, (8, 128)), 0.0), axis=1, keepdims=True), (8, 128))
            for t in part))

    def spread(t, k):
        return jnp.broadcast_to(t[k:k + 1, :], (8, 128))

    def dot(a, b):
        return sublane_total(mul2(a, b))

    wide_shift = jnp.broadcast_to(shift, (8, 128))
    moved = [add2(columns[k + 1], mul1(columns[k], wide_shift)) for k in range(ITERS)]
    moved = [tidy(t) for t in moved]
    hmat = jnp.zeros((8, 128), jnp.float32)
    zeros = jnp.zeros((8, 128), jnp.float32)
    u = (jnp.where(sub == 0, -1.0, 0.0), zeros)
    e = tuple(-t for t in columns[0])
    ratio = None
    coefs, images = [], []
    for j in range(NV):
        square = dot(u, e)[0]
        square = (square if ratio is None else square * (ratio * ratio)) + FLOOR
        inv = lax.rsqrt(square)
        if j > 0:
            hmat = jnp.where((sub == j) & (lane == j - 1), square * inv, hmat)
        unit = inv if ratio is None else inv * ratio
        coefs.append(tidy(mul1(u, unit)))
        if j == ITERS:
            break
        images.append(tidy(mul1(e, unit)))
        m = tidy(add2(tuple(pltpu.roll(t, 1, 0) for t in u), mul1(u, wide_shift)))
        f = tree([mul2(moved[k], tuple(spread(t, k) for t in u)) for k in range(j + 1)], add2)
        parts = [dot(images[i], m)[0] for i in range(j)]
        own = dot(e, m)[0] * (unit * unit)
        for i in range(j):
            hmat = jnp.where((sub == i) & (lane == j), parts[i] * unit, hmat)
        hmat = jnp.where((sub == j) & (lane == j), own, hmat)
        u, e = (
            tidy(tree([x] + [mul1(basis[i], -parts[i]) for i in range(j)] + [mul1(latest, -own)], add2))
            for x, basis, latest in ((m, coefs, u), (f, images, e)))
        ratio = unit
    hm[...] = hmat
    for j in range(NV):
        cw[j] = coefs[j][0]


def output_kernel(w, cw, hm, hess_h, out_h, hess, vout, sem):
    half = w.shape[1]
    hess[...] = hm[0:NV, 0:ITERS]
    outs = [pltpu.make_async_copy(hess, hess_h, sem.at[0])]
    outs[0].start()
    for j in range(NV):
        weights = [jnp.broadcast_to(cw[j, pl.ds(i, 1), :], (8, 128)) for i in range(j + 1)]

        def combine(q, carry):
            t = tree([weights[i] * w[i, q] for i in range(j + 1)], jnp.add)
            vout[j, 2 * q] = t[0:4, :]
            vout[j, 2 * q + 1] = t[4:8, :]
            return carry

        lax.fori_loop(0, half, combine, 0, unroll=8)
        cp = pltpu.make_async_copy(vout.at[j], out_h.at[j], sem.at[j + 1])
        cp.start()
        outs.append(cp)
    for cp in outs:
        cp.wait()


def solution(mesh):
    ny, nc, nx, nz = 4, 2, 4, 8
    finer = Mesh(mesh.devices.reshape(ny, nc, nx, nz), AXES)
    gxs, gys = ("y", "c"), ("x", "z")
    sizes = (ny, nc, nx, nz)
    f32 = jnp.float32

    def body(source, initial, reaction, stiffness, line_op, face_deriv, wall_flags):
        nodes, ex, ey = source.shape
        hbm = pl.BlockSpec(memory_space=pltpu.HBM)
        scalars = pl.BlockSpec(memory_space=pltpu.SMEM)
        local = pl.BlockSpec(memory_space=pltpu.VMEM)
        vm = pltpu.VMEM
        dma = pltpu.SemaphoreType.DMA
        tile = (8, ey)
        sends = 2 + 8 + 12 + 10
        w, cw, hm = pl.pallas_call(
            functools.partial(kernel, sizes),
            out_shape=(
                pltpu.VMEM((NV, nodes // 2) + tile, f32), pltpu.VMEM((NV,) + tile, f32), pltpu.VMEM(tile, f32),
            ),
            in_specs=[hbm] * 7,
            out_specs=(local, local, local),
            scratch_shapes=[
                vm((nodes,) + tile, f32), vm((nodes,) + tile, f32), vm((nodes,) + tile, f32), vm(tile, f32),
                vm((4,) + tile, jnp.int32), vm((4,) + tile, f32),
                vm((NV - 1, nodes) + tile, f32), vm((nodes,) + tile, f32), vm((nodes,) + tile, f32), vm((nodes,) + tile, f32),
                vm(tile, f32), vm((4,) + tile, f32), vm((NV, 8) + tile, f32),
                vm((2, 9) + tile, f32), vm((9,) + tile, f32), vm((9,) + tile, f32),
                vm((2, 2) + tile, f32), vm((2, 2) + tile, f32), vm((2, 2) + tile, f32), vm((1, 2) + tile, f32),
                vm((2, 2) + tile, f32), vm((4, 8) + tile, f32),
                vm((1, 128), f32), vm((nc * ny * nx, 1, 128), f32), vm((2, 128), f32), vm((nz, 2, 128), f32),
                pltpu.SMEM((P_SIZE, P_SIZE), f32), pltpu.SMEM((P_SIZE,), f32),
                vm((nodes // 2,) + tile, f32), vm((2, 16) + tile, f32),
                dma((10,)), dma((sends,)), dma((sends,)), dma((ny * nx,)), dma((nc * ny * nx,)), dma((2 * nz - 1,)), dma((nz,)),
            ],
            compiler_params=pltpu.CompilerParams(
                collective_id=0, has_side_effects=True, vmem_limit_bytes=48 * 1024 * 1024),
            name="arnoldi",
        )(*[pltpu.with_memory_space_constraint(t, pltpu.HBM) for t in (
            line_op, face_deriv, source, initial, reaction, stiffness, wall_flags)])
        return pl.pallas_call(
            output_kernel,
            out_shape=(
                jax.ShapeDtypeStruct((NV, ITERS), f32),
                jax.ShapeDtypeStruct((NV, nodes, ex, ey), f32),
            ),
            in_specs=[local] * 3,
            out_specs=(hbm, hbm),
            scratch_shapes=[vm((NV, ITERS), f32), vm((NV, nodes, ex, ey), f32), dma((NV + 1,))],
            compiler_params=pltpu.CompilerParams(vmem_limit_bytes=16 * 1024 * 1024),
            name="combine",
        )(w, cw, hm)

    placed = (P(None, gxs, gys), P(None, gxs, gys), P(None, gxs, gys), P(gxs, gys), P(), P(), P(None, gxs, gys))
    return jax.shard_map(
        body, mesh=finer, in_specs=placed, out_specs=(P(), P(None, None, gxs, gys)), check_vma=False)
```

```python
import functools

import jax
import jax.numpy as jnp
from jax import lax
from jax.experimental import pallas as pl
from jax.experimental.pallas import tpu as pltpu
from jax.sharding import Mesh
from jax.sharding import PartitionSpec as P

P_SIZE = 8
ITERS = 5
NV = ITERS + 1
TAU = 2.0
FLOOR = 0.1
MESH = pl.DeviceIdType.MESH
AXES = ("y", "c", "x", "z")
PAIRS = [(i, j) for j in range(NV) for i in range(j + 1)]


def two_sum(a, b):
    s = a + b
    t = s - a
    return s, (a - (s - t)) + (b - t)


def split(a):
    c = a * 4097.0
    hi = c - (c - a)
    return hi, a - hi


def two_prod(a, b):
    p = a * b
    ah, al = split(a)
    bh, bl = split(b)
    return p, ((ah * bh - p) + ah * bl + al * bh) + al * bl


def add2(a, b):
    s, e = two_sum(a[0], b[0])
    return s, e + (a[1] + b[1])


def mul2(a, b):
    p, e = two_prod(a[0], b[0])
    return p, e + (a[0] * b[1] + a[1] * b[0])


def mul1(a, b):
    p, e = two_prod(a[0], b)
    return p, e + a[1] * b


def tidy(a):
    return two_sum(*a)


def tree(items, op):
    items = list(items)
    while len(items) > 1:
        nxt = [op(items[i], items[i + 1]) for i in range(0, len(items) - 1, 2)]
        if len(items) % 2:
            nxt.append(items[-1])
        items = nxt
    return items[0]


def sublane_total(a):
    for s in (4, 2, 1):
        a = add2(a, tuple(pltpu.roll(v, s, 0) for v in a))
    return tidy(a)


def kernel(sizes, line_h, fd_h, src_h, x0_h, rx_h, st_h, wf_h, wp, cw, hm,
           xl, sl, rl, stl, wfl, opl, w, rx, st, op, gw, pk, lb, rb, qs, qr, gqs, gql, gqr, qf,
           row1, buf1, row2, buf2, line, fd, rxp, cpair, xc, mm,
           lsem, hs, hr, s1, r1, s2, r2):
    ny, nc, nx, nz = sizes
    y, c, x, z = (lax.axis_index(a) for a in AXES)

    def at(dx, dy):
        i = lax.rem(y * nc + c + ny * nc + dx, ny * nc)
        j = lax.rem(x * nz + z + nx * nz + dy, nx * nz)
        return (i // nc, lax.rem(i, nc), j // nz, lax.rem(j, nz))

    hub = c == nc - 1
    plane = [(lax.rem(y + i, ny), lax.rem(x + k, nx)) for i in range(ny) for k in range(nx)]
    planes = [lax.rem(z + k, nz) for k in range(1, nz)]
    me = (c * ny + y) * nx + x
    around = {(i, j): at(i, j) for i in (-1, 0, 1) for j in (-1, 0, 1) if (i, j) != (0, 0)}
    own = pl.ds(0, 4)
    pairs = [(line_h, line), (fd_h, fd), (x0_h, xl.at[:, own, :]), (rx_h, rl.at[:, own, :]), (src_h, sl.at[:, own, :]), (st_h, stl.at[own, :]),
             (wf_h, wfl.at[:, own, :]), (rx_h, rx.at[:, own, :])]
    loads = [pltpu.make_async_copy(a, b, lsem.at[i]) for i, (a, b) in enumerate(pairs)]
    for cp in loads:
        cp.start()

    barrier = pltpu.get_barrier_semaphore()

    def greet(peer):
        pl.semaphore_signal(barrier, inc=1, device_id=peer, device_id_type=MESH)

    far = sorted(range(1, nz), key=lambda k: -min(k, nz - k))
    flat = sorted(range(1, ny * nx), key=lambda i: -min(i // nx, ny - i // nx) - min(i % nx, nx - i % nx))
    for k in far:
        greet((y, nc - 1, x, planes[k - 1]))
    for i in flat:
        greet((plane[i][0], nc - 1, plane[i][1], z))

    @pl.when(hub)
    def _():
        for k in far:
            greet((y, 0, x, planes[k - 1]))
        for i in flat:
            greet((plane[i][0], 0, plane[i][1], z))

    for peer in around.values():
        greet(peer)
    greet((y, nc - 1 - c, x, z))

    for cp in loads[:2]:
        cp.wait()
    n = P_SIZE
    total = float(ny * nc * nx * nz * src_h.shape[0] * src_h.shape[1] * src_h.shape[2])
    lop = [[line[i, j] for j in range(n)] for i in range(n)]
    g = [0.5 * fd[i] + (TAU if i == 0 else 0.0) for i in range(n)]
    diag = lop[0][0]
    for i in range(1, n):
        diag = diag + lop[i][i]
    shift = 3.0 + 0.3125 * diag + 0.25 * fd[0]

    lane = lax.broadcasted_iota(jnp.int32, (8, 128), 1)
    sub = lax.broadcasted_iota(jnp.int32, (8, 128), 0)
    group = lane // 16
    slot16 = lax.rem(lane, 16)

    def lroll(t, s):
        s = s % 128
        return t if s == 0 else pltpu.roll(t, s, 1)

    def gather_groups(items, s):
        out = lroll(items[0], s)
        for a in range(1, len(items)):
            out = jnp.where(group == a, lroll(items[a], 16 * a + s), out)
        return out

    cline, cface = [], []
    for k in range(n):
        t = jnp.zeros((8, 128), jnp.float32)
        for a in range(n):
            t = jnp.where(group == a, lop[a][(a - k) % n], t)
        cline.append(t)
        cface.append(jnp.where(group == 0, g[(n - k) % n], jnp.where(group == n - 1, g[k], 0.0)))

    def x_faces(v):
        qw = [tree([g[i] * v(i, b) for i in range(n)], jnp.add) for b in range(n)]
        qe = [tree([g[i] * v(n - 1 - i, b) for i in range(n)], jnp.add) for b in range(n)]
        return qw, qe

    def strip_faces(t):
        rolled = [t] + [lroll(t, 16 * k) for k in range(1, n)]
        return rolled, tree([cface[k] * rolled[k] for k in range(n)], jnp.add)

    for cp in loads[2:7]:
        cp.wait()
    opl[...] = 1.0 - wfl[...].astype(jnp.float32)
    qw, qe = x_faces(lambda a, b: xl[a * n + b])
    qsouth = [tree([g[i] * xl[a * n + i] for i in range(n)], jnp.add) for a in range(n)]
    qnorth = [tree([g[i] * xl[a * n + n - 1 - i] for i in range(n)], jnp.add) for a in range(n)]
    for b in range(n):
        qs[0, 0, pl.ds(b, 1), :] = qw[b][0:1, :]
        qs[0, 1, pl.ds(b, 1), :] = qe[b][3:4, :]
        gqs[0, 0, pl.ds(b, 1), :] = qw[b][2:3, :]
        gqs[0, 1, pl.ds(b, 1), :] = qe[b][1:2, :]
        xc[0, b] = pltpu.roll(qe[b], 1, 0)
        xc[1, b] = pltpu.roll(qw[b], 7, 0)
        qf[0, b] = qw[b] - opl[0] * jnp.where(sub == 0, 0.0, xc[0, b])
        qf[1, b] = qe[b] - opl[1] * jnp.where(sub == 3, 0.0, xc[1, b])
    for a in range(n):
        qf[2, a] = qsouth[a] - opl[2] * jnp.where(lane == 0, 0.0, lroll(qnorth[a], 1))
        qf[3, a] = qnorth[a] - opl[3] * jnp.where(lane == 127, 0.0, lroll(qsouth[a], -1))
    mm[0, 0:4, :] = gather_groups(qnorth, 7)[0:4, :]
    mm[1, 0:4, :] = gather_groups(qsouth, 5)[0:4, :]
    for a in range(n):
        row = [xl[a * n + i] for i in range(n)]
        for b in range(n):
            acc = tree([lop[b][i] * row[i] for i in range(n)] + [lop[a][i] * xl[i * n + b] for i in range(n)], jnp.add)
            t = rl[a * n + b] * row[b] - sl[a * n + b] + stl[...] * acc
            for edge, f, i in ((a == 0, 0, b), (a == n - 1, 1, b), (b == 0, 2, a), (b == n - 1, 3, a)):
                if edge:
                    t = t + qf[f, i]
            w[0, a * n + b, 0:4, :] = t[0:4, :]
    for b in range(n):
        px = gather_groups([xl[a * n + b] for a in range(n)], 6)
        ps = gather_groups([sl[a * n + b] for a in range(n)], 6)
        pr = gather_groups([rl[a * n + b] for a in range(n)], 6)
        pk[0, b] = jnp.where(slot16 < 6, px, jnp.where(slot16 < 11, lroll(ps, 5), lroll(pr, 10)))
        pk[1, b] = jnp.where(slot16 < 6, lroll(px, -6), jnp.where(slot16 < 11, ps, lroll(pr, 5)))
    gqs[0, 0] = lroll(gqs[0, 0], 6)
    gqs[0, 1] = lroll(gqs[0, 1], 118)
    for f, t in enumerate([stl[...]] + [opl[i] for i in range(4)]):
        spread_out = gather_groups([t] * n, 6)
        pk[0, n + f] = spread_out
        pk[1, n + f] = spread_out
    @pl.when(hub)
    def _():
        pl.semaphore_wait(barrier, 8 + 31 + 14)

    @pl.when(jnp.logical_not(hub))
    def _():
        pl.semaphore_wait(barrier, 8 + 16 + 7)


    def send(copies, peer, pieces, first):
        for i, (a, b) in enumerate(pieces):
            cp = pltpu.make_async_remote_copy(
                src_ref=a, dst_ref=b, send_sem=hs.at[first + i], recv_sem=hr.at[first + i],
                device_id=peer, device_id_type=MESH)
            cp.start()
            copies.append(cp)
        return first + len(pieces)

    def rows(lo):
        return pl.ds(lo, 2)

    copies, used = [], 0
    for dy, k, dst in ((1, 0, lb), (-1, 1, rb)):
        used = send(copies, around[0, dy], [(pk.at[k, :, own, :], dst.at[:, own, :])], used)
    for dy, k, dst, gq in ((1, 0, lb, gql), (-1, 1, rb, gqr)):
        for dx, lo, to in ((1, 2, 6), (-1, 0, 4)):
            side = 1 if dx > 0 else 0
            used = send(copies, around[dx, dy], [
                (pk.at[k, :, rows(lo), :], dst.at[:, rows(to), :]), (gqs.at[0, side], gq.at[0, side])], used)
    for dx, lo, to in ((1, 2, 6), (-1, 0, 4)):
        side = 1 if dx > 0 else 0
        used = send(copies, around[dx, 0], [
            (w.at[0, :, rows(lo), :], w.at[0, :, rows(to), :]),
            (rl.at[:, rows(lo), :], rx.at[:, rows(to), :]),
            (mm.at[:, rows(lo), :], mm.at[:, rows(to), :]),
            (stl.at[rows(lo), :], st.at[rows(to), :]),
            (opl.at[:, rows(lo), :], op.at[:, rows(to), :]),
            (qs.at[0, side], qr.at[0, side])], used)
    st[0:4, :] = stl[0:4, :]
    op[:, 0:4, :] = opl[:, 0:4, :]
    for q in range(0, n * n, 2):
        rxp[q // 2] = jnp.where(sub < 4, rl[q], pltpu.roll(rl[q + 1], 4, 0)) - shift
    for cp in loads[7:]:
        cp.wait()
    for cp in copies:
        cp.wait()

    before_half = slot16 < 6
    gsv, grx = [], []
    for b in range(n):
        lo, hi = lb[b], rb[b]
        gw[0, b] = jnp.where(before_half, lo, lroll(hi, 6))
        gsv.append(jnp.where(before_half, lroll(lo, -5), hi))
        grx.append(jnp.where(before_half, lroll(lo, -10), lroll(hi, -5)))
    spreads = [jnp.where(before_half, lb[n + f], rb[n + f]) for f in range(5)]
    gst = spreads[0]
    gopw = jnp.where(group == 0, spreads[1], 0.0)
    gope = jnp.where(group == n - 1, spreads[2], 0.0)
    gops, gopn = spreads[3], spreads[4]
    for side in (0, 1):
        gqr[0, side] = jnp.where(before_half, gql[0, side], gqr[0, side])

    low = sub < 4
    for j in range(n // 2):
        for i in range(n // 2):
            cpair[0, j * 4 + i] = jnp.where(low, lop[2 * j][2 * i], lop[2 * j + 1][2 * i + 1])
            cpair[1, j * 4 + i] = jnp.where(low, lop[2 * j][2 * i + 1], lop[2 * j + 1][2 * i])

    def pair_up(even, odd):
        return jnp.where(low, even, pltpu.roll(odd, 4, 0))

    def apply(k, last=False, fresh=None, after_strip=None, after_half=None):
        wide = k != 2

        def v(a, b):
            return w[k - 1, a * n + b]

        gv = [gw[k, b] for b in range(n)]
        gqsouth = tree([g[i] * gv[i] for i in range(n)], jnp.add)
        gqnorth = tree([g[i] * gv[n - 1 - i] for i in range(n)], jnp.add)
        if k:
            qsouth = [tree([g[i] * v(a, i) for i in range(n)], jnp.add) for a in range(n)]
            qnorth = [tree([g[i] * v(a, n - 1 - i) for i in range(n)], jnp.add) for a in range(n)]
        for a in range(n):
            below = jnp.where(lane == 0, lroll(gqnorth, -(16 * a + 5)), lroll(qnorth[a], 1) if k else 0.0)
            above = jnp.where(lane == 127, lroll(gqsouth, 121 - 16 * a), lroll(qsouth[a], -1) if k else 0.0)
            qf[2, a] = qsouth[a] - op[2] * below if k else -op[2] * below
            qf[3, a] = qnorth[a] - op[3] * above if k else -op[3] * above
        if not last:
            mn = gather_groups(qnorth, 7) if k else mm[0]
            ms = gather_groups(qsouth, 5) if k else mm[1]
            sterm = gqsouth - gops * jnp.where(slot16 == 6, mn, lroll(gqnorth, 1))
            nterm = gqnorth - gopn * jnp.where(slot16 == 5, ms, lroll(gqsouth, -1))
            for b in range(n):
                rolled, face = strip_faces(gv[b])
                prev = pltpu.roll(lroll(face, 16), 1, 0)
                nxt = pltpu.roll(lroll(face, -16), 7, 0)
                if fresh is not None:
                    prev = jnp.where(sub == 6, jnp.broadcast_to(lroll(gqr[fresh, 1, pl.ds(b, 1), :], 16), (8, 128)), prev)
                    nxt = jnp.where(sub == 5, jnp.broadcast_to(lroll(gqr[fresh, 0, pl.ds(b, 1), :], -16), (8, 128)), nxt)
                acc = tree([cline[i] * rolled[i] for i in range(n)] + [lop[b][i] * gv[i] for i in range(n)], jnp.add)
                t = grx[b] * gv[b] + gst * acc + (face - (gopw * prev + gope * nxt))
                if b == 0:
                    t = t + sterm
                if b == n - 1:
                    t = t + nterm
                t = t - (gsv[b] if k == 0 else shift * gv[b])
                if wide:
                    gw[k + 1, b] = t
                else:
                    gw[k + 1, b, 0:4, :] = t[0:4, :]
            if after_strip is not None:
                after_strip()
        if k == 0:
            for b in range(n):
                prev = jnp.where(sub == 4, xc[0, b], 0.0)
                nxt = jnp.where(sub == 7, xc[1, b], 0.0)
                prev = jnp.where(sub == 0, jnp.broadcast_to(qr[0, 1, pl.ds(b, 1), :], (8, 128)), prev)
                nxt = jnp.where(sub == 3, jnp.broadcast_to(qr[0, 0, pl.ds(b, 1), :], (8, 128)), nxt)
                qf[0, b] = -op[0] * prev
                qf[1, b] = -op[1] * nxt
            for a in range(n):
                for b in range(n):
                    t = w[0, a * n + b]
                    edges = ((a == 0, 0, b), (a == n - 1, 1, b), (b == 0, 2, a), (b == n - 1, 3, a))
                    for edge, f, i in edges:
                        if edge:
                            t = t + qf[f, i]
                    if any(edge for edge, f, i in edges):
                        w[0, a * n + b] = t
                    if b % 2 == 0:
                        even = t
                    else:
                        wp[0, (a * n + b) // 2] = pair_up(even, t)
            return
        for b in range(n):
            qwest = tree([g[i] * v(i, b) for i in range(n)], jnp.add)
            qeast = tree([g[i] * v(n - 1 - i, b) for i in range(n)], jnp.add)
            prev = pltpu.roll(qeast, 1, 0)
            nxt = pltpu.roll(qwest, 7, 0)
            if fresh is not None:
                prev = jnp.where(sub == 6, jnp.broadcast_to(qr[fresh, 1, pl.ds(b, 1), :], (8, 128)), prev)
                nxt = jnp.where(sub == 5, jnp.broadcast_to(qr[fresh, 0, pl.ds(b, 1), :], (8, 128)), nxt)
            qf[0, b] = qwest - op[0] * prev
            qf[1, b] = qeast - op[1] * nxt
        if not wide or last:
            stiff = pair_up(st[...], st[...])
            for a in range(n):
                tiles = [wp[k - 1, a * 4 + j] for j in range(4)]
                swapped = [pltpu.roll(t, 4, 0) for t in tiles]
                for j in range(4):
                    q = a * n + 2 * j
                    acc = tree([lop[a][i] * wp[k - 1, i * 4 + j] for i in range(n)]
                               + [cpair[0, j * 4 + i] * tiles[i] for i in range(4)]
                               + [cpair[1, j * 4 + i] * swapped[i] for i in range(4)], jnp.add)
                    t = rxp[q // 2] * tiles[j] + stiff * acc
                    if a == 0:
                        t = t + pair_up(qf[0, 2 * j], qf[0, 2 * j + 1])
                    if a == n - 1:
                        t = t + pair_up(qf[1, 2 * j], qf[1, 2 * j + 1])
                    if j == 0:
                        t = t + jnp.where(low, qf[2, a], 0.0)
                    if j == 3:
                        t = t + jnp.where(low, 0.0, pltpu.roll(qf[3, a], 4, 0))
                    wp[k, q // 2] = t
                    if not last:
                        w[k, q, 0:4, :] = t[0:4, :]
                        w[k, q + 1, 0:4, :] = pltpu.roll(t, 4, 0)[0:4, :]
                if a == 3 and after_half is not None:
                    after_half()
            return
        stiff = st[...]
        for a in range(n):
            row = [v(a, i) for i in range(n)]
            even = None
            for b in range(n):
                acc = tree([lop[b][i] * row[i] for i in range(n)] + [lop[a][i] * v(i, b) for i in range(n)], jnp.add)
                t = (rx[a * n + b] - shift) * row[b] + stiff * acc
                if a == 0:
                    t = t + qf[0, b]
                if a == n - 1:
                    t = t + qf[1, b]
                if b == 0:
                    t = t + qf[2, a]
                if b == n - 1:
                    t = t + qf[3, a]
                w[k, a * n + b] = t
                if b % 2 == 0:
                    even = t
                else:
                    wp[k, (a * n + b) // 2] = pair_up(even, t)

    apply(0, fresh=0)
    apply(1)
    copies = []
    sides = ((1, 2, 6), (-1, 0, 4))

    def send_strip():
        nonlocal used
        for b in range(n):
            t = jnp.concatenate([gw[3, b, 0:4, :]] * 2, axis=0)
            face = strip_faces(t)[1]
            gqs[1, 0, pl.ds(b, 1), :] = face[2:3, :]
            gqs[1, 1, pl.ds(b, 1), :] = face[1:2, :]
        for dx, lo, to in sides:
            side = 1 if dx > 0 else 0
            used = send(copies, around[dx, 0], [
                (gw.at[3, :, rows(lo), :], gw.at[3, :, rows(to), :]), (gqs.at[1, side], gqr.at[1, side])], used)

    def send_block(first):
        nonlocal used
        part = pl.ds(first, n * n // 2)
        for dx, lo, to in sides:
            used = send(copies, around[dx, 0], [(w.at[2, part, rows(lo), :], w.at[2, part, rows(to), :])], used)

    apply(2, after_strip=send_strip, after_half=lambda: send_block(0))
    send_block(n * n // 2)
    qw, qe = x_faces(lambda a, b: w[2, a * n + b, 0:4, :])
    for b in range(n):
        qs[1, 0, pl.ds(b, 1), :] = qw[b][2:3, :]
        qs[1, 1, pl.ds(b, 1), :] = qe[b][1:2, :]
    for dx, lo, to in sides:
        side = 1 if dx > 0 else 0
        used = send(copies, around[dx, 0], [(qs.at[1, side], qr.at[1, side])], used)
    def gram(pairs):
        top = max(j for i, j in pairs) + 1

        def body(q, acc):
            vals = [wp[i, q] for i in range(top)]
            return tuple(t + vals[i] * vals[j] for t, (i, j) in zip(acc, pairs))

        return lax.fori_loop(0, n * n // 2, body, tuple(jnp.zeros((8, 128), jnp.float32) for _ in pairs), unroll=8)

    early = [p for p in PAIRS if p[1] < 3]
    first = gram(early)
    for cp in copies:
        cp.wait()
    apply(3, fresh=1)
    apply(4)
    apply(5, last=True)

    acc = first + gram(PAIRS[len(early):])
    line_row = jnp.zeros((8, 128), jnp.float32)
    for base in range(0, len(PAIRS), 8):
        packed = jnp.zeros((8, 128), jnp.float32)
        for i, t in enumerate(acc[base:base + 8]):
            t = t + pltpu.roll(t, 4, 0)
            t = t + pltpu.roll(t, 2, 0)
            t = t + pltpu.roll(t, 1, 0)
            packed = jnp.where(sub == i, t, packed)
        packed = jnp.sum(packed, axis=1, keepdims=True) * (1.0 / total)
        line_row = line_row + jnp.where(lane == sub + base, packed, 0.0)
    for s in (4, 2, 1):
        line_row = line_row + pltpu.roll(line_row, s, 0)
    zero1 = jnp.zeros((1, 128), jnp.float32)
    row1[...] = line_row[0:1, :]

    def to_hub(j, index, peer):
        return pltpu.make_async_remote_copy(
            src_ref=row1, dst_ref=buf1.at[index], send_sem=s1.at[j], recv_sem=r1.at[index],
            device_id=peer, device_id_type=MESH)

    def across(j, index, peer):
        return pltpu.make_async_remote_copy(
            src_ref=row2, dst_ref=buf2.at[index], send_sem=s2.at[j], recv_sem=r2.at[index],
            device_id=peer, device_id_type=MESH)

    partner = (y, nc - 1 - c, x, z)
    for j, (yy, xx) in enumerate(plane):
        if j:
            to_hub(j, me, (yy, nc - 1, xx, z)).start()

    @pl.when(hub)
    def _():
        buf1[me] = row1[...]
        for j, (yy, xx) in enumerate(plane):
            for cc in range(nc):
                if j or cc != nc - 1:
                    to_hub(j, (cc * ny + yy) * nx + xx, partner).wait_recv()
        total1 = tree([(buf1[j], zero1) for j in range(nc * ny * nx)], add2)
        total1 = tidy(total1)
        row2[0:1, :] = total1[0]
        row2[1:2, :] = total1[1]
        k = 0
        for zz in planes:
            for cc in (nc - 1, 0):
                across(k, z, (y, cc, x, zz)).start()
                k += 1
        across(k, z, partner).start()
        buf2[z] = row2[...]

    @pl.when(jnp.logical_not(hub))
    def _():
        to_hub(0, me, partner).start()
        across(0, z, partner).wait_recv()
        to_hub(0, me, partner).wait_send()

    for zz in planes:
        across(0, zz, partner).wait_recv()
    for j in range(1, len(plane)):
        to_hub(j, me, partner).wait_send()

    @pl.when(hub)
    def _():
        for k in range(2 * len(planes) + 1):
            across(k, z, partner).wait_send()

    part = tidy(tree([(buf2[j, 0:1, :], buf2[j, 1:2, :]) for j in range(nz)], add2))

    slot = {}
    for p, (i, j) in enumerate(PAIRS):
        slot[i, j] = slot[j, i] = p
    columns = []
    for k in range(NV):
        at = jnp.full((8, 128), -1, jnp.int32)
        for i in range(NV):
            at = jnp.where(sub == i, slot[i, k], at)
        columns.append(tuple(
            jnp.broadcast_to(
                jnp.sum(jnp.where(lane == at, jnp.broadcast_to(t, (8, 128)), 0.0), axis=1, keepdims=True), (8, 128))
            for t in part))

    def spread(t, k):
        return jnp.broadcast_to(t[k:k + 1, :], (8, 128))

    def dot(a, b):
        return sublane_total(mul2(a, b))

    wide_shift = jnp.broadcast_to(shift, (8, 128))
    moved = [add2(columns[k + 1], mul1(columns[k], wide_shift)) for k in range(ITERS)]
    moved = [tidy(t) for t in moved]
    hmat = jnp.zeros((8, 128), jnp.float32)
    zeros = jnp.zeros((8, 128), jnp.float32)
    u = (jnp.where(sub == 0, -1.0, 0.0), zeros)
    e = tuple(-t for t in columns[0])
    ratio = None
    coefs, images = [], []
    for j in range(NV):
        square = dot(u, e)[0]
        square = (square if ratio is None else square * (ratio * ratio)) + FLOOR
        inv = lax.rsqrt(square)
        if j > 0:
            hmat = jnp.where((sub == j) & (lane == j - 1), square * inv, hmat)
        unit = inv if ratio is None else inv * ratio
        coefs.append(tidy(mul1(u, unit)))
        if j == ITERS:
            break
        images.append(tidy(mul1(e, unit)))
        m = tidy(add2(tuple(pltpu.roll(t, 1, 0) for t in u), mul1(u, wide_shift)))
        f = tree([mul2(moved[k], tuple(spread(t, k) for t in u)) for k in range(j + 1)], add2)
        parts = [dot(images[i], m)[0] for i in range(j)]
        own = dot(e, m)[0] * (unit * unit)
        for i in range(j):
            hmat = jnp.where((sub == i) & (lane == j), parts[i] * unit, hmat)
        hmat = jnp.where((sub == j) & (lane == j), own, hmat)
        u, e = (
            tidy(tree([x] + [mul1(basis[i], -parts[i]) for i in range(j)] + [mul1(latest, -own)], add2))
            for x, basis, latest in ((m, coefs, u), (f, images, e)))
        ratio = unit
    hm[...] = hmat
    for j in range(NV):
        cw[j] = coefs[j][0]


def output_kernel(w, cw, hm, hess_h, out_h, hess, vout, sem):
    half = w.shape[1]
    hess[...] = hm[0:NV, 0:ITERS]
    outs = [pltpu.make_async_copy(hess, hess_h, sem.at[0])]
    outs[0].start()
    for j in range(NV):
        weights = [jnp.broadcast_to(cw[j, pl.ds(i, 1), :], (8, 128)) for i in range(j + 1)]

        def combine(q, carry):
            t = tree([weights[i] * w[i, q] for i in range(j + 1)], jnp.add)
            vout[j, 2 * q] = t[0:4, :]
            vout[j, 2 * q + 1] = t[4:8, :]
            return carry

        lax.fori_loop(0, half, combine, 0, unroll=8)
        cp = pltpu.make_async_copy(vout.at[j], out_h.at[j], sem.at[j + 1])
        cp.start()
        outs.append(cp)
    for cp in outs:
        cp.wait()


def solution(mesh):
    ny, nc, nx, nz = 4, 2, 4, 8
    finer = Mesh(mesh.devices.reshape(ny, nc, nx, nz), AXES)
    gxs, gys = ("y", "c"), ("x", "z")
    sizes = (ny, nc, nx, nz)
    f32 = jnp.float32

    def body(source, initial, reaction, stiffness, line_op, face_deriv, wall_flags):
        nodes, ex, ey = source.shape
        hbm = pl.BlockSpec(memory_space=pltpu.HBM)
        scalars = pl.BlockSpec(memory_space=pltpu.SMEM)
        local = pl.BlockSpec(memory_space=pltpu.VMEM)
        vm = pltpu.VMEM
        dma = pltpu.SemaphoreType.DMA
        tile = (8, ey)
        sends = 2 + 8 + 12 + 10
        w, cw, hm = pl.pallas_call(
            functools.partial(kernel, sizes),
            out_shape=(
                pltpu.VMEM((NV, nodes // 2) + tile, f32), pltpu.VMEM((NV,) + tile, f32), pltpu.VMEM(tile, f32),
            ),
            in_specs=[hbm] * 7,
            out_specs=(local, local, local),
            scratch_shapes=[
                vm((nodes,) + tile, f32), vm((nodes,) + tile, f32), vm((nodes,) + tile, f32), vm(tile, f32),
                vm((4,) + tile, jnp.int32), vm((4,) + tile, f32),
                vm((NV - 1, nodes) + tile, f32), vm((nodes,) + tile, f32),
                vm(tile, f32), vm((4,) + tile, f32), vm((NV, 8) + tile, f32),
                vm((2, 13) + tile, f32), vm((13,) + tile, f32), vm((13,) + tile, f32),
                vm((2, 2) + tile, f32), vm((2, 2) + tile, f32), vm((2, 2) + tile, f32), vm((1, 2) + tile, f32),
                vm((2, 2) + tile, f32), vm((4, 8) + tile, f32),
                vm((1, 128), f32), vm((nc * ny * nx, 1, 128), f32), vm((2, 128), f32), vm((nz, 2, 128), f32),
                pltpu.SMEM((P_SIZE, P_SIZE), f32), pltpu.SMEM((P_SIZE,), f32),
                vm((nodes // 2,) + tile, f32), vm((2, 16) + tile, f32),
                vm((2, 8) + tile, f32), vm((2,) + tile, f32),
                dma((8,)), dma((sends,)), dma((sends,)), dma((ny * nx,)), dma((nc * ny * nx,)), dma((2 * nz - 1,)), dma((nz,)),
            ],
            compiler_params=pltpu.CompilerParams(
                collective_id=0, has_side_effects=True, vmem_limit_bytes=48 * 1024 * 1024),
            name="arnoldi",
        )(*[pltpu.with_memory_space_constraint(t, pltpu.HBM) for t in (
            line_op, face_deriv, source, initial, reaction, stiffness, wall_flags)])
        return pl.pallas_call(
            output_kernel,
            out_shape=(
                jax.ShapeDtypeStruct((NV, ITERS), f32),
                jax.ShapeDtypeStruct((NV, nodes, ex, ey), f32),
            ),
            in_specs=[local] * 3,
            out_specs=(hbm, hbm),
            scratch_shapes=[vm((NV, ITERS), f32), vm((NV, nodes, ex, ey), f32), dma((NV + 1,))],
            compiler_params=pltpu.CompilerParams(vmem_limit_bytes=16 * 1024 * 1024),
            name="combine",
        )(w, cw, hm)

    placed = (P(None, gxs, gys), P(None, gxs, gys), P(None, gxs, gys), P(gxs, gys), P(), P(), P(None, gxs, gys))
    return jax.shard_map(
        body, mesh=finer, in_specs=placed, out_specs=(P(), P(None, None, gxs, gys)), check_vma=False)
```

```python
import functools

import jax
import jax.numpy as jnp
from jax import lax
from jax.experimental import pallas as pl
from jax.experimental.pallas import tpu as pltpu
from jax.sharding import Mesh
from jax.sharding import PartitionSpec as P

P_SIZE = 8
ITERS = 5
NV = ITERS + 1
TAU = 2.0
FLOOR = 0.1
MESH = pl.DeviceIdType.MESH
AXES = ("y", "c", "x", "z")
PAIRS = [(i, j) for j in range(NV) for i in range(j + 1)]


def two_sum(a, b):
    s = a + b
    t = s - a
    return s, (a - (s - t)) + (b - t)


def split(a):
    c = a * 4097.0
    hi = c - (c - a)
    return hi, a - hi


def two_prod(a, b):
    p = a * b
    ah, al = split(a)
    bh, bl = split(b)
    return p, ((ah * bh - p) + ah * bl + al * bh) + al * bl


def add2(a, b):
    s, e = two_sum(a[0], b[0])
    return s, e + (a[1] + b[1])


def mul2(a, b):
    p, e = two_prod(a[0], b[0])
    return p, e + (a[0] * b[1] + a[1] * b[0])


def mul1(a, b):
    p, e = two_prod(a[0], b)
    return p, e + a[1] * b


def tidy(a):
    return two_sum(*a)


def tree(items, op):
    items = list(items)
    while len(items) > 1:
        nxt = [op(items[i], items[i + 1]) for i in range(0, len(items) - 1, 2)]
        if len(items) % 2:
            nxt.append(items[-1])
        items = nxt
    return items[0]


def sublane_total(a):
    for s in (4, 2, 1):
        a = add2(a, tuple(pltpu.roll(v, s, 0) for v in a))
    return tidy(a)


def kernel(sizes, line_h, fd_h, src_h, x0_h, rx_h, st_h, wf_h, wp, cw, hm,
           xl, sl, rl, stl, wfl, opl, w, rx, st, op, gw, pk, lb, rb, qs, qr, gqs, gql, gqr, qf,
           row1, buf1, row2, buf2, line, fd, rxp, cpair, xc, mm, known,
           lsem, hs, hr, s1, r1, s2, r2):
    ny, nc, nx, nz = sizes
    y, c, x, z = (lax.axis_index(a) for a in AXES)

    def at(dx, dy):
        i = lax.rem(y * nc + c + ny * nc + dx, ny * nc)
        j = lax.rem(x * nz + z + nx * nz + dy, nx * nz)
        return (i // nc, lax.rem(i, nc), j // nz, lax.rem(j, nz))

    hub = c == nc - 1
    plane = [(lax.rem(y + i, ny), lax.rem(x + k, nx)) for i in range(ny) for k in range(nx)]
    planes = [lax.rem(z + k, nz) for k in range(1, nz)]
    me = (c * ny + y) * nx + x
    around = {(i, j): at(i, j) for i in (-1, 0, 1) for j in (-1, 0, 1) if (i, j) != (0, 0)}
    own = pl.ds(0, 4)
    pairs = [(line_h, line), (fd_h, fd), (x0_h, xl.at[:, own, :]), (rx_h, rl.at[:, own, :]), (src_h, sl.at[:, own, :]), (st_h, stl.at[own, :]),
             (wf_h, wfl.at[:, own, :]), (rx_h, rx.at[:, own, :])]
    loads = [pltpu.make_async_copy(a, b, lsem.at[i]) for i, (a, b) in enumerate(pairs)]
    for cp in loads:
        cp.start()

    barrier = pltpu.get_barrier_semaphore()

    def greet(peer):
        pl.semaphore_signal(barrier, inc=1, device_id=peer, device_id_type=MESH)

    far = sorted(range(1, nz), key=lambda k: -min(k, nz - k))
    flat = sorted(range(1, ny * nx), key=lambda i: -min(i // nx, ny - i // nx) - min(i % nx, nx - i % nx))
    partner = (y, nc - 1 - c, x, z)
    lines = {
        "y": [(lax.rem(y + i, ny), c, x, z) for i in (1, ny - 1)],
        "x": [(y, c, lax.rem(x + i, nx), z) for i in (1, nx - 1)],
        "z": [(y, c, x, lax.rem(z + i, nz)) for i in (1, nz - 1)],
    }
    greeted = lines["y"] + lines["x"] + lines["z"] + list(around.values()) + [partner]
    for peer in greeted:
        greet(peer)

    def tell(first, axes):
        for i, axis in enumerate(axes):
            for peer in lines[axis]:
                pl.semaphore_signal(known.at[first + i], inc=1, device_id=peer, device_id_type=MESH)

    def hear(first, axes):
        for i in range(len(axes)):
            pl.semaphore_wait(known.at[first + i], 2)

    for cp in loads[:2]:
        cp.wait()
    n = P_SIZE
    total = float(ny * nc * nx * nz * src_h.shape[0] * src_h.shape[1] * src_h.shape[2])
    lop = [[line[i, j] for j in range(n)] for i in range(n)]
    g = [0.5 * fd[i] + (TAU if i == 0 else 0.0) for i in range(n)]
    diag = lop[0][0]
    for i in range(1, n):
        diag = diag + lop[i][i]
    shift = 3.0 + 0.3125 * diag + 0.25 * fd[0]

    lane = lax.broadcasted_iota(jnp.int32, (8, 128), 1)
    sub = lax.broadcasted_iota(jnp.int32, (8, 128), 0)
    group = lane // 16
    slot16 = lax.rem(lane, 16)

    def lroll(t, s):
        s = s % 128
        return t if s == 0 else pltpu.roll(t, s, 1)

    def gather_groups(items, s):
        out = lroll(items[0], s)
        for a in range(1, len(items)):
            out = jnp.where(group == a, lroll(items[a], 16 * a + s), out)
        return out

    cline, cface = [], []
    for k in range(n):
        t = jnp.zeros((8, 128), jnp.float32)
        for a in range(n):
            t = jnp.where(group == a, lop[a][(a - k) % n], t)
        cline.append(t)
        cface.append(jnp.where(group == 0, g[(n - k) % n], jnp.where(group == n - 1, g[k], 0.0)))

    def x_faces(v):
        qw = [tree([g[i] * v(i, b) for i in range(n)], jnp.add) for b in range(n)]
        qe = [tree([g[i] * v(n - 1 - i, b) for i in range(n)], jnp.add) for b in range(n)]
        return qw, qe

    def strip_faces(t):
        rolled = [t] + [lroll(t, 16 * k) for k in range(1, n)]
        return rolled, tree([cface[k] * rolled[k] for k in range(n)], jnp.add)

    for cp in loads[2:7]:
        cp.wait()
    opl[...] = 1.0 - wfl[...].astype(jnp.float32)
    qw, qe = x_faces(lambda a, b: xl[a * n + b])
    qsouth = [tree([g[i] * xl[a * n + i] for i in range(n)], jnp.add) for a in range(n)]
    qnorth = [tree([g[i] * xl[a * n + n - 1 - i] for i in range(n)], jnp.add) for a in range(n)]
    for b in range(n):
        qs[0, 0, pl.ds(b, 1), :] = qw[b][0:1, :]
        qs[0, 1, pl.ds(b, 1), :] = qe[b][3:4, :]
        gqs[0, 0, pl.ds(b, 1), :] = qw[b][2:3, :]
        gqs[0, 1, pl.ds(b, 1), :] = qe[b][1:2, :]
        xc[0, b] = pltpu.roll(qe[b], 1, 0)
        xc[1, b] = pltpu.roll(qw[b], 7, 0)
    mm[0, 0:4, :] = gather_groups(qnorth, 7)[0:4, :]
    mm[1, 0:4, :] = gather_groups(qsouth, 5)[0:4, :]
    for b in range(n):
        px = gather_groups([xl[a * n + b] for a in range(n)], 6)
        ps = gather_groups([sl[a * n + b] for a in range(n)], 6)
        pr = gather_groups([rl[a * n + b] for a in range(n)], 6)
        pk[0, b] = jnp.where(slot16 < 6, px, jnp.where(slot16 < 11, lroll(ps, 5), lroll(pr, 10)))
        pk[1, b] = jnp.where(slot16 < 6, lroll(px, -6), jnp.where(slot16 < 11, ps, lroll(pr, 5)))
    gqs[0, 0] = lroll(gqs[0, 0], 6)
    gqs[0, 1] = lroll(gqs[0, 1], 118)
    for f, t in enumerate([stl[...]] + [opl[i] for i in range(4)]):
        spread_out = gather_groups([t] * n, 6)
        pk[0, n + f] = spread_out
        pk[1, n + f] = spread_out
    pl.semaphore_wait(barrier, len(greeted))
    tell(0, "yz")

    def send(copies, peer, pieces, first):
        for i, (a, b) in enumerate(pieces):
            cp = pltpu.make_async_remote_copy(
                src_ref=a, dst_ref=b, send_sem=hs.at[first + i], recv_sem=hr.at[first + i],
                device_id=peer, device_id_type=MESH)
            cp.start()
            copies.append(cp)
        return first + len(pieces)

    def rows(lo):
        return pl.ds(lo, 2)

    copies, used = [], 0
    for dy, k, dst in ((1, 0, lb), (-1, 1, rb)):
        used = send(copies, around[0, dy], [(pk.at[k, :, own, :], dst.at[:, own, :])], used)
    for dy, k, dst, gq in ((1, 0, lb, gql), (-1, 1, rb, gqr)):
        for dx, lo, to in ((1, 2, 6), (-1, 0, 4)):
            side = 1 if dx > 0 else 0
            used = send(copies, around[dx, dy], [
                (pk.at[k, :, rows(lo), :], dst.at[:, rows(to), :]), (gqs.at[0, side], gq.at[0, side])], used)
    for dx, lo, to in ((1, 2, 6), (-1, 0, 4)):
        side = 1 if dx > 0 else 0
        used = send(copies, around[dx, 0], [
            (rl.at[:, rows(lo), :], rx.at[:, rows(to), :]),
            (mm.at[:, rows(lo), :], mm.at[:, rows(to), :]),
            (stl.at[rows(lo), :], st.at[rows(to), :]),
            (opl.at[:, rows(lo), :], op.at[:, rows(to), :]),
            (qs.at[0, side], qr.at[0, side])], used)
    for b in range(n):
        qf[0, b] = qw[b] - opl[0] * jnp.where(sub == 0, 0.0, xc[0, b])
        qf[1, b] = qe[b] - opl[1] * jnp.where(sub == 3, 0.0, xc[1, b])
    for a in range(n):
        qf[2, a] = qsouth[a] - opl[2] * jnp.where(lane == 0, 0.0, lroll(qnorth[a], 1))
        qf[3, a] = qnorth[a] - opl[3] * jnp.where(lane == 127, 0.0, lroll(qsouth[a], -1))
    for a in range(n):
        row = [xl[a * n + i] for i in range(n)]
        for b in range(n):
            acc = tree([lop[b][i] * row[i] for i in range(n)] + [lop[a][i] * xl[i * n + b] for i in range(n)], jnp.add)
            t = rl[a * n + b] * row[b] - sl[a * n + b] + stl[...] * acc
            for edge, f, i in ((a == 0, 0, b), (a == n - 1, 1, b), (b == 0, 2, a), (b == n - 1, 3, a)):
                if edge:
                    t = t + qf[f, i]
            w[0, a * n + b, 0:4, :] = t[0:4, :]
    for dx, lo, to in ((1, 2, 6), (-1, 0, 4)):
        used = send(copies, around[dx, 0], [(w.at[0, :, rows(lo), :], w.at[0, :, rows(to), :])], used)
    st[0:4, :] = stl[0:4, :]
    op[:, 0:4, :] = opl[:, 0:4, :]
    for q in range(0, n * n, 2):
        rxp[q // 2] = jnp.where(sub < 4, rl[q], pltpu.roll(rl[q + 1], 4, 0)) - shift
    for cp in loads[7:]:
        cp.wait()
    hear(0, "yz")
    tell(2, "xz")
    for cp in copies:
        cp.wait()

    before_half = slot16 < 6
    gsv, grx = [], []
    for b in range(n):
        lo, hi = lb[b], rb[b]
        gw[0, b] = jnp.where(before_half, lo, lroll(hi, 6))
        gsv.append(jnp.where(before_half, lroll(lo, -5), hi))
        grx.append(jnp.where(before_half, lroll(lo, -10), lroll(hi, -5)))
    spreads = [jnp.where(before_half, lb[n + f], rb[n + f]) for f in range(5)]
    gst = spreads[0]
    gopw = jnp.where(group == 0, spreads[1], 0.0)
    gope = jnp.where(group == n - 1, spreads[2], 0.0)
    gops, gopn = spreads[3], spreads[4]
    for side in (0, 1):
        gqr[0, side] = jnp.where(before_half, gql[0, side], gqr[0, side])

    low = sub < 4
    for j in range(n // 2):
        for i in range(n // 2):
            cpair[0, j * 4 + i] = jnp.where(low, lop[2 * j][2 * i], lop[2 * j + 1][2 * i + 1])
            cpair[1, j * 4 + i] = jnp.where(low, lop[2 * j][2 * i + 1], lop[2 * j + 1][2 * i])

    def pair_up(even, odd):
        return jnp.where(low, even, pltpu.roll(odd, 4, 0))

    def apply(k, last=False, fresh=None, after_strip=None, after_half=None):
        wide = k != 2

        def v(a, b):
            return w[k - 1, a * n + b]

        gv = [gw[k, b] for b in range(n)]
        gqsouth = tree([g[i] * gv[i] for i in range(n)], jnp.add)
        gqnorth = tree([g[i] * gv[n - 1 - i] for i in range(n)], jnp.add)
        if k:
            qsouth = [tree([g[i] * v(a, i) for i in range(n)], jnp.add) for a in range(n)]
            qnorth = [tree([g[i] * v(a, n - 1 - i) for i in range(n)], jnp.add) for a in range(n)]
        for a in range(n):
            below = jnp.where(lane == 0, lroll(gqnorth, -(16 * a + 5)), lroll(qnorth[a], 1) if k else 0.0)
            above = jnp.where(lane == 127, lroll(gqsouth, 121 - 16 * a), lroll(qsouth[a], -1) if k else 0.0)
            qf[2, a] = qsouth[a] - op[2] * below if k else -op[2] * below
            qf[3, a] = qnorth[a] - op[3] * above if k else -op[3] * above
        if not last:
            mn = gather_groups(qnorth, 7) if k else mm[0]
            ms = gather_groups(qsouth, 5) if k else mm[1]
            sterm = gqsouth - gops * jnp.where(slot16 == 6, mn, lroll(gqnorth, 1))
            nterm = gqnorth - gopn * jnp.where(slot16 == 5, ms, lroll(gqsouth, -1))
            for b in range(n):
                rolled, face = strip_faces(gv[b])
                prev = pltpu.roll(lroll(face, 16), 1, 0)
                nxt = pltpu.roll(lroll(face, -16), 7, 0)
                if fresh is not None:
                    prev = jnp.where(sub == 6, jnp.broadcast_to(lroll(gqr[fresh, 1, pl.ds(b, 1), :], 16), (8, 128)), prev)
                    nxt = jnp.where(sub == 5, jnp.broadcast_to(lroll(gqr[fresh, 0, pl.ds(b, 1), :], -16), (8, 128)), nxt)
                acc = tree([cline[i] * rolled[i] for i in range(n)] + [lop[b][i] * gv[i] for i in range(n)], jnp.add)
                t = grx[b] * gv[b] + gst * acc + (face - (gopw * prev + gope * nxt))
                if b == 0:
                    t = t + sterm
                if b == n - 1:
                    t = t + nterm
                t = t - (gsv[b] if k == 0 else shift * gv[b])
                if wide:
                    gw[k + 1, b] = t
                else:
                    gw[k + 1, b, 0:4, :] = t[0:4, :]
            if after_strip is not None:
                after_strip()
        if k == 0:
            for b in range(n):
                prev = jnp.where(sub == 4, xc[0, b], 0.0)
                nxt = jnp.where(sub == 7, xc[1, b], 0.0)
                prev = jnp.where(sub == 0, jnp.broadcast_to(qr[0, 1, pl.ds(b, 1), :], (8, 128)), prev)
                nxt = jnp.where(sub == 3, jnp.broadcast_to(qr[0, 0, pl.ds(b, 1), :], (8, 128)), nxt)
                qf[0, b] = -op[0] * prev
                qf[1, b] = -op[1] * nxt
            for a in range(n):
                for b in range(n):
                    t = w[0, a * n + b]
                    edges = ((a == 0, 0, b), (a == n - 1, 1, b), (b == 0, 2, a), (b == n - 1, 3, a))
                    for edge, f, i in edges:
                        if edge:
                            t = t + qf[f, i]
                    if any(edge for edge, f, i in edges):
                        w[0, a * n + b] = t
                    if b % 2 == 0:
                        even = t
                    else:
                        wp[0, (a * n + b) // 2] = pair_up(even, t)
            return
        for b in range(n):
            qwest = tree([g[i] * v(i, b) for i in range(n)], jnp.add)
            qeast = tree([g[i] * v(n - 1 - i, b) for i in range(n)], jnp.add)
            prev = pltpu.roll(qeast, 1, 0)
            nxt = pltpu.roll(qwest, 7, 0)
            if fresh is not None:
                prev = jnp.where(sub == 6, jnp.broadcast_to(qr[fresh, 1, pl.ds(b, 1), :], (8, 128)), prev)
                nxt = jnp.where(sub == 5, jnp.broadcast_to(qr[fresh, 0, pl.ds(b, 1), :], (8, 128)), nxt)
            qf[0, b] = qwest - op[0] * prev
            qf[1, b] = qeast - op[1] * nxt
        if not wide or last:
            stiff = pair_up(st[...], st[...])
            for a in range(n):
                tiles = [wp[k - 1, a * 4 + j] for j in range(4)]
                swapped = [pltpu.roll(t, 4, 0) for t in tiles]
                for j in range(4):
                    q = a * n + 2 * j
                    acc = tree([lop[a][i] * wp[k - 1, i * 4 + j] for i in range(n)]
                               + [cpair[0, j * 4 + i] * tiles[i] for i in range(4)]
                               + [cpair[1, j * 4 + i] * swapped[i] for i in range(4)], jnp.add)
                    t = rxp[q // 2] * tiles[j] + stiff * acc
                    if a == 0:
                        t = t + pair_up(qf[0, 2 * j], qf[0, 2 * j + 1])
                    if a == n - 1:
                        t = t + pair_up(qf[1, 2 * j], qf[1, 2 * j + 1])
                    if j == 0:
                        t = t + jnp.where(low, qf[2, a], 0.0)
                    if j == 3:
                        t = t + jnp.where(low, 0.0, pltpu.roll(qf[3, a], 4, 0))
                    wp[k, q // 2] = t
                    if not last:
                        w[k, q, 0:4, :] = t[0:4, :]
                        w[k, q + 1, 0:4, :] = pltpu.roll(t, 4, 0)[0:4, :]
                if a == 3 and after_half is not None:
                    after_half()
            return
        stiff = st[...]
        for a in range(n):
            row = [v(a, i) for i in range(n)]
            even = None
            for b in range(n):
                acc = tree([lop[b][i] * row[i] for i in range(n)] + [lop[a][i] * v(i, b) for i in range(n)], jnp.add)
                t = (rx[a * n + b] - shift) * row[b] + stiff * acc
                if a == 0:
                    t = t + qf[0, b]
                if a == n - 1:
                    t = t + qf[1, b]
                if b == 0:
                    t = t + qf[2, a]
                if b == n - 1:
                    t = t + qf[3, a]
                w[k, a * n + b] = t
                if b % 2 == 0:
                    even = t
                else:
                    wp[k, (a * n + b) // 2] = pair_up(even, t)

    apply(0, fresh=0)
    apply(1)
    hear(2, "xz")
    tell(4, "xz")
    copies = []
    sides = ((1, 2, 6), (-1, 0, 4))

    def send_strip():
        nonlocal used
        for b in range(n):
            t = jnp.concatenate([gw[3, b, 0:4, :]] * 2, axis=0)
            face = strip_faces(t)[1]
            gqs[1, 0, pl.ds(b, 1), :] = face[2:3, :]
            gqs[1, 1, pl.ds(b, 1), :] = face[1:2, :]
        for dx, lo, to in sides:
            side = 1 if dx > 0 else 0
            used = send(copies, around[dx, 0], [
                (gw.at[3, :, rows(lo), :], gw.at[3, :, rows(to), :]), (gqs.at[1, side], gqr.at[1, side])], used)

    def send_block(first):
        nonlocal used
        part = pl.ds(first, n * n // 2)
        for dx, lo, to in sides:
            used = send(copies, around[dx, 0], [(w.at[2, part, rows(lo), :], w.at[2, part, rows(to), :])], used)

    apply(2, after_strip=send_strip, after_half=lambda: send_block(0))
    send_block(n * n // 2)
    qw, qe = x_faces(lambda a, b: w[2, a * n + b, 0:4, :])
    for b in range(n):
        qs[1, 0, pl.ds(b, 1), :] = qw[b][2:3, :]
        qs[1, 1, pl.ds(b, 1), :] = qe[b][1:2, :]
    for dx, lo, to in sides:
        side = 1 if dx > 0 else 0
        used = send(copies, around[dx, 0], [(qs.at[1, side], qr.at[1, side])], used)
    def gram(pairs):
        top = max(j for i, j in pairs) + 1

        def body(q, acc):
            vals = [wp[i, q] for i in range(top)]
            return tuple(t + vals[i] * vals[j] for t, (i, j) in zip(acc, pairs))

        return lax.fori_loop(0, n * n // 2, body, tuple(jnp.zeros((8, 128), jnp.float32) for _ in pairs), unroll=8)

    early = [p for p in PAIRS if p[1] < 3]
    first = gram(early)
    hear(4, "xz")
    pl.semaphore_signal(known.at[6], inc=1, device_id=partner, device_id_type=MESH)
    for cp in copies:
        cp.wait()
    apply(3, fresh=1)
    apply(4)
    apply(5, last=True)

    acc = first + gram(PAIRS[len(early):])
    line_row = jnp.zeros((8, 128), jnp.float32)
    for base in range(0, len(PAIRS), 8):
        packed = jnp.zeros((8, 128), jnp.float32)
        for i, t in enumerate(acc[base:base + 8]):
            t = t + pltpu.roll(t, 4, 0)
            t = t + pltpu.roll(t, 2, 0)
            t = t + pltpu.roll(t, 1, 0)
            packed = jnp.where(sub == i, t, packed)
        packed = jnp.sum(packed, axis=1, keepdims=True) * (1.0 / total)
        line_row = line_row + jnp.where(lane == sub + base, packed, 0.0)
    for s in (4, 2, 1):
        line_row = line_row + pltpu.roll(line_row, s, 0)
    zero1 = jnp.zeros((1, 128), jnp.float32)
    row1[...] = line_row[0:1, :]

    def to_hub(j, index, peer):
        return pltpu.make_async_remote_copy(
            src_ref=row1, dst_ref=buf1.at[index], send_sem=s1.at[j], recv_sem=r1.at[index],
            device_id=peer, device_id_type=MESH)

    def across(j, index, peer):
        return pltpu.make_async_remote_copy(
            src_ref=row2, dst_ref=buf2.at[index], send_sem=s2.at[j], recv_sem=r2.at[index],
            device_id=peer, device_id_type=MESH)

    pl.semaphore_wait(known.at[6], 1)
    for j in flat:
        to_hub(j, me, (plane[j][0], nc - 1, plane[j][1], z)).start()

    @pl.when(hub)
    def _():
        buf1[me] = row1[...]
        for j, (yy, xx) in enumerate(plane):
            for cc in range(nc):
                if j or cc != nc - 1:
                    to_hub(j, (cc * ny + yy) * nx + xx, partner).wait_recv()
        total1 = tree([(buf1[j], zero1) for j in range(nc * ny * nx)], add2)
        total1 = tidy(total1)
        row2[0:1, :] = total1[0]
        row2[1:2, :] = total1[1]
        for cc in (nc - 1, 0):
            for k in far:
                across(cc * len(planes) + k - 1, z, (y, cc, x, planes[k - 1])).start()
        across(2 * len(planes), z, partner).start()
        buf2[z] = row2[...]

    @pl.when(jnp.logical_not(hub))
    def _():
        to_hub(0, me, partner).start()
        across(0, z, partner).wait_recv()
        to_hub(0, me, partner).wait_send()

    for zz in planes:
        across(0, zz, partner).wait_recv()
    for j in range(1, len(plane)):
        to_hub(j, me, partner).wait_send()

    @pl.when(hub)
    def _():
        for k in range(2 * len(planes) + 1):
            across(k, z, partner).wait_send()

    part = tidy(tree([(buf2[j, 0:1, :], buf2[j, 1:2, :]) for j in range(nz)], add2))

    slot = {}
    for p, (i, j) in enumerate(PAIRS):
        slot[i, j] = slot[j, i] = p
    columns = []
    for k in range(NV):
        at = jnp.full((8, 128), -1, jnp.int32)
        for i in range(NV):
            at = jnp.where(sub == i, slot[i, k], at)
        columns.append(tuple(
            jnp.broadcast_to(
                jnp.sum(jnp.where(lane == at, jnp.broadcast_to(t, (8, 128)), 0.0), axis=1, keepdims=True), (8, 128))
            for t in part))

    def spread(t, k):
        return jnp.broadcast_to(t[k:k + 1, :], (8, 128))

    def dot(a, b):
        return sublane_total(mul2(a, b))

    wide_shift = jnp.broadcast_to(shift, (8, 128))
    moved = [add2(columns[k + 1], mul1(columns[k], wide_shift)) for k in range(ITERS)]
    moved = [tidy(t) for t in moved]
    hmat = jnp.zeros((8, 128), jnp.float32)
    zeros = jnp.zeros((8, 128), jnp.float32)
    u = (jnp.where(sub == 0, -1.0, 0.0), zeros)
    e = tuple(-t for t in columns[0])
    ratio = None
    coefs, images = [], []
    for j in range(NV):
        square = dot(u, e)[0]
        square = (square if ratio is None else square * (ratio * ratio)) + FLOOR
        inv = lax.rsqrt(square)
        if j > 0:
            hmat = jnp.where((sub == j) & (lane == j - 1), square * inv, hmat)
        unit = inv if ratio is None else inv * ratio
        coefs.append(tidy(mul1(u, unit)))
        if j == ITERS:
            break
        images.append(tidy(mul1(e, unit)))
        m = tidy(add2(tuple(pltpu.roll(t, 1, 0) for t in u), mul1(u, wide_shift)))
        f = tree([mul2(moved[k], tuple(spread(t, k) for t in u)) for k in range(j + 1)], add2)
        parts = [dot(images[i], m)[0] for i in range(j)]
        own = dot(e, m)[0] * (unit * unit)
        for i in range(j):
            hmat = jnp.where((sub == i) & (lane == j), parts[i] * unit, hmat)
        hmat = jnp.where((sub == j) & (lane == j), own, hmat)
        u, e = (
            tidy(tree([x] + [mul1(basis[i], -parts[i]) for i in range(j)] + [mul1(latest, -own)], add2))
            for x, basis, latest in ((m, coefs, u), (f, images, e)))
        ratio = unit
    hm[...] = hmat
    for j in range(NV):
        cw[j] = coefs[j][0]


def output_kernel(w, cw, hm, hess_h, out_h, hess, vout, sem):
    half = w.shape[1]
    hess[...] = hm[0:NV, 0:ITERS]
    outs = [pltpu.make_async_copy(hess, hess_h, sem.at[0])]
    outs[0].start()
    for j in range(NV):
        weights = [jnp.broadcast_to(cw[j, pl.ds(i, 1), :], (8, 128)) for i in range(j + 1)]

        def combine(q, carry):
            t = tree([weights[i] * w[i, q] for i in range(j + 1)], jnp.add)
            vout[j, 2 * q] = t[0:4, :]
            vout[j, 2 * q + 1] = t[4:8, :]
            return carry

        lax.fori_loop(0, half, combine, 0, unroll=8)
        cp = pltpu.make_async_copy(vout.at[j], out_h.at[j], sem.at[j + 1])
        cp.start()
        outs.append(cp)
    for cp in outs:
        cp.wait()


def solution(mesh):
    ny, nc, nx, nz = 4, 2, 4, 8
    finer = Mesh(mesh.devices.reshape(ny, nc, nx, nz), AXES)
    gxs, gys = ("y", "c"), ("x", "z")
    sizes = (ny, nc, nx, nz)
    f32 = jnp.float32

    def body(source, initial, reaction, stiffness, line_op, face_deriv, wall_flags):
        nodes, ex, ey = source.shape
        hbm = pl.BlockSpec(memory_space=pltpu.HBM)
        scalars = pl.BlockSpec(memory_space=pltpu.SMEM)
        local = pl.BlockSpec(memory_space=pltpu.VMEM)
        vm = pltpu.VMEM
        dma = pltpu.SemaphoreType.DMA
        tile = (8, ey)
        sends = 2 + 8 + 12 + 10
        w, cw, hm = pl.pallas_call(
            functools.partial(kernel, sizes),
            out_shape=(
                pltpu.VMEM((NV, nodes // 2) + tile, f32), pltpu.VMEM((NV,) + tile, f32), pltpu.VMEM(tile, f32),
            ),
            in_specs=[hbm] * 7,
            out_specs=(local, local, local),
            scratch_shapes=[
                vm((nodes,) + tile, f32), vm((nodes,) + tile, f32), vm((nodes,) + tile, f32), vm(tile, f32),
                vm((4,) + tile, jnp.int32), vm((4,) + tile, f32),
                vm((NV - 1, nodes) + tile, f32), vm((nodes,) + tile, f32),
                vm(tile, f32), vm((4,) + tile, f32), vm((NV, 8) + tile, f32),
                vm((2, 13) + tile, f32), vm((13,) + tile, f32), vm((13,) + tile, f32),
                vm((2, 2) + tile, f32), vm((2, 2) + tile, f32), vm((2, 2) + tile, f32), vm((1, 2) + tile, f32),
                vm((2, 2) + tile, f32), vm((4, 8) + tile, f32),
                vm((1, 128), f32), vm((nc * ny * nx, 1, 128), f32), vm((2, 128), f32), vm((nz, 2, 128), f32),
                pltpu.SMEM((P_SIZE, P_SIZE), f32), pltpu.SMEM((P_SIZE,), f32),
                vm((nodes // 2,) + tile, f32), vm((2, 16) + tile, f32),
                vm((2, 8) + tile, f32), vm((2,) + tile, f32), pltpu.SemaphoreType.REGULAR((7,)),
                dma((8,)), dma((sends,)), dma((sends,)), dma((ny * nx,)), dma((nc * ny * nx,)), dma((2 * nz - 1,)), dma((nz,)),
            ],
            compiler_params=pltpu.CompilerParams(
                collective_id=0, has_side_effects=True, vmem_limit_bytes=48 * 1024 * 1024),
            name="arnoldi",
        )(*[pltpu.with_memory_space_constraint(t, pltpu.HBM) for t in (
            line_op, face_deriv, source, initial, reaction, stiffness, wall_flags)])
        return pl.pallas_call(
            output_kernel,
            out_shape=(
                jax.ShapeDtypeStruct((NV, ITERS), f32),
                jax.ShapeDtypeStruct((NV, nodes, ex, ey), f32),
            ),
            in_specs=[local] * 3,
            out_specs=(hbm, hbm),
            scratch_shapes=[vm((NV, ITERS), f32), vm((NV, nodes, ex, ey), f32), dma((NV + 1,))],
            compiler_params=pltpu.CompilerParams(vmem_limit_bytes=16 * 1024 * 1024),
            name="combine",
        )(w, cw, hm)

    placed = (P(None, gxs, gys), P(None, gxs, gys), P(None, gxs, gys), P(gxs, gys), P(), P(), P(None, gxs, gys))
    return jax.shard_map(
        body, mesh=finer, in_specs=placed, out_specs=(P(), P(None, None, gxs, gys)), check_vma=False)
```

```python
import functools

import jax
import jax.numpy as jnp
from jax import lax
from jax.experimental import pallas as pl
from jax.experimental.pallas import tpu as pltpu
from jax.sharding import Mesh
from jax.sharding import PartitionSpec as P

P_SIZE = 8
ITERS = 5
NV = ITERS + 1
TAU = 2.0
FLOOR = 0.1
MESH = pl.DeviceIdType.MESH
AXES = ("y", "c", "x", "z")
PAIRS = [(i, j) for j in range(NV) for i in range(j + 1)]


def two_sum(a, b):
    s = a + b
    t = s - a
    return s, (a - (s - t)) + (b - t)


def split(a):
    c = a * 4097.0
    hi = c - (c - a)
    return hi, a - hi


def two_prod(a, b):
    p = a * b
    ah, al = split(a)
    bh, bl = split(b)
    return p, ((ah * bh - p) + ah * bl + al * bh) + al * bl


def add2(a, b):
    s, e = two_sum(a[0], b[0])
    return s, e + (a[1] + b[1])


def mul2(a, b):
    p, e = two_prod(a[0], b[0])
    return p, e + (a[0] * b[1] + a[1] * b[0])


def mul1(a, b):
    p, e = two_prod(a[0], b)
    return p, e + a[1] * b


def tidy(a):
    return two_sum(*a)


def tree(items, op):
    items = list(items)
    while len(items) > 1:
        nxt = [op(items[i], items[i + 1]) for i in range(0, len(items) - 1, 2)]
        if len(items) % 2:
            nxt.append(items[-1])
        items = nxt
    return items[0]


def sublane_total(a):
    for s in (4, 2, 1):
        a = add2(a, tuple(pltpu.roll(v, s, 0) for v in a))
    return tidy(a)


def kernel(sizes, line_h, fd_h, src_h, x0_h, rx_h, st_h, wf_h, wp, cw, hm,
           xl, sl, rl, stl, wfl, opl, w, rx, st, op, gw, pk, lb, rb, qs, qr, gqs, gql, gqr, qf,
           row1, buf1, row2, buf2, line, fd, rxp, cpair, xc, mm, known,
           lsem, hs, hr, s1, r1, s2, r2):
    ny, nc, nx, nz = sizes
    y, c, x, z = (lax.axis_index(a) for a in AXES)

    def at(dx, dy):
        i = lax.rem(y * nc + c + ny * nc + dx, ny * nc)
        j = lax.rem(x * nz + z + nx * nz + dy, nx * nz)
        return (i // nc, lax.rem(i, nc), j // nz, lax.rem(j, nz))

    hub = c == nc - 1
    plane = [(lax.rem(y + i, ny), lax.rem(x + k, nx)) for i in range(ny) for k in range(nx)]
    planes = [lax.rem(z + k, nz) for k in range(1, nz)]
    me = (c * ny + y) * nx + x
    around = {(i, j): at(i, j) for i in (-1, 0, 1) for j in (-1, 0, 1) if (i, j) != (0, 0)}
    own = pl.ds(0, 4)
    pairs = [(line_h, line), (fd_h, fd), (x0_h, xl.at[:, own, :]), (rx_h, rl.at[:, own, :]), (src_h, sl.at[:, own, :]), (st_h, stl.at[own, :]),
             (wf_h, wfl.at[:, own, :]), (rx_h, rx.at[:, own, :])]
    loads = [pltpu.make_async_copy(a, b, lsem.at[i]) for i, (a, b) in enumerate(pairs)]
    for cp in loads:
        cp.start()

    barrier = pltpu.get_barrier_semaphore()

    def greet(peer):
        pl.semaphore_signal(barrier, inc=1, device_id=peer, device_id_type=MESH)

    far = sorted(range(1, nz), key=lambda k: -min(k, nz - k))
    flat = sorted(range(1, ny * nx), key=lambda i: -min(i // nx, ny - i // nx) - min(i % nx, nx - i % nx))
    partner = (y, nc - 1 - c, x, z)
    lines = {
        "y": [(lax.rem(y + i, ny), c, x, z) for i in (1, ny - 1)],
        "x": [(y, c, lax.rem(x + i, nx), z) for i in (1, nx - 1)],
        "z": [(y, c, x, lax.rem(z + i, nz)) for i in (1, nz - 1)],
    }
    greeted = lines["y"] + lines["x"] + lines["z"] + list(around.values()) + [partner]
    for peer in greeted:
        greet(peer)

    def tell(first, axes):
        for i, axis in enumerate(axes):
            for peer in lines[axis]:
                pl.semaphore_signal(known.at[first + i], inc=1, device_id=peer, device_id_type=MESH)

    def hear(first, axes):
        for i in range(len(axes)):
            pl.semaphore_wait(known.at[first + i], 2)

    for cp in loads[:2]:
        cp.wait()
    n = P_SIZE
    total = float(ny * nc * nx * nz * src_h.shape[0] * src_h.shape[1] * src_h.shape[2])
    lop = [[line[i, j] for j in range(n)] for i in range(n)]
    g = [0.5 * fd[i] + (TAU if i == 0 else 0.0) for i in range(n)]
    diag = lop[0][0]
    for i in range(1, n):
        diag = diag + lop[i][i]
    shift = 3.0 + 0.3125 * diag + 0.25 * fd[0]

    lane = lax.broadcasted_iota(jnp.int32, (8, 128), 1)
    sub = lax.broadcasted_iota(jnp.int32, (8, 128), 0)
    group = lane // 16
    slot16 = lax.rem(lane, 16)

    def lroll(t, s):
        s = s % 128
        return t if s == 0 else pltpu.roll(t, s, 1)

    def gather_groups(items, s):
        out = lroll(items[0], s)
        for a in range(1, len(items)):
            out = jnp.where(group == a, lroll(items[a], 16 * a + s), out)
        return out

    cline, cface = [], []
    for k in range(n):
        t = jnp.zeros((8, 128), jnp.float32)
        for a in range(n):
            t = jnp.where(group == a, lop[a][(a - k) % n], t)
        cline.append(t)
        cface.append(jnp.where(group == 0, g[(n - k) % n], jnp.where(group == n - 1, g[k], 0.0)))

    def x_faces(v):
        qw = [tree([g[i] * v(i, b) for i in range(n)], jnp.add) for b in range(n)]
        qe = [tree([g[i] * v(n - 1 - i, b) for i in range(n)], jnp.add) for b in range(n)]
        return qw, qe

    def strip_faces(t):
        rolled = [t] + [lroll(t, 16 * k) for k in range(1, n)]
        return rolled, tree([cface[k] * rolled[k] for k in range(n)], jnp.add)

    for cp in loads[2:7]:
        cp.wait()
    opl[...] = 1.0 - wfl[...].astype(jnp.float32)
    qw, qe = x_faces(lambda a, b: xl[a * n + b])
    for b in range(n):
        qs[0, 0, pl.ds(b, 1), :] = qw[b][0:1, :]
        qs[0, 1, pl.ds(b, 1), :] = qe[b][3:4, :]
        gqs[0, 0, pl.ds(b, 1), :] = qw[b][2:3, :]
        gqs[0, 1, pl.ds(b, 1), :] = qe[b][1:2, :]
        xc[0, b] = pltpu.roll(qe[b], 1, 0)
        xc[1, b] = pltpu.roll(qw[b], 7, 0)
    for b in range(n):
        px = gather_groups([xl[a * n + b] for a in range(n)], 6)
        ps = gather_groups([sl[a * n + b] for a in range(n)], 6)
        pr = gather_groups([rl[a * n + b] for a in range(n)], 6)
        pk[0, b] = jnp.where(slot16 < 6, px, jnp.where(slot16 < 11, lroll(ps, 5), lroll(pr, 10)))
        pk[1, b] = jnp.where(slot16 < 6, lroll(px, -6), jnp.where(slot16 < 11, ps, lroll(pr, 5)))
    gqs[0, 0] = lroll(gqs[0, 0], 6)
    gqs[0, 1] = lroll(gqs[0, 1], 118)
    for f, t in enumerate([stl[...]] + [opl[i] for i in range(4)]):
        spread_out = gather_groups([t] * n, 6)
        pk[0, n + f] = spread_out
        pk[1, n + f] = spread_out
    pl.semaphore_wait(barrier, len(greeted))
    tell(0, "yz")

    def send(copies, peer, pieces, first):
        for i, (a, b) in enumerate(pieces):
            cp = pltpu.make_async_remote_copy(
                src_ref=a, dst_ref=b, send_sem=hs.at[first + i], recv_sem=hr.at[first + i],
                device_id=peer, device_id_type=MESH)
            cp.start()
            copies.append(cp)
        return first + len(pieces)

    def rows(lo):
        return pl.ds(lo, 2)

    copies, used = [], 0
    for dy, k, dst in ((1, 0, lb), (-1, 1, rb)):
        used = send(copies, around[0, dy], [(pk.at[k, :, own, :], dst.at[:, own, :])], used)
    for dy, k, dst, gq in ((1, 0, lb, gql), (-1, 1, rb, gqr)):
        for dx, lo, to in ((1, 2, 6), (-1, 0, 4)):
            side = 1 if dx > 0 else 0
            used = send(copies, around[dx, dy], [
                (pk.at[k, :, rows(lo), :], dst.at[:, rows(to), :]), (gqs.at[0, side], gq.at[0, side])], used)
    for dx, lo, to in ((1, 2, 6), (-1, 0, 4)):
        side = 1 if dx > 0 else 0
        used = send(copies, around[dx, 0], [
            (rl.at[:, rows(lo), :], rx.at[:, rows(to), :]),
            (stl.at[rows(lo), :], st.at[rows(to), :]),
            (opl.at[:, rows(lo), :], op.at[:, rows(to), :]),
            (qs.at[0, side], qr.at[0, side])], used)
    qsouth = [tree([g[i] * xl[a * n + i] for i in range(n)], jnp.add) for a in range(n)]
    qnorth = [tree([g[i] * xl[a * n + n - 1 - i] for i in range(n)], jnp.add) for a in range(n)]
    mm[0, 0:4, :] = gather_groups(qnorth, 7)[0:4, :]
    mm[1, 0:4, :] = gather_groups(qsouth, 5)[0:4, :]
    for b in range(n):
        qf[0, b] = qw[b] - opl[0] * jnp.where(sub == 0, 0.0, xc[0, b])
        qf[1, b] = qe[b] - opl[1] * jnp.where(sub == 3, 0.0, xc[1, b])
    for a in range(n):
        qf[2, a] = qsouth[a] - opl[2] * jnp.where(lane == 0, 0.0, lroll(qnorth[a], 1))
        qf[3, a] = qnorth[a] - opl[3] * jnp.where(lane == 127, 0.0, lroll(qsouth[a], -1))
    for a in range(n):
        row = [xl[a * n + i] for i in range(n)]
        for b in range(n):
            acc = tree([lop[b][i] * row[i] for i in range(n)] + [lop[a][i] * xl[i * n + b] for i in range(n)], jnp.add)
            t = rl[a * n + b] * row[b] - sl[a * n + b] + stl[...] * acc
            for edge, f, i in ((a == 0, 0, b), (a == n - 1, 1, b), (b == 0, 2, a), (b == n - 1, 3, a)):
                if edge:
                    t = t + qf[f, i]
            w[0, a * n + b, 0:4, :] = t[0:4, :]
    for dx, lo, to in ((1, 2, 6), (-1, 0, 4)):
        used = send(copies, around[dx, 0], [
            (w.at[0, :, rows(lo), :], w.at[0, :, rows(to), :]), (mm.at[:, rows(lo), :], mm.at[:, rows(to), :])], used)
    st[0:4, :] = stl[0:4, :]
    op[:, 0:4, :] = opl[:, 0:4, :]
    for q in range(0, n * n, 2):
        rxp[q // 2] = jnp.where(sub < 4, rl[q], pltpu.roll(rl[q + 1], 4, 0)) - shift
    for cp in loads[7:]:
        cp.wait()
    hear(0, "yz")
    tell(2, "xz")
    for cp in copies:
        cp.wait()

    before_half = slot16 < 6
    gsv, grx = [], []
    for b in range(n):
        lo, hi = lb[b], rb[b]
        gw[0, b] = jnp.where(before_half, lo, lroll(hi, 6))
        gsv.append(jnp.where(before_half, lroll(lo, -5), hi))
        grx.append(jnp.where(before_half, lroll(lo, -10), lroll(hi, -5)))
    spreads = [jnp.where(before_half, lb[n + f], rb[n + f]) for f in range(5)]
    gst = spreads[0]
    gopw = jnp.where(group == 0, spreads[1], 0.0)
    gope = jnp.where(group == n - 1, spreads[2], 0.0)
    gops, gopn = spreads[3], spreads[4]
    for side in (0, 1):
        gqr[0, side] = jnp.where(before_half, gql[0, side], gqr[0, side])

    low = sub < 4
    for j in range(n // 2):
        for i in range(n // 2):
            cpair[0, j * 4 + i] = jnp.where(low, lop[2 * j][2 * i], lop[2 * j + 1][2 * i + 1])
            cpair[1, j * 4 + i] = jnp.where(low, lop[2 * j][2 * i + 1], lop[2 * j + 1][2 * i])

    def pair_up(even, odd):
        return jnp.where(low, even, pltpu.roll(odd, 4, 0))

    def apply(k, last=False, fresh=None, after_strip=None, after_half=None):
        wide = k != 2

        def v(a, b):
            return w[k - 1, a * n + b]

        gv = [gw[k, b] for b in range(n)]
        gqsouth = tree([g[i] * gv[i] for i in range(n)], jnp.add)
        gqnorth = tree([g[i] * gv[n - 1 - i] for i in range(n)], jnp.add)
        if k:
            qsouth = [tree([g[i] * v(a, i) for i in range(n)], jnp.add) for a in range(n)]
            qnorth = [tree([g[i] * v(a, n - 1 - i) for i in range(n)], jnp.add) for a in range(n)]
        for a in range(n):
            below = jnp.where(lane == 0, lroll(gqnorth, -(16 * a + 5)), lroll(qnorth[a], 1) if k else 0.0)
            above = jnp.where(lane == 127, lroll(gqsouth, 121 - 16 * a), lroll(qsouth[a], -1) if k else 0.0)
            qf[2, a] = qsouth[a] - op[2] * below if k else -op[2] * below
            qf[3, a] = qnorth[a] - op[3] * above if k else -op[3] * above
        if not last:
            mn = gather_groups(qnorth, 7) if k else mm[0]
            ms = gather_groups(qsouth, 5) if k else mm[1]
            sterm = gqsouth - gops * jnp.where(slot16 == 6, mn, lroll(gqnorth, 1))
            nterm = gqnorth - gopn * jnp.where(slot16 == 5, ms, lroll(gqsouth, -1))
            for b in range(n):
                rolled, face = strip_faces(gv[b])
                prev = pltpu.roll(lroll(face, 16), 1, 0)
                nxt = pltpu.roll(lroll(face, -16), 7, 0)
                if fresh is not None:
                    prev = jnp.where(sub == 6, jnp.broadcast_to(lroll(gqr[fresh, 1, pl.ds(b, 1), :], 16), (8, 128)), prev)
                    nxt = jnp.where(sub == 5, jnp.broadcast_to(lroll(gqr[fresh, 0, pl.ds(b, 1), :], -16), (8, 128)), nxt)
                acc = tree([cline[i] * rolled[i] for i in range(n)] + [lop[b][i] * gv[i] for i in range(n)], jnp.add)
                t = grx[b] * gv[b] + gst * acc + (face - (gopw * prev + gope * nxt))
                if b == 0:
                    t = t + sterm
                if b == n - 1:
                    t = t + nterm
                t = t - (gsv[b] if k == 0 else shift * gv[b])
                if wide:
                    gw[k + 1, b] = t
                else:
                    gw[k + 1, b, 0:4, :] = t[0:4, :]
            if after_strip is not None:
                after_strip()
        if k == 0:
            for b in range(n):
                prev = jnp.where(sub == 4, xc[0, b], 0.0)
                nxt = jnp.where(sub == 7, xc[1, b], 0.0)
                prev = jnp.where(sub == 0, jnp.broadcast_to(qr[0, 1, pl.ds(b, 1), :], (8, 128)), prev)
                nxt = jnp.where(sub == 3, jnp.broadcast_to(qr[0, 0, pl.ds(b, 1), :], (8, 128)), nxt)
                qf[0, b] = -op[0] * prev
                qf[1, b] = -op[1] * nxt
            for a in range(n):
                for b in range(n):
                    t = w[0, a * n + b]
                    edges = ((a == 0, 0, b), (a == n - 1, 1, b), (b == 0, 2, a), (b == n - 1, 3, a))
                    for edge, f, i in edges:
                        if edge:
                            t = t + qf[f, i]
                    if any(edge for edge, f, i in edges):
                        w[0, a * n + b] = t
                    if b % 2 == 0:
                        even = t
                    else:
                        wp[0, (a * n + b) // 2] = pair_up(even, t)
            return
        for b in range(n):
            qwest = tree([g[i] * v(i, b) for i in range(n)], jnp.add)
            qeast = tree([g[i] * v(n - 1 - i, b) for i in range(n)], jnp.add)
            prev = pltpu.roll(qeast, 1, 0)
            nxt = pltpu.roll(qwest, 7, 0)
            if fresh is not None:
                prev = jnp.where(sub == 6, jnp.broadcast_to(qr[fresh, 1, pl.ds(b, 1), :], (8, 128)), prev)
                nxt = jnp.where(sub == 5, jnp.broadcast_to(qr[fresh, 0, pl.ds(b, 1), :], (8, 128)), nxt)
            qf[0, b] = qwest - op[0] * prev
            qf[1, b] = qeast - op[1] * nxt
        if not wide or last:
            stiff = pair_up(st[...], st[...])
            for a in range(n):
                tiles = [wp[k - 1, a * 4 + j] for j in range(4)]
                swapped = [pltpu.roll(t, 4, 0) for t in tiles]
                for j in range(4):
                    q = a * n + 2 * j
                    acc = tree([lop[a][i] * wp[k - 1, i * 4 + j] for i in range(n)]
                               + [cpair[0, j * 4 + i] * tiles[i] for i in range(4)]
                               + [cpair[1, j * 4 + i] * swapped[i] for i in range(4)], jnp.add)
                    t = rxp[q // 2] * tiles[j] + stiff * acc
                    if a == 0:
                        t = t + pair_up(qf[0, 2 * j], qf[0, 2 * j + 1])
                    if a == n - 1:
                        t = t + pair_up(qf[1, 2 * j], qf[1, 2 * j + 1])
                    if j == 0:
                        t = t + jnp.where(low, qf[2, a], 0.0)
                    if j == 3:
                        t = t + jnp.where(low, 0.0, pltpu.roll(qf[3, a], 4, 0))
                    wp[k, q // 2] = t
                    if not last:
                        w[k, q, 0:4, :] = t[0:4, :]
                        w[k, q + 1, 0:4, :] = pltpu.roll(t, 4, 0)[0:4, :]
                if a == 3 and after_half is not None:
                    after_half()
            return
        stiff = st[...]
        for a in range(n):
            row = [v(a, i) for i in range(n)]
            even = None
            for b in range(n):
                acc = tree([lop[b][i] * row[i] for i in range(n)] + [lop[a][i] * v(i, b) for i in range(n)], jnp.add)
                t = (rx[a * n + b] - shift) * row[b] + stiff * acc
                if a == 0:
                    t = t + qf[0, b]
                if a == n - 1:
                    t = t + qf[1, b]
                if b == 0:
                    t = t + qf[2, a]
                if b == n - 1:
                    t = t + qf[3, a]
                w[k, a * n + b] = t
                if b % 2 == 0:
                    even = t
                else:
                    wp[k, (a * n + b) // 2] = pair_up(even, t)

    apply(0, fresh=0)
    apply(1)
    hear(2, "xz")
    tell(4, "xz")
    copies = []
    sides = ((1, 2, 6), (-1, 0, 4))

    def send_strip():
        nonlocal used
        for b in range(n):
            t = jnp.concatenate([gw[3, b, 0:4, :]] * 2, axis=0)
            face = strip_faces(t)[1]
            gqs[1, 0, pl.ds(b, 1), :] = face[2:3, :]
            gqs[1, 1, pl.ds(b, 1), :] = face[1:2, :]
        for dx, lo, to in sides:
            side = 1 if dx > 0 else 0
            used = send(copies, around[dx, 0], [
                (gw.at[3, :, rows(lo), :], gw.at[3, :, rows(to), :]), (gqs.at[1, side], gqr.at[1, side])], used)

    def send_block(first):
        nonlocal used
        part = pl.ds(first, n * n // 2)
        for dx, lo, to in sides:
            used = send(copies, around[dx, 0], [(w.at[2, part, rows(lo), :], w.at[2, part, rows(to), :])], used)

    apply(2, after_strip=send_strip, after_half=lambda: send_block(0))
    send_block(n * n // 2)
    qw, qe = x_faces(lambda a, b: w[2, a * n + b, 0:4, :])
    for b in range(n):
        qs[1, 0, pl.ds(b, 1), :] = qw[b][2:3, :]
        qs[1, 1, pl.ds(b, 1), :] = qe[b][1:2, :]
    for dx, lo, to in sides:
        side = 1 if dx > 0 else 0
        used = send(copies, around[dx, 0], [(qs.at[1, side], qr.at[1, side])], used)
    def gram(pairs):
        top = max(j for i, j in pairs) + 1

        def body(q, acc):
            vals = [wp[i, q] for i in range(top)]
            return tuple(t + vals[i] * vals[j] for t, (i, j) in zip(acc, pairs))

        return lax.fori_loop(0, n * n // 2, body, tuple(jnp.zeros((8, 128), jnp.float32) for _ in pairs), unroll=8)

    early = [p for p in PAIRS if p[1] < 3]
    first = gram(early)
    hear(4, "xz")
    pl.semaphore_signal(known.at[6], inc=1, device_id=partner, device_id_type=MESH)
    for cp in copies:
        cp.wait()
    apply(3, fresh=1)
    apply(4)
    apply(5, last=True)

    acc = first + gram(PAIRS[len(early):])
    high = low_part = jnp.zeros((8, 128), jnp.float32)
    for base in range(0, len(PAIRS), 8):
        packed = jnp.zeros((8, 128), jnp.float32)
        for i, t in enumerate(acc[base:base + 8]):
            t = t + pltpu.roll(t, 4, 0)
            t = t + pltpu.roll(t, 2, 0)
            t = t + pltpu.roll(t, 1, 0)
            packed = jnp.where(sub == i, t, packed)
        packed = packed * (1.0 / total)
        bias = jnp.max(jnp.abs(packed), axis=1, keepdims=True) * 256.0
        lead = (packed + bias) - bias
        here = lane == sub + base
        high = jnp.where(here, jnp.sum(lead, axis=1, keepdims=True), high)
        low_part = jnp.where(here, jnp.sum(packed - lead, axis=1, keepdims=True), low_part)
    for s in (4, 2, 1):
        high = high + pltpu.roll(high, s, 0)
        low_part = low_part + pltpu.roll(low_part, s, 0)
    row1[0:1, :] = high[0:1, :]
    row1[1:2, :] = low_part[0:1, :]

    def to_hub(j, index, peer):
        return pltpu.make_async_remote_copy(
            src_ref=row1, dst_ref=buf1.at[index], send_sem=s1.at[j], recv_sem=r1.at[index],
            device_id=peer, device_id_type=MESH)

    def across(j, index, peer):
        return pltpu.make_async_remote_copy(
            src_ref=row2, dst_ref=buf2.at[index], send_sem=s2.at[j], recv_sem=r2.at[index],
            device_id=peer, device_id_type=MESH)

    pl.semaphore_wait(known.at[6], 1)
    for j in flat:
        to_hub(j, me, (plane[j][0], nc - 1, plane[j][1], z)).start()

    @pl.when(hub)
    def _():
        buf1[me] = row1[...]
        for j, (yy, xx) in enumerate(plane):
            for cc in range(nc):
                if j or cc != nc - 1:
                    to_hub(j, (cc * ny + yy) * nx + xx, partner).wait_recv()
        total1 = tree([(buf1[j, 0:1, :], buf1[j, 1:2, :]) for j in range(nc * ny * nx)], add2)
        total1 = tidy(total1)
        row2[0:1, :] = total1[0]
        row2[1:2, :] = total1[1]
        for cc in (nc - 1, 0):
            for k in far:
                across(cc * len(planes) + k - 1, z, (y, cc, x, planes[k - 1])).start()
        across(2 * len(planes), z, partner).start()
        buf2[z] = row2[...]

    @pl.when(jnp.logical_not(hub))
    def _():
        to_hub(0, me, partner).start()
        across(0, z, partner).wait_recv()
        to_hub(0, me, partner).wait_send()

    for zz in planes:
        across(0, zz, partner).wait_recv()
    for j in range(1, len(plane)):
        to_hub(j, me, partner).wait_send()

    @pl.when(hub)
    def _():
        for k in range(2 * len(planes) + 1):
            across(k, z, partner).wait_send()

    part = tidy(tree([(buf2[j, 0:1, :], buf2[j, 1:2, :]) for j in range(nz)], add2))

    slot = {}
    for p, (i, j) in enumerate(PAIRS):
        slot[i, j] = slot[j, i] = p
    columns = []
    for k in range(NV):
        at = jnp.full((8, 128), -1, jnp.int32)
        for i in range(NV):
            at = jnp.where(sub == i, slot[i, k], at)
        columns.append(tuple(
            jnp.broadcast_to(
                jnp.sum(jnp.where(lane == at, jnp.broadcast_to(t, (8, 128)), 0.0), axis=1, keepdims=True), (8, 128))
            for t in part))

    def spread(t, k):
        return jnp.broadcast_to(t[k:k + 1, :], (8, 128))

    def dot(a, b):
        return sublane_total(mul2(a, b))

    wide_shift = jnp.broadcast_to(shift, (8, 128))
    moved = [add2(columns[k + 1], mul1(columns[k], wide_shift)) for k in range(ITERS)]
    moved = [tidy(t) for t in moved]
    hmat = jnp.zeros((8, 128), jnp.float32)
    zeros = jnp.zeros((8, 128), jnp.float32)
    u = (jnp.where(sub == 0, -1.0, 0.0), zeros)
    e = tuple(-t for t in columns[0])
    ratio = None
    coefs, images = [], []
    for j in range(NV):
        square = dot(u, e)[0]
        square = (square if ratio is None else square * (ratio * ratio)) + FLOOR
        inv = lax.rsqrt(square)
        if j > 0:
            hmat = jnp.where((sub == j) & (lane == j - 1), square * inv, hmat)
        unit = inv if ratio is None else inv * ratio
        coefs.append(tidy(mul1(u, unit)))
        if j == ITERS:
            break
        images.append(tidy(mul1(e, unit)))
        m = tidy(add2(tuple(pltpu.roll(t, 1, 0) for t in u), mul1(u, wide_shift)))
        f = tree([mul2(moved[k], tuple(spread(t, k) for t in u)) for k in range(j + 1)], add2)
        parts = [dot(images[i], m)[0] for i in range(j)]
        own = dot(e, m)[0] * (unit * unit)
        for i in range(j):
            hmat = jnp.where((sub == i) & (lane == j), parts[i] * unit, hmat)
        hmat = jnp.where((sub == j) & (lane == j), own, hmat)
        u, e = (
            tidy(tree([x] + [mul1(basis[i], -parts[i]) for i in range(j)] + [mul1(latest, -own)], add2))
            for x, basis, latest in ((m, coefs, u), (f, images, e)))
        ratio = unit
    hm[...] = hmat
    for j in range(NV):
        cw[j] = coefs[j][0]


def output_kernel(w, cw, hm, hess_h, out_h, hess, vout, sem):
    half = w.shape[1]
    hess[...] = hm[0:NV, 0:ITERS]
    outs = [pltpu.make_async_copy(hess, hess_h, sem.at[0])]
    outs[0].start()
    for j in range(NV):
        weights = [jnp.broadcast_to(cw[j, pl.ds(i, 1), :], (8, 128)) for i in range(j + 1)]

        def combine(q, carry):
            t = tree([weights[i] * w[i, q] for i in range(j + 1)], jnp.add)
            vout[j, 2 * q] = t[0:4, :]
            vout[j, 2 * q + 1] = t[4:8, :]
            return carry

        lax.fori_loop(0, half, combine, 0, unroll=8)
        cp = pltpu.make_async_copy(vout.at[j], out_h.at[j], sem.at[j + 1])
        cp.start()
        outs.append(cp)
    for cp in outs:
        cp.wait()


def solution(mesh):
    ny, nc, nx, nz = 4, 2, 4, 8
    finer = Mesh(mesh.devices.reshape(ny, nc, nx, nz), AXES)
    gxs, gys = ("y", "c"), ("x", "z")
    sizes = (ny, nc, nx, nz)
    f32 = jnp.float32

    def body(source, initial, reaction, stiffness, line_op, face_deriv, wall_flags):
        nodes, ex, ey = source.shape
        hbm = pl.BlockSpec(memory_space=pltpu.HBM)
        scalars = pl.BlockSpec(memory_space=pltpu.SMEM)
        local = pl.BlockSpec(memory_space=pltpu.VMEM)
        vm = pltpu.VMEM
        dma = pltpu.SemaphoreType.DMA
        tile = (8, ey)
        sends = 2 + 8 + 12 + 10
        w, cw, hm = pl.pallas_call(
            functools.partial(kernel, sizes),
            out_shape=(
                pltpu.VMEM((NV, nodes // 2) + tile, f32), pltpu.VMEM((NV,) + tile, f32), pltpu.VMEM(tile, f32),
            ),
            in_specs=[hbm] * 7,
            out_specs=(local, local, local),
            scratch_shapes=[
                vm((nodes,) + tile, f32), vm((nodes,) + tile, f32), vm((nodes,) + tile, f32), vm(tile, f32),
                vm((4,) + tile, jnp.int32), vm((4,) + tile, f32),
                vm((NV - 1, nodes) + tile, f32), vm((nodes,) + tile, f32),
                vm(tile, f32), vm((4,) + tile, f32), vm((NV, 8) + tile, f32),
                vm((2, 13) + tile, f32), vm((13,) + tile, f32), vm((13,) + tile, f32),
                vm((2, 2) + tile, f32), vm((2, 2) + tile, f32), vm((2, 2) + tile, f32), vm((1, 2) + tile, f32),
                vm((2, 2) + tile, f32), vm((4, 8) + tile, f32),
                vm((2, 128), f32), vm((nc * ny * nx, 2, 128), f32), vm((2, 128), f32), vm((nz, 2, 128), f32),
                pltpu.SMEM((P_SIZE, P_SIZE), f32), pltpu.SMEM((P_SIZE,), f32),
                vm((nodes // 2,) + tile, f32), vm((2, 16) + tile, f32),
                vm((2, 8) + tile, f32), vm((2,) + tile, f32), pltpu.SemaphoreType.REGULAR((7,)),
                dma((8,)), dma((sends,)), dma((sends,)), dma((ny * nx,)), dma((nc * ny * nx,)), dma((2 * nz - 1,)), dma((nz,)),
            ],
            compiler_params=pltpu.CompilerParams(
                collective_id=0, has_side_effects=True, vmem_limit_bytes=48 * 1024 * 1024),
            name="arnoldi",
        )(*[pltpu.with_memory_space_constraint(t, pltpu.HBM) for t in (
            line_op, face_deriv, source, initial, reaction, stiffness, wall_flags)])
        return pl.pallas_call(
            output_kernel,
            out_shape=(
                jax.ShapeDtypeStruct((NV, ITERS), f32),
                jax.ShapeDtypeStruct((NV, nodes, ex, ey), f32),
            ),
            in_specs=[local] * 3,
            out_specs=(hbm, hbm),
            scratch_shapes=[vm((NV, ITERS), f32), vm((NV, nodes, ex, ey), f32), dma((NV + 1,))],
            compiler_params=pltpu.CompilerParams(vmem_limit_bytes=16 * 1024 * 1024),
            name="combine",
        )(w, cw, hm)

    placed = (P(None, gxs, gys), P(None, gxs, gys), P(None, gxs, gys), P(gxs, gys), P(), P(), P(None, gxs, gys))
    return jax.shard_map(
        body, mesh=finer, in_specs=placed, out_specs=(P(), P(None, None, gxs, gys)), check_vma=False)
```
